32 devices in a mesh: ctx: 8 (over y, x, core), fsdp: 4 (over z).
Axes of the slice: x: 2, y: 2, z: 4, core: 2. Of those that a mesh axis runs over, the one named last changes fastest.
Arguments:
- block_input: bfloat16 [4096, 2048], P(('ctx', 'fsdp')), may hold values from -6 to 6
- positions: int32 [4096], P(('ctx', 'fsdp')), may hold values from 0 to 4095, as said below
- query_weight: bfloat16 [2048, 2048], P(None, 'fsdp'), may hold values from -0.125 to 0.125
- key_weight: bfloat16 [2048, 2048], P(None, 'fsdp'), may hold values from -0.125 to 0.125
- value_weight: bfloat16 [2048, 2048], P(None, 'fsdp'), may hold values from -0.125 to 0.125
- output_weight: bfloat16 [2048, 2048], P('fsdp'), may hold values from -0.125 to 0.125
- query_gain: float32 [2048], replicated, may hold values from 0.7 to 6.5
- key_gain: float32 [2048], replicated, may hold values from 0.7 to 6.5
- attn_gain: float32 [2048], replicated, may hold values from 0.1 to 1.9
- mlp_gain: float32 [2048], replicated, may hold values from 0.1 to 1.9
- gate_weight: bfloat16 [2048, 8192], P(None, 'fsdp'), may hold values from -0.125 to 0.125
- up_weight: bfloat16 [2048, 8192], P(None, 'fsdp'), may hold values from -0.125 to 0.125
- down_weight: bfloat16 [8192, 2048], P('fsdp'), may hold values from -0.0625 to 0.0625
- cotangent: bfloat16 [4096, 2048], P(('ctx', 'fsdp')), may hold values from -6 to 6
Outputs:
- block_output: bfloat16 [4096, 2048], P(('ctx', 'fsdp'))
- input_grad: float32 [4096, 2048], P(('ctx', 'fsdp'))
- query_weight_grad: float32 [2048, 2048], P('ctx', 'fsdp')
- key_weight_grad: float32 [2048, 2048], P('ctx', 'fsdp')
- value_weight_grad: float32 [2048, 2048], P('ctx', 'fsdp')
- output_weight_grad: float32 [2048, 2048], P('fsdp', 'ctx')
- query_gain_grad: float32 [2048], P('ctx')
- key_gain_grad: float32 [2048], P('ctx')
- attn_gain_grad: float32 [2048], P('ctx')
- mlp_gain_grad: float32 [2048], P('ctx')
- gate_weight_grad: float32 [2048, 8192], P('ctx', 'fsdp')
- up_weight_grad: float32 [2048, 8192], P('ctx', 'fsdp')
- down_weight_grad: float32 [8192, 2048], P('fsdp', 'ctx')
The draws below stay inside these ranges and needn't reach their ends.
Inputs may be any that keep to these rules, and one draw needn't show every extreme that they name: positions hold every number below 4096 once, in runs of 256 consecutive numbers each starting at a multiple of 256; the order of the runs is arbitrary.
All inputs are finite; a program needn't handle non-finite values.
Results may differ from the reference program's by a relative error of at most 0.04.
Values may be sent and summed in bfloat16 or wider, within the bound.
A program may use at most 384 MiB of HBM per device.

```python
import math
import jax
import jax.numpy as jnp
from jax import lax

D = 2048
HEADS = 16
HD = 128
FF = 8192
BLOCK = 256
HALVES = 16
TOKENS = 4096


def draw_positions(key, part):
    order = jax.random.permutation(key, HALVES).astype(jnp.int32)
    offsets = jnp.arange(BLOCK).astype(jnp.int32)
    return (order[:, None] * BLOCK + offsets[None, :]).reshape(-1)


def gain_values(key):
    base_key = jax.random.fold_in(key, 0)
    spread = jax.random.uniform(base_key, (D,), jnp.float32, 0.7, 1.3)
    return spread


def draw_query_gain(key, part):
    return gain_values(jax.random.fold_in(key, 11))


def draw_key_gain(key, part):
    return gain_values(jax.random.fold_in(key, 23))


def block_scale(stream_key, extent, pieces, low, top_value):
    loudness = 1.0
    for position, shards_of in pieces:
        steps = jax.random.uniform(jax.random.fold_in(jax.random.fold_in(stream_key, 6), position), (shards_of,), jnp.float32, low / len(pieces), top_value / len(pieces))
        loudness = loudness * jnp.repeat(jnp.exp(steps), extent[position] // shards_of).reshape((-1,) + (1,) * (len(extent) - 1 - position))
    return loudness


def bell_draw(stream_key, shape, scale, limit, cuts=(), held_as=jnp.bfloat16):
    result = scale * jax.random.normal(stream_key, shape, jnp.float32)
    if cuts:
        result = result * block_scale(stream_key, shape, cuts, -0.22, 0.18)
    return jnp.clip(result, -limit, limit).astype(held_as)


def setup_inputs(seed: int = 0) -> dict:
    streams_of = jax.random.split(jax.random.key(seed), 15)
    return {
        "block_input": bell_draw(streams_of[0], (TOKENS, D), 1.0, 6.0, ((0, 32),)),
        "positions": draw_positions(jax.random.fold_in(streams_of[14], 71), 0),
        "query_weight": bell_draw(streams_of[2], (D, D), D ** -0.5, 0.125, ((1, 4),)),
        "key_weight": bell_draw(streams_of[3], (D, D), D ** -0.5, 0.125, ((1, 4),)),
        "value_weight": bell_draw(streams_of[4], (D, D), D ** -0.5, 0.125, ((1, 4),)),
        "output_weight": bell_draw(streams_of[5], (D, D), D ** -0.5, 0.125, ((0, 4),)),
        "query_gain": draw_query_gain(jax.random.fold_in(streams_of[14], 71), 0),
        "key_gain": draw_key_gain(jax.random.fold_in(streams_of[14], 71), 0),
        "attn_gain": jnp.clip(1.0 + 0.18 * jax.random.normal(streams_of[8], (D,), jnp.float32), 0.1, 1.9),
        "mlp_gain": jnp.clip(1.0 + 0.18 * jax.random.normal(streams_of[9], (D,), jnp.float32), 0.1, 1.9),
        "gate_weight": bell_draw(streams_of[10], (D, FF), D ** -0.5, 0.125, ((1, 4),)),
        "up_weight": bell_draw(streams_of[11], (D, FF), D ** -0.5, 0.125, ((1, 4),)),
        "down_weight": bell_draw(streams_of[12], (FF, D), FF ** -0.5, 0.0625, ((0, 4),)),
        "cotangent": bell_draw(streams_of[13], (TOKENS, D), 1.0, 6.0, ((0, 32),)),
    }


norm_eps = 1e-06
rope_base = 500000.0
big_negative = -1e+30

def rotate(tensor, row_positions, heads_count, head_width, inverse):
    row_count = tensor.shape[0]
    halfway = head_width // 2
    shaped = tensor.reshape(row_count, heads_count, head_width)
    freqs = jnp.exp(-math.log(rope_base) * 2.0 * jnp.arange(halfway).astype(jnp.float32) / head_width)
    angles = row_positions.astype(jnp.float32)[:, None] * freqs[None, :]
    cosine = jnp.cos(angles)[:, None, :]
    sine = jnp.sin(angles)[:, None, :]
    if inverse:
        sine = -sine
    first = shaped[:, :, :halfway]
    second = shaped[:, :, halfway:]
    turned = jnp.concatenate([first * cosine - second * sine, second * cosine + first * sine], axis=2)
    return turned.reshape(row_count, heads_count * head_width)

def norm_back(raw, rms_inv, gain, grad_out, width):
    weighted = gain * grad_out
    inner = lax.optimization_barrier(jnp.sum(weighted * raw, axis=1, keepdims=True))
    return rms_inv[:, None] * weighted - raw * (rms_inv * rms_inv * rms_inv)[:, None] * inner / width

def reference(block_input, positions, query_weight, key_weight, value_weight, output_weight, query_gain, key_gain, attn_gain, mlp_gain, gate_weight, up_weight, down_weight, cotangent):
    score_scale = 1.0 / math.sqrt(HD)
    qblock = math.gcd(2048, TOKENS)
    nblocks = TOKENS // qblock
    block_ids = jnp.arange(nblocks).astype(jnp.int32)
    queries = jnp.dot(block_input, query_weight, preferred_element_type=jnp.float32)
    keys_raw = jnp.dot(block_input, key_weight, preferred_element_type=jnp.float32)
    values_b = jnp.dot(block_input, value_weight, preferred_element_type=jnp.float32).astype(jnp.bfloat16)
    query_rms = lax.rsqrt(lax.optimization_barrier(jnp.mean(queries * queries, axis=1)) + norm_eps)
    key_rms = lax.rsqrt(lax.optimization_barrier(jnp.mean(keys_raw * keys_raw, axis=1)) + norm_eps)
    query_normed = queries * query_rms[:, None] * query_gain[None, :]
    key_normed = keys_raw * key_rms[:, None] * key_gain[None, :]
    query_rot = rotate(query_normed, positions, HEADS, HD, False).astype(jnp.bfloat16)
    key_rot = rotate(key_normed, positions, HEADS, HD, False).astype(jnp.bfloat16)

    def split_heads(tensor):
        return tensor.reshape(TOKENS, HEADS, HD).transpose(1, 0, 2)

    def join_heads(tensor):
        return tensor.transpose(1, 0, 2).reshape(TOKENS, D)

    def head_forward(operands):
        query_head, key_head, value_head = operands

        def step_block(unused, block_id):
            first_row = block_id * qblock
            query_rows = lax.dynamic_slice_in_dim(query_head, first_row, qblock, 0)
            row_pos = lax.dynamic_slice_in_dim(positions, first_row, qblock, 0)
            scores = jnp.dot(query_rows, key_head.T, preferred_element_type=jnp.float32) * score_scale
            allowed = positions[None, :] <= row_pos[:, None]
            scores = jnp.where(allowed, scores, big_negative)
            row_max = lax.optimization_barrier(jnp.max(scores, axis=1))
            weights = jnp.where(allowed, jnp.exp(scores - row_max[:, None]), 0.0)
            row_sum = lax.optimization_barrier(jnp.sum(weights, axis=1))
            mixture = jnp.dot(weights.astype(jnp.bfloat16), value_head, preferred_element_type=jnp.float32) / row_sum[:, None]
            return (unused, (mixture, row_max + jnp.log(row_sum)))
        unused, outputs = lax.scan(step_block, jnp.zeros((), jnp.float32), block_ids)
        return (outputs[0].reshape(TOKENS, HD), outputs[1].reshape(TOKENS))
    query_heads = split_heads(query_rot)
    key_heads = split_heads(key_rot)
    value_heads = split_heads(values_b)
    mixture_heads, log_total = lax.map(head_forward, (query_heads, key_heads, value_heads))
    mixture = join_heads(mixture_heads)
    mixture_b = mixture.astype(jnp.bfloat16)
    attn_out = jnp.dot(mixture_b, output_weight, preferred_element_type=jnp.float32)
    attn_rms = lax.rsqrt(lax.optimization_barrier(jnp.mean(attn_out * attn_out, axis=1)) + norm_eps)
    hidden_state = block_input.astype(jnp.float32) + attn_out * attn_rms[:, None] * attn_gain[None, :]
    state_b = hidden_state.astype(jnp.bfloat16)
    gate_pre = jnp.dot(state_b, gate_weight, preferred_element_type=jnp.float32)
    up_pre = jnp.dot(state_b, up_weight, preferred_element_type=jnp.float32)
    activated = (jax.nn.silu(gate_pre) * up_pre).astype(jnp.bfloat16)
    mlp_out = jnp.dot(activated, down_weight, preferred_element_type=jnp.float32)
    mlp_rms = lax.rsqrt(lax.optimization_barrier(jnp.mean(mlp_out * mlp_out, axis=1)) + norm_eps)
    block_output = (hidden_state + mlp_out * mlp_rms[:, None] * mlp_gain[None, :]).astype(jnp.bfloat16)
    upstream = cotangent.astype(jnp.float32)
    mlp_gain_grad = lax.optimization_barrier(jnp.sum(upstream * mlp_out * mlp_rms[:, None], axis=0))
    mlp_grad_b = norm_back(mlp_out, mlp_rms, mlp_gain[None, :], upstream, D).astype(jnp.bfloat16)
    activ_grad = jnp.dot(mlp_grad_b, down_weight.T, preferred_element_type=jnp.float32)
    down_weight_grad = jnp.dot(activated.T, mlp_grad_b, preferred_element_type=jnp.float32)
    sigmoid_gate = jax.nn.sigmoid(gate_pre)
    gate_grad_b = (activ_grad * up_pre * sigmoid_gate * (1.0 + gate_pre * (1.0 - sigmoid_gate))).astype(jnp.bfloat16)
    up_grad_b = (activ_grad * gate_pre * sigmoid_gate).astype(jnp.bfloat16)
    gate_weight_grad = jnp.dot(state_b.T, gate_grad_b, preferred_element_type=jnp.float32)
    up_weight_grad = jnp.dot(state_b.T, up_grad_b, preferred_element_type=jnp.float32)
    state_grad = upstream + jnp.dot(gate_grad_b, gate_weight.T, preferred_element_type=jnp.float32) + jnp.dot(up_grad_b, up_weight.T, preferred_element_type=jnp.float32)
    attn_gain_grad = lax.optimization_barrier(jnp.sum(state_grad * attn_out * attn_rms[:, None], axis=0))
    attn_grad_b = norm_back(attn_out, attn_rms, attn_gain[None, :], state_grad, D).astype(jnp.bfloat16)
    output_weight_grad = jnp.dot(mixture_b.T, attn_grad_b, preferred_element_type=jnp.float32)
    mixture_grad_b = jnp.dot(attn_grad_b, output_weight.T, preferred_element_type=jnp.float32).astype(jnp.bfloat16)

    def head_backward(operands):
        query_head, key_head, value_head, grad_head, mixture_head, log_head = operands
        row_delta = lax.optimization_barrier(jnp.sum(grad_head.astype(jnp.float32) * mixture_head, axis=1))

        def step_block(carry_grads, block_id):
            key_acc, value_acc = carry_grads
            first_row = block_id * qblock
            query_rows = lax.dynamic_slice_in_dim(query_head, first_row, qblock, 0)
            grad_rows = lax.dynamic_slice_in_dim(grad_head, first_row, qblock, 0)
            delta_rows = lax.dynamic_slice_in_dim(row_delta, first_row, qblock, 0)
            log_rows = lax.dynamic_slice_in_dim(log_head, first_row, qblock, 0)
            row_pos = lax.dynamic_slice_in_dim(positions, first_row, qblock, 0)
            scores = jnp.dot(query_rows, key_head.T, preferred_element_type=jnp.float32) * score_scale
            allowed = positions[None, :] <= row_pos[:, None]
            scores = jnp.where(allowed, scores, big_negative)
            probs = jnp.where(allowed, jnp.exp(scores - log_rows[:, None]), 0.0)
            prob_grad = jnp.dot(grad_rows, value_head.T, preferred_element_type=jnp.float32)
            score_grad_b = (probs * (prob_grad - delta_rows[:, None])).astype(jnp.bfloat16)
            query_grad = jnp.dot(score_grad_b, key_head, preferred_element_type=jnp.float32) * score_scale
            key_acc = key_acc + jnp.dot(score_grad_b.T, query_rows, preferred_element_type=jnp.float32) * score_scale
            value_acc = value_acc + jnp.dot(probs.astype(jnp.bfloat16).T, grad_rows, preferred_element_type=jnp.float32)
            return ((key_acc, value_acc), query_grad)
        empty_grads = jnp.zeros((TOKENS, HD), jnp.float32)
        carried, query_grad = lax.scan(step_block, (empty_grads, empty_grads), block_ids)
        return (query_grad.reshape(TOKENS, HD), carried[0], carried[1])
    query_head_grad, key_head_grad, value_head_grad = lax.map(head_backward, (query_heads, key_heads, value_heads, split_heads(mixture_grad_b), mixture_heads, log_total))
    query_normed_grad = rotate(join_heads(query_head_grad), positions, HEADS, HD, True)
    key_normed_grad = rotate(join_heads(key_head_grad), positions, HEADS, HD, True)
    query_gain_grad = lax.optimization_barrier(jnp.sum(query_normed_grad * queries * query_rms[:, None], axis=0))
    key_gain_grad = lax.optimization_barrier(jnp.sum(key_normed_grad * keys_raw * key_rms[:, None], axis=0))
    query_grad_b = norm_back(queries, query_rms, query_gain[None, :], query_normed_grad, D).astype(jnp.bfloat16)
    key_grad_b = norm_back(keys_raw, key_rms, key_gain[None, :], key_normed_grad, D).astype(jnp.bfloat16)
    value_grad_b = join_heads(value_head_grad).astype(jnp.bfloat16)
    query_weight_grad = jnp.dot(block_input.T, query_grad_b, preferred_element_type=jnp.float32)
    key_weight_grad = jnp.dot(block_input.T, key_grad_b, preferred_element_type=jnp.float32)
    value_weight_grad = jnp.dot(block_input.T, value_grad_b, preferred_element_type=jnp.float32)
    input_grad = state_grad + jnp.dot(query_grad_b, query_weight.T, preferred_element_type=jnp.float32) + jnp.dot(key_grad_b, key_weight.T, preferred_element_type=jnp.float32) + jnp.dot(value_grad_b, value_weight.T, preferred_element_type=jnp.float32)
    return (block_output, input_grad, query_weight_grad, key_weight_grad, value_weight_grad, output_weight_grad, query_gain_grad, key_gain_grad, attn_gain_grad, mlp_gain_grad, gate_weight_grad, up_weight_grad, down_weight_grad)
```

```python
import functools
import math

import jax
import jax.numpy as jnp
from jax import lax
from jax.experimental import pallas as pl
from jax.experimental.pallas import tpu as pltpu
from jax.sharding import PartitionSpec as P

HD = 128
norm_eps = 1e-06
rope_base = 500000.0
big_negative = -1e30
LOG2E = math.log2(math.e)
BF = jnp.bfloat16
F32 = jnp.float32


def mm(left, right):
    return jnp.dot(left, right, preferred_element_type=F32)


def contract_rows(left, right):
    return lax.dot_general(left, right, (((0,), (0,)), ((), ())), preferred_element_type=F32)


def contract_cols(left, right):
    return lax.dot_general(left, right, (((1,), (1,)), ((), ())), preferred_element_type=F32)


def gate(x, *tokens):
    return lax.optimization_barrier((x, *tokens))[0]


def shift(x, n, by):
    return lax.ppermute(x, "fsdp", [(i, (i + by) % n) for i in range(n)])


def ring_gather(x, n, under=()):
    slots = [x]
    for i in range(n - 1):
        got = shift(slots[-1], n, 1)
        slots.append(gate(got, under[i]) if i < len(under) else got)
    return slots


def ring_scatter(part, n, under=()):
    if n == 1:
        return part(0)
    acc = part(1).astype(BF)
    for s in range(2, n):
        acc = (shift(acc, n, 1).astype(F32) + part(s)).astype(BF)
    return gate(shift(acc, n, 1), *under).astype(F32) + part(0)


def slot_sum(x, n):
    total = x
    for t in range(1, n):
        total = total + jnp.roll(shift(x, n, t), t, axis=0)
    return total


def flat_sum(x, n):
    total = x
    for t in range(1, n):
        total = total + shift(x, n, t)
    return total


def swap(x, n, bit):
    return lax.ppermute(x, "ctx", [(i, i ^ bit) for i in range(n)])


def bit_orders(n):
    bits = []
    b = 2
    while b < n:
        bits.append(b)
        b *= 2
    return bits, bits[::-1]


def distance(m):
    return bin(m >> 1).count("1")


def group_order(n):
    pairs = [(m, m + 1) if n > 1 else (m,) for m in range(0, n, 2)]
    return sorted(pairs, key=lambda g: (distance(g[0]), g[0]))


def came_from(m, order):
    if m & 1:
        return m ^ 1, 1
    bit = [b for b in order if m & b][-1]
    return m ^ bit, bit


def vmem(*_):
    return pl.BlockSpec(memory_space=pltpu.VMEM)


def prep_kernel(n, heads, *refs):
    q_refs, k_refs, v_refs = refs[:n], refs[n : 2 * n], refs[2 * n : 3 * n]
    qr_ref, kr_ref, qg_ref, kg_ref, cos_ref, sin_ref = refs[3 * n : 3 * n + 6]
    qo_ref, kva_ref, kvb_ref = refs[3 * n + 6 :]
    rows = q_refs[0].shape[0]
    half = n // 2
    for s in range(n):
        r = slice(s * rows, (s + 1) * rows)
        cosine, sine = cos_ref[r, :], sin_ref[r, :]
        out = kva_ref if s < half else kvb_ref
        o = slice((s % half) * rows, (s % half + 1) * rows)
        for h in range(heads):
            c = slice(h * HD, (h + 1) * HD)
            x = q_refs[s][:, c] * qr_ref[r, :] * qg_ref[:, c]
            qo_ref[r, c] = (x * cosine + pltpu.roll(x, HD // 2, 1) * sine).astype(BF)
            y = k_refs[s][:, c] * kr_ref[r, :] * kg_ref[:, c]
            out[o, c] = (y * cosine + pltpu.roll(y, HD // 2, 1) * sine).astype(BF)
            out[o, heads * HD + h * HD : heads * HD + (h + 1) * HD] = v_refs[s][:, c].astype(BF)


def key_mask(starts_ref, piece, slots, rows, qpos):
    parts = []
    for j in range(slots):
        row = lax.broadcasted_iota(jnp.int32, (rows, 1), 0)
        parts.append(row + starts_ref[piece * slots + j])
    return jnp.concatenate(parts, axis=0) <= qpos


def fwd_kernel(npieces, slots, first, last, *refs):
    starts_ref, q_ref, qpos_ref = refs[:3]
    k_refs = refs[3 : 3 + npieces]
    v_refs = refs[3 + npieces : 3 + 2 * npieces]
    rest = refs[3 + 2 * npieces :]
    if not first:
        m_in, l_in, a_in = rest[:3]
        rest = rest[3:]
    rows = k_refs[0].shape[0] // slots
    c2 = LOG2E / math.sqrt(HD)
    q = q_ref[...]
    qpos = qpos_ref[...]
    scores = []
    top = None if first else m_in[0]
    for i in range(npieces):
        s = contract_cols(k_refs[i][...], q)
        s = jnp.where(key_mask(starts_ref, i, slots, rows, qpos), s, big_negative)
        scores.append(s)
        t = jnp.max(s, axis=0, keepdims=True)
        top = t if top is None else jnp.maximum(top, t)
    total = None
    acc = None
    for i in range(npieces):
        p = jnp.exp2((scores[i] - top) * c2)
        t = jnp.sum(p, axis=0, keepdims=True)
        a = contract_rows(v_refs[i][...], p.astype(BF))
        total = t if total is None else total + t
        acc = a if acc is None else acc + a
    if not first:
        alpha = jnp.exp2((m_in[0] - top) * c2)
        total = total + l_in[0] * alpha
        acc = acc + a_in[...] * alpha
    if last:
        mix_ref, mixb_ref, log_ref = rest
        mix = (acc / total).T
        mix_ref[...] = mix
        mixb_ref[...] = mix.astype(BF)
        log_ref[0] = top * c2 + jnp.log2(total)
    else:
        m_out, l_out, a_out = rest
        m_out[0] = top
        l_out[0] = total
        a_out[...] = acc


def attend(starts, q, qpos, kv, carry, heads, slots, last):
    span = q.shape[0]
    first = carry is None
    np_ = len(kv)
    pr = kv[0].shape[0]
    row = pl.BlockSpec((1, 1, span), lambda h: (h, 0, 0))
    accs = pl.BlockSpec((HD, span), lambda h: (h, 0))
    specs = [
        pl.BlockSpec(memory_space=pltpu.SMEM),
        pl.BlockSpec((span, HD), lambda h: (0, h)),
        pl.BlockSpec((1, span), lambda h: (0, 0)),
    ]
    specs += [pl.BlockSpec((pr, HD), lambda h: (0, h))] * np_
    specs += [pl.BlockSpec((pr, HD), lambda h: (0, heads + h))] * np_
    args = [starts, q, qpos, *kv, *kv]
    if not first:
        specs += [row, row, accs]
        args += list(carry)
    rshape = jax.ShapeDtypeStruct((heads, 1, span), F32)
    if last:
        mix = pl.BlockSpec((span, HD), lambda h: (0, h))
        outs = [mix, mix, row]
        shapes = [
            jax.ShapeDtypeStruct((span, heads * HD), F32),
            jax.ShapeDtypeStruct((span, heads * HD), BF),
            rshape,
        ]
    else:
        outs = [row, row, accs]
        shapes = [rshape, rshape, jax.ShapeDtypeStruct((heads * HD, span), F32)]
    keys = np_ * pr
    return pl.pallas_call(
        functools.partial(fwd_kernel, np_, slots, first, last),
        grid=(heads,),
        in_specs=specs,
        out_specs=outs,
        out_shape=shapes,
        cost_estimate=pl.CostEstimate(
            flops=8 * span * keys * HD * heads,
            bytes_accessed=4 * keys * heads * HD,
            transcendentals=span * keys * heads,
        ),
    )(*args)


def bwd_kernel(npieces, slots, heads, first, *refs):
    starts_ref, q_ref, do_ref, mix_ref, log_ref, qpos_ref = refs[:6]
    k_refs = refs[6 : 6 + npieces]
    v_refs = refs[6 + npieces : 6 + 2 * npieces]
    rest = refs[6 + 2 * npieces :]
    if not first:
        dq_in = rest[0]
        rest = rest[1:]
    dq_ref, out_refs = rest[0], rest[1:]
    h = pl.program_id(0)
    rows = k_refs[0].shape[0] // slots
    scale = 1.0 / math.sqrt(HD)
    c2 = LOG2E * scale
    q = q_ref[...]
    do = do_ref[...]
    delta = jnp.sum((do.astype(F32) * mix_ref[...]).T, axis=0, keepdims=True)
    log2 = log_ref[0]
    qpos = qpos_ref[...]
    dq = None
    for i in range(npieces):
        k = k_refs[i][...]
        s = contract_cols(k, q) * c2 - log2
        s = jnp.where(key_mask(starts_ref, i, slots, rows, qpos), s, big_negative)
        p = jnp.exp2(s)
        dp = contract_cols(v_refs[i][...], do)
        ds = (p * (dp - delta)).astype(BF)
        t = contract_rows(k, ds)
        dq = t if dq is None else dq + t
        kc = pl.ds(pl.multiple_of(h * HD, HD), HD)
        vc = pl.ds(pl.multiple_of((heads + h) * HD, HD), HD)
        out_refs[i][:, kc] = (mm(ds, q) * scale).astype(BF)
        out_refs[i][:, vc] = mm(p.astype(BF), do).astype(BF)
    dq = dq * scale
    dq_ref[...] = dq if first else dq + dq_in[...]


def attend_back(starts, q, do, mix, log, qpos, kv, dq, heads, slots):
    span = q.shape[0]
    first = dq is None
    np_ = len(kv)
    pr = kv[0].shape[0]
    head = pl.BlockSpec((span, HD), lambda h: (0, h))
    accs = pl.BlockSpec((HD, span), lambda h: (h, 0))
    specs = [
        pl.BlockSpec(memory_space=pltpu.SMEM),
        head,
        head,
        head,
        pl.BlockSpec((1, 1, span), lambda h: (h, 0, 0)),
        pl.BlockSpec((1, span), lambda h: (0, 0)),
    ]
    specs += [pl.BlockSpec((pr, HD), lambda h: (0, h))] * np_
    specs += [pl.BlockSpec((pr, HD), lambda h: (0, heads + h))] * np_
    args = [starts, q, do, mix, log, qpos, *kv, *kv]
    if not first:
        specs.append(accs)
        args.append(dq)
    keys = np_ * pr
    return pl.pallas_call(
        functools.partial(bwd_kernel, np_, slots, heads, first),
        grid=(heads,),
        in_specs=specs,
        out_specs=[accs] + [pl.BlockSpec((pr, 2 * heads * HD), lambda h: (0, 0))] * np_,
        out_shape=[jax.ShapeDtypeStruct((heads * HD, span), F32)]
        + [jax.ShapeDtypeStruct((pr, 2 * heads * HD), BF)] * np_,
        cost_estimate=pl.CostEstimate(
            flops=20 * span * keys * HD * heads,
            bytes_accessed=8 * keys * heads * HD,
            transcendentals=span * keys * heads,
        ),
    )(*args)


def turn_back(x, cosine, sine):
    return x * cosine - pltpu.roll(x, HD // 2, 1) * sine


def unrotate_kernel(n, heads, transposed, *refs):
    nd = 1 if transposed else 2
    d_refs = refs[:nd]
    raw_refs = refs[nd : nd + n]
    r_ref, g_ref, cos_ref, sin_ref, w_ref, inner_ref, gain_ref = refs[nd + n :]
    rows = raw_refs[0].shape[0]
    half = n // 2
    for h in range(heads):
        c = slice(h * HD, (h + 1) * HD)
        gain_sum = None
        whole = d_refs[0][c, :].T if transposed else None
        for s in range(n):
            r = slice(s * rows, (s + 1) * rows)
            if transposed:
                d = whole[r, :]
            else:
                o = slice((s % half) * rows, (s % half + 1) * rows)
                d = d_refs[0 if s < half else 1][o, c].astype(F32)
            grad = turn_back(d, cos_ref[r, :], sin_ref[r, :])
            raw = raw_refs[s][:, c]
            weighted = grad * g_ref[:, c]
            w_ref[r, c] = weighted
            t = jnp.sum(weighted * raw, axis=1, keepdims=True)
            inner_ref[r, :] = t if h == 0 else inner_ref[r, :] + t
            u = jnp.sum(grad * raw * r_ref[r, :], axis=0, keepdims=True)
            gain_sum = u if gain_sum is None else gain_sum + u
        gain_ref[:, c] = gain_sum


def unrotate(d, raw, rms, gain, cosine, sine, heads, transposed):
    n = len(raw)
    span = n * raw[0].shape[0]
    units = heads * HD
    return pl.pallas_call(
        functools.partial(unrotate_kernel, n, heads, transposed),
        in_specs=[vmem()] * (len(d) + n + 4),
        out_specs=[vmem()] * 3,
        out_shape=[
            jax.ShapeDtypeStruct((span, units), F32),
            jax.ShapeDtypeStruct((span, 1), F32),
            jax.ShapeDtypeStruct((1, units), F32),
        ],
    )(*d, *raw, rms, gain, cosine, sine)


def norm_back(raw, rms_inv, gain, grad_out):
    weighted = gain * grad_out
    inner = jnp.sum(weighted * raw, axis=1, keepdims=True)
    width = raw.shape[1]
    return (
        rms_inv[:, None] * weighted - raw * (rms_inv * rms_inv * rms_inv)[:, None] * inner / width
    )


def local(
    nc,
    nf,
    block_input,
    positions,
    query_weight,
    key_weight,
    value_weight,
    output_weight,
    query_gain,
    key_gain,
    attn_gain,
    mlp_gain,
    gate_weight,
    up_weight,
    down_weight,
    cotangent,
):
    rows, width = block_input.shape
    span = rows * nf
    units = query_weight.shape[1]
    heads = units // HD
    half = nf // 2
    me_c = lax.axis_index("ctx")
    me_f = lax.axis_index("fsdp")
    unit_start = me_f * units

    x_slots = ring_gather(block_input, nf)

    begin = positions[:1]
    begins = jnp.concatenate([begin] + [shift(begin, nf, t) for t in range(1, nf)])[None, :]
    b = 1
    while b < nc:
        begins = jnp.concatenate([begins, swap(begins, nc, b)])
        b *= 2
    row_pos = (begins[0][:, None] + jnp.arange(rows)[None, :]).reshape(span)
    freqs = jnp.exp(-math.log(rope_base) * 2.0 * jnp.arange(HD // 2).astype(F32) / HD)
    angles = row_pos.astype(F32)[:, None] * freqs[None, :]
    cosine, sine = jnp.cos(angles), jnp.sin(angles)
    cosine = jnp.concatenate([cosine, cosine], axis=1)
    sine = jnp.concatenate([-sine, sine], axis=1)
    qpos = row_pos[None, :]

    q_raw = [mm(x, query_weight) for x in x_slots]
    k_raw = [mm(x, key_weight) for x in x_slots]
    v_raw = [mm(x, value_weight) for x in x_slots]
    squares = jnp.stack(
        [
            jnp.stack([jnp.sum(q * q, axis=1), jnp.sum(k * k, axis=1)])
            for q, k in zip(q_raw, k_raw)
        ]
    )
    squares = slot_sum(squares, nf)
    query_rms = lax.rsqrt(squares[:, 0].reshape(span, 1) / width + norm_eps)
    key_rms = lax.rsqrt(squares[:, 1].reshape(span, 1) / width + norm_eps)
    query_scale = lax.dynamic_slice_in_dim(query_gain, unit_start, units)[None, :]
    key_scale = lax.dynamic_slice_in_dim(key_gain, unit_start, units)[None, :]

    query_rot, kv_a, kv_b = pl.pallas_call(
        functools.partial(prep_kernel, nf, heads),
        in_specs=[vmem()] * (3 * nf + 6),
        out_specs=[vmem()] * 3,
        out_shape=[jax.ShapeDtypeStruct((span, units), BF)]
        + [jax.ShapeDtypeStruct((span // 2, 2 * units), BF)] * 2,
    )(*q_raw, *k_raw, *v_raw, query_rms, key_rms, query_scale, key_scale, cosine, sine)

    orders = bit_orders(nc)
    groups = group_order(nc)
    pieces = [{0: kv_a}, {0: kv_b}]

    def fetch(i, m, token):
        if m not in pieces[i]:
            src, bit = came_from(m, orders[i])
            have = fetch(i, src, token)
            if token is not None:
                have = gate(have, token)
            pieces[i][m] = swap(have, nc, bit)
        return pieces[i][m]

    def group_inputs(group):
        kv = [pieces[0][m] for m in group] + [pieces[1][m] for m in group]
        starts = jnp.concatenate(
            [begins[m, :half] for m in group] + [begins[m, half:] for m in group]
        )
        return starts, kv

    carry = None
    tokens = []
    for group in groups:
        for m in group:
            for i in range(2):
                far = distance(m)
                if far < 2:
                    fetch(i, m, None)
                else:
                    fetch(i, m, tokens[1] if m & 1 else tokens[0])
        starts, kv = group_inputs(group)
        carry = attend(
            starts, query_rot, qpos, kv, carry, heads, half, group is groups[-1]
        )
        tokens.append(carry[0])
    mixture, mixture_b, log_total = carry

    def rows_of(x, s):
        return x[s * rows : (s + 1) * rows]

    attn_out = ring_scatter(lambda s: mm(rows_of(mixture_b, s), output_weight), nf)
    attn_rms = lax.rsqrt(jnp.mean(attn_out * attn_out, axis=1) + norm_eps)
    hidden_state = block_input.astype(F32) + attn_out * attn_rms[:, None] * attn_gain[None, :]
    state_slots = ring_gather(hidden_state.astype(BF), nf)
    gate_pre = [mm(x, gate_weight) for x in state_slots]
    up_pre = [mm(x, up_weight) for x in state_slots]
    activated = [(jax.nn.silu(g) * u).astype(BF) for g, u in zip(gate_pre, up_pre)]
    mlp_out = ring_scatter(lambda s: mm(activated[s], down_weight), nf)
    mlp_rms = lax.rsqrt(jnp.mean(mlp_out * mlp_out, axis=1) + norm_eps)
    block_output = (hidden_state + mlp_out * mlp_rms[:, None] * mlp_gain[None, :]).astype(BF)
    upstream = cotangent.astype(F32)
    mlp_gain_part = jnp.sum(upstream * mlp_out * mlp_rms[:, None], axis=0)
    mlp_grad_b = norm_back(mlp_out, mlp_rms, mlp_gain[None, :], upstream).astype(BF)
    grad_slots = ring_gather(mlp_grad_b, nf)

    gate_grads, up_grads = [], []
    for s in range(nf):
        activ_grad = contract_cols(grad_slots[s], down_weight)
        sg = jax.nn.sigmoid(gate_pre[s])
        gate_grads.append(
            (activ_grad * up_pre[s] * sg * (1.0 + gate_pre[s] * (1.0 - sg))).astype(BF)
        )
        up_grads.append((activ_grad * gate_pre[s] * sg).astype(BF))
    def ctx_scatter(x):
        return lax.psum_scatter(x, "ctx", scatter_dimension=0, tiled=True)

    down_part = contract_rows(jnp.concatenate(grad_slots), jnp.concatenate(activated)).astype(BF)
    gate_up_part = contract_rows(
        jnp.concatenate(state_slots),
        jnp.concatenate([jnp.concatenate(gate_grads), jnp.concatenate(up_grads)], axis=1),
    ).astype(BF)
    state_grad = upstream + ring_scatter(
        lambda s: contract_cols(gate_grads[s], gate_weight)
        + contract_cols(up_grads[s], up_weight),
        nf,
        (down_part,),
    )
    down_sum = ctx_scatter(down_part)
    gate_up_sum = ctx_scatter(gate_up_part)

    attn_gain_part = jnp.sum(state_grad * attn_out * attn_rms[:, None], axis=0)
    attn_grad_b = norm_back(attn_out, attn_rms, attn_gain[None, :], state_grad).astype(BF)
    proj_slots = ring_gather(attn_grad_b, nf, (gate_up_part,))
    mixture_grad_b = jnp.concatenate(
        [contract_cols(x, output_weight).astype(BF) for x in proj_slots]
    )

    dq = None
    sums = [{}, {}]

    def send(i, m):
        into, bit = came_from(m, orders[i])
        got = swap(sums[i].pop(m), nc, bit)
        sums[i][into] = (sums[i][into].astype(F32) + got.astype(F32)).astype(BF)
        return sums[i][into]

    waits = []
    for gi, group in enumerate(groups[::-1]):
        starts, kv = group_inputs(group)
        if gi >= 2 and waits:
            dq = gate(dq, *waits[gi - 2])
        dq, *out = attend_back(
            starts, query_rot, mixture_grad_b, mixture, log_total, qpos, kv, dq, heads, half
        )
        for m, a, b in zip(group, out[: len(group)], out[len(group) :]):
            sums[0][m], sums[1][m] = a, b
        waits.append([send(i, m) for i in range(2) for m in group if m & 1])
    for far in range(max(distance(m) for m in range(nc)), 0, -1):
        for i in range(2):
            for m in [m for m in sums[i] if distance(m) == far]:
                send(i, m)
    own_a, own_b = sums[0][0], sums[1][0]

    def unit_full(x):
        return lax.dynamic_update_slice_in_dim(jnp.zeros((width,), F32), x, unit_start, 0)

    def norm_grads(weighted, inner, raw, rms):
        cube = rms * rms * rms
        return [
            (
                rows_of(rms, s) * rows_of(weighted, s)
                - raw[s] * rows_of(cube, s) * inner[s][:, None] / width
            ).astype(BF)
            for s in range(nf)
        ]

    query_weighted, query_inner, query_gain_part = unrotate(
        [dq], q_raw, query_rms, query_scale, cosine, sine, heads, True
    )
    query_inner = slot_sum(query_inner.reshape(nf, rows), nf)
    early_gains = flat_sum(
        jnp.stack([unit_full(query_gain_part[0]), attn_gain_part, mlp_gain_part]), nf
    )
    query_grads = norm_grads(query_weighted, query_inner, q_raw, query_rms)

    x_rows = jnp.concatenate(x_slots)
    qo_part = jnp.concatenate(
        [
            contract_rows(x_rows, jnp.concatenate(query_grads)).astype(BF),
            contract_rows(jnp.concatenate(proj_slots), mixture_b).astype(BF),
        ],
        axis=1,
    )
    qo_part, down_sum = lax.optimization_barrier((qo_part, down_sum))
    qo_grad = ctx_scatter(qo_part).astype(F32)
    query_grad, output_grad = qo_grad[:, :units], qo_grad[:, units:].T

    key_weighted, key_inner, key_gain_part = unrotate(
        [own_a, own_b], k_raw, key_rms, key_scale, cosine, sine, heads, False
    )
    key_inner = slot_sum(key_inner.reshape(nf, rows), nf)
    key_gain_sum = flat_sum(unit_full(key_gain_part[0])[None, :], nf)
    key_grads = norm_grads(key_weighted, key_inner, k_raw, key_rms)
    own = jnp.concatenate([own_a[:, units:], own_b[:, units:]])
    value_grads = [rows_of(own, s) for s in range(nf)]

    input_grad = state_grad + ring_scatter(
        lambda s: contract_cols(query_grads[s], query_weight)
        + contract_cols(key_grads[s], key_weight)
        + contract_cols(value_grads[s], value_weight),
        nf,
    )
    kv_rows = jnp.concatenate([jnp.concatenate(key_grads), own], axis=1)
    gains = jnp.concatenate([early_gains, key_gain_sum]).T
    gains = jnp.pad(gains, ((0, 0), (0, 128 - gains.shape[1]))).astype(BF)
    kv_part = jnp.concatenate([contract_rows(x_rows, kv_rows).astype(BF), gains], axis=1)
    kv_part, gate_up_sum = lax.optimization_barrier((kv_part, gate_up_sum))
    kv_grad = ctx_scatter(kv_part).astype(F32)
    down_grad = down_sum.astype(F32).T
    ff = gate_weight.shape[1]
    gate_up = gate_up_sum.astype(F32)
    gate_grad, up_grad = gate_up[:, :ff], gate_up[:, ff:]
    key_grad, value_grad = kv_grad[:, :units], kv_grad[:, units : 2 * units]
    gains_own = kv_grad[:, 2 * units : 2 * units + 4].T
    return (
        block_output,
        input_grad,
        query_grad,
        key_grad,
        value_grad,
        output_grad,
        gains_own[0],
        gains_own[3],
        gains_own[1],
        gains_own[2],
        gate_grad,
        up_grad,
        down_grad,
    )


def solution(mesh):
    return jax.shard_map(
        functools.partial(local, mesh.shape["ctx"], mesh.shape["fsdp"]),
        mesh=mesh,
        in_specs=(
            P(("ctx", "fsdp"), None),
            P(("ctx", "fsdp")),
            P(None, "fsdp"),
            P(None, "fsdp"),
            P(None, "fsdp"),
            P("fsdp", None),
            P(),
            P(),
            P(),
            P(),
            P(None, "fsdp"),
            P(None, "fsdp"),
            P("fsdp", None),
            P(("ctx", "fsdp"), None),
        ),
        out_specs=(
            P(("ctx", "fsdp"), None),
            P(("ctx", "fsdp"), None),
            P("ctx", "fsdp"),
            P("ctx", "fsdp"),
            P("ctx", "fsdp"),
            P("fsdp", "ctx"),
            P("ctx"),
            P("ctx"),
            P("ctx"),
            P("ctx"),
            P("ctx", "fsdp"),
            P("ctx", "fsdp"),
            P("fsdp", "ctx"),
        ),
        check_vma=False,
    )
```

```python
import functools
import math

import jax
import jax.numpy as jnp
from jax import lax
from jax.experimental import pallas as pl
from jax.experimental.pallas import tpu as pltpu
from jax.sharding import PartitionSpec as P

HD = 128
norm_eps = 1e-06
rope_base = 500000.0
big_negative = -1e30
LOG2E = math.log2(math.e)
BF = jnp.bfloat16
F32 = jnp.float32


def mm(left, right):
    return jnp.dot(left, right, preferred_element_type=F32)


def contract_rows(left, right):
    return lax.dot_general(left, right, (((0,), (0,)), ((), ())), preferred_element_type=F32)


def contract_cols(left, right):
    return lax.dot_general(left, right, (((1,), (1,)), ((), ())), preferred_element_type=F32)


def gate(x, *tokens):
    return lax.optimization_barrier((x, *tokens))[0]


def shift(x, n, by):
    return lax.ppermute(x, "fsdp", [(i, (i + by) % n) for i in range(n)])


def ring_gather(x, n, under={}):
    slots = [x]
    for i in range(n - 1):
        got = shift(slots[-1], n, 1)
        slots.append(gate(got, *under[i]) if i in under else got)
    return slots


def ring_scatter(part, n, under=(), started=None):
    if n == 1:
        return part(0)
    acc = part(1).astype(BF)
    if started is not None:
        started.append(acc)
    for s in range(2, n):
        acc = (shift(acc, n, 1).astype(F32) + part(s)).astype(BF)
    return gate(shift(acc, n, 1), *under).astype(F32) + part(0)


def slot_sum(x, n, flat=None):
    total, flat_total = x, flat
    cut = x.shape[-1]
    both = x if flat is None else jnp.concatenate([x, flat], axis=-1)
    for t in range(1, n):
        got = shift(both, n, t)
        total = total + jnp.roll(got[..., :cut], t, axis=0)
        if flat is not None:
            flat_total = flat_total + got[..., cut:]
    return total if flat is None else (total, flat_total)


def swap(x, n, bit):
    return lax.ppermute(x, "ctx", [(i, i ^ bit) for i in range(n)])


def bit_orders(n):
    bits = []
    b = 2
    while b < n:
        bits.append(b)
        b *= 2
    return bits, bits[::-1]


def halving(part, me, n, order, under=()):
    seq = ([1] if n > 1 else []) + list(order[::-1])
    block = part.shape[0] // n
    levels = len(seq)
    masks = [
        sum(seq[k] for k in range(levels) if t >> (levels - 1 - k) & 1) for t in range(n)
    ]

    def blocks(ms):
        return jnp.concatenate(
            [lax.dynamic_slice_in_dim(part, (me ^ m) * block, block) for m in ms]
        )

    keep, away = blocks(masks[: n // 2]), blocks(masks[n // 2 :])
    for k, bit in enumerate(seq):
        got = swap(away.astype(BF), n, bit)
        if k == levels - 1 and under:
            got = gate(got, *under)
        total = keep.astype(F32) + got.astype(F32)
        rest = total.shape[0] // 2
        if k < levels - 1:
            total = total.astype(BF)
            keep, away = total[:rest], total[rest:]
    return total


def distance(m):
    return bin(m >> 1).count("1")


def group_order(n):
    pairs = [(m, m + 1) if n > 1 else (m,) for m in range(0, n, 2)]
    return sorted(pairs, key=lambda g: (distance(g[0]), g[0]))


def came_from(m, order):
    if m & 1:
        return m ^ 1, 1
    bit = [b for b in order if m & b][-1]
    return m ^ bit, bit


def vmem(*_):
    return pl.BlockSpec(memory_space=pltpu.VMEM)


def prep_kernel(n, heads, *refs):
    q_refs, k_refs, v_refs = refs[:n], refs[n : 2 * n], refs[2 * n : 3 * n]
    qr_ref, kr_ref, qg_ref, kg_ref, cos_ref, sin_ref = refs[3 * n : 3 * n + 6]
    qo_ref, kva_ref, kvb_ref = refs[3 * n + 6 :]
    rows = q_refs[0].shape[0]
    half = n // 2
    for s in range(n):
        r = slice(s * rows, (s + 1) * rows)
        cosine, sine = cos_ref[r, :], sin_ref[r, :]
        out = kva_ref if s < half else kvb_ref
        o = slice((s % half) * rows, (s % half + 1) * rows)
        for h in range(heads):
            c = slice(h * HD, (h + 1) * HD)
            x = q_refs[s][:, c] * qr_ref[r, :] * qg_ref[:, c]
            qo_ref[r, c] = (x * cosine + pltpu.roll(x, HD // 2, 1) * sine).astype(BF)
            y = k_refs[s][:, c] * kr_ref[r, :] * kg_ref[:, c]
            out[o, c] = (y * cosine + pltpu.roll(y, HD // 2, 1) * sine).astype(BF)
            out[o, heads * HD + h * HD : heads * HD + (h + 1) * HD] = v_refs[s][:, c].astype(BF)


def key_mask(starts_ref, piece, slots, rows, qpos):
    parts = []
    for j in range(slots):
        row = lax.broadcasted_iota(jnp.int32, (rows, 1), 0)
        parts.append(row + starts_ref[piece * slots + j])
    return jnp.concatenate(parts, axis=0) <= qpos


def fwd_kernel(npieces, slots, first, last, *refs):
    starts_ref, q_ref, qpos_ref = refs[:3]
    k_refs = refs[3 : 3 + npieces]
    v_refs = refs[3 + npieces : 3 + 2 * npieces]
    rest = refs[3 + 2 * npieces :]
    if not first:
        m_in, l_in, a_in = rest[:3]
        rest = rest[3:]
    rows = k_refs[0].shape[0] // slots
    c2 = LOG2E / math.sqrt(HD)
    q = q_ref[...]
    qpos = qpos_ref[...]
    scores = []
    top = None if first else m_in[0]
    for i in range(npieces):
        s = contract_cols(k_refs[i][...], q)
        s = jnp.where(key_mask(starts_ref, i, slots, rows, qpos), s, big_negative)
        scores.append(s)
        t = jnp.max(s, axis=0, keepdims=True)
        top = t if top is None else jnp.maximum(top, t)
    total = None
    acc = None
    for i in range(npieces):
        p = jnp.exp2((scores[i] - top) * c2)
        t = jnp.sum(p, axis=0, keepdims=True)
        a = contract_rows(v_refs[i][...], p.astype(BF))
        total = t if total is None else total + t
        acc = a if acc is None else acc + a
    if not first:
        alpha = jnp.exp2((m_in[0] - top) * c2)
        total = total + l_in[0] * alpha
        acc = acc + a_in[...] * alpha
    if last:
        mix_ref, mixb_ref, log_ref = rest
        mix = (acc / total).T
        mix_ref[...] = mix
        mixb_ref[...] = mix.astype(BF)
        log_ref[0] = top * c2 + jnp.log2(total)
    else:
        m_out, l_out, a_out = rest
        m_out[0] = top
        l_out[0] = total
        a_out[...] = acc


def attend(starts, q, qpos, kv, carry, heads, slots, last):
    span = q.shape[0]
    first = carry is None
    np_ = len(kv)
    pr = kv[0].shape[0]
    row = pl.BlockSpec((1, 1, span), lambda h: (h, 0, 0))
    accs = pl.BlockSpec((HD, span), lambda h: (h, 0))
    specs = [
        pl.BlockSpec(memory_space=pltpu.SMEM),
        pl.BlockSpec((span, HD), lambda h: (0, h)),
        pl.BlockSpec((1, span), lambda h: (0, 0)),
    ]
    specs += [pl.BlockSpec((pr, HD), lambda h: (0, h))] * np_
    specs += [pl.BlockSpec((pr, HD), lambda h: (0, heads + h))] * np_
    args = [starts, q, qpos, *kv, *kv]
    if not first:
        specs += [row, row, accs]
        args += list(carry)
    rshape = jax.ShapeDtypeStruct((heads, 1, span), F32)
    if last:
        mix = pl.BlockSpec((span, HD), lambda h: (0, h))
        outs = [mix, mix, row]
        shapes = [
            jax.ShapeDtypeStruct((span, heads * HD), F32),
            jax.ShapeDtypeStruct((span, heads * HD), BF),
            rshape,
        ]
    else:
        outs = [row, row, accs]
        shapes = [rshape, rshape, jax.ShapeDtypeStruct((heads * HD, span), F32)]
    keys = np_ * pr
    return pl.pallas_call(
        functools.partial(fwd_kernel, np_, slots, first, last),
        grid=(heads,),
        in_specs=specs,
        out_specs=outs,
        out_shape=shapes,
        cost_estimate=pl.CostEstimate(
            flops=8 * span * keys * HD * heads,
            bytes_accessed=4 * keys * heads * HD,
            transcendentals=span * keys * heads,
        ),
    )(*args)


def bwd_kernel(npieces, slots, heads, first, *refs):
    starts_ref, q_ref, do_ref, mix_ref, log_ref, qpos_ref = refs[:6]
    k_refs = refs[6 : 6 + npieces]
    v_refs = refs[6 + npieces : 6 + 2 * npieces]
    rest = refs[6 + 2 * npieces :]
    if not first:
        dq_in = rest[0]
        rest = rest[1:]
    dq_ref, out_refs = rest[0], rest[1:]
    h = pl.program_id(0)
    rows = k_refs[0].shape[0] // slots
    scale = 1.0 / math.sqrt(HD)
    c2 = LOG2E * scale
    q = q_ref[...]
    do = do_ref[...]
    delta = jnp.sum((do.astype(F32) * mix_ref[...]).T, axis=0, keepdims=True)
    log2 = log_ref[0]
    qpos = qpos_ref[...]
    dq = None
    for i in range(npieces):
        k = k_refs[i][...]
        s = contract_cols(k, q) * c2 - log2
        s = jnp.where(key_mask(starts_ref, i, slots, rows, qpos), s, big_negative)
        p = jnp.exp2(s)
        dp = contract_cols(v_refs[i][...], do)
        ds = (p * (dp - delta)).astype(BF)
        t = contract_rows(k, ds)
        dq = t if dq is None else dq + t
        kc = pl.ds(pl.multiple_of(h * HD, HD), HD)
        vc = pl.ds(pl.multiple_of((heads + h) * HD, HD), HD)
        out_refs[i][:, kc] = (mm(ds, q) * scale).astype(BF)
        out_refs[i][:, vc] = mm(p.astype(BF), do).astype(BF)
    dq = dq * scale
    dq_ref[...] = dq if first else dq + dq_in[...]


def attend_back(starts, q, do, mix, log, qpos, kv, dq, heads, slots):
    span = q.shape[0]
    first = dq is None
    np_ = len(kv)
    pr = kv[0].shape[0]
    head = pl.BlockSpec((span, HD), lambda h: (0, h))
    accs = pl.BlockSpec((HD, span), lambda h: (h, 0))
    specs = [
        pl.BlockSpec(memory_space=pltpu.SMEM),
        head,
        head,
        head,
        pl.BlockSpec((1, 1, span), lambda h: (h, 0, 0)),
        pl.BlockSpec((1, span), lambda h: (0, 0)),
    ]
    specs += [pl.BlockSpec((pr, HD), lambda h: (0, h))] * np_
    specs += [pl.BlockSpec((pr, HD), lambda h: (0, heads + h))] * np_
    args = [starts, q, do, mix, log, qpos, *kv, *kv]
    if not first:
        specs.append(accs)
        args.append(dq)
    keys = np_ * pr
    return pl.pallas_call(
        functools.partial(bwd_kernel, np_, slots, heads, first),
        grid=(heads,),
        in_specs=specs,
        out_specs=[accs] + [pl.BlockSpec((pr, 2 * heads * HD), lambda h: (0, 0))] * np_,
        out_shape=[jax.ShapeDtypeStruct((heads * HD, span), F32)]
        + [jax.ShapeDtypeStruct((pr, 2 * heads * HD), BF)] * np_,
        cost_estimate=pl.CostEstimate(
            flops=20 * span * keys * HD * heads,
            bytes_accessed=8 * keys * heads * HD,
            transcendentals=span * keys * heads,
        ),
    )(*args)


def turn_back(x, cosine, sine):
    return x * cosine - pltpu.roll(x, HD // 2, 1) * sine


def unrotate_kernel(n, heads, transposed, *refs):
    nd = 1 if transposed else 2
    d_refs = refs[:nd]
    raw_refs = refs[nd : nd + n]
    r_ref, g_ref, cos_ref, sin_ref, w_ref, inner_ref, gain_ref = refs[nd + n :]
    rows = raw_refs[0].shape[0]
    half = n // 2
    for h in range(heads):
        c = slice(h * HD, (h + 1) * HD)
        gain_sum = None
        whole = d_refs[0][c, :].T if transposed else None
        for s in range(n):
            r = slice(s * rows, (s + 1) * rows)
            if transposed:
                d = whole[r, :]
            else:
                o = slice((s % half) * rows, (s % half + 1) * rows)
                d = d_refs[0 if s < half else 1][o, c].astype(F32)
            grad = turn_back(d, cos_ref[r, :], sin_ref[r, :])
            raw = raw_refs[s][:, c]
            weighted = grad * g_ref[:, c]
            w_ref[r, c] = weighted
            t = jnp.sum(weighted * raw, axis=1, keepdims=True)
            inner_ref[r, :] = t if h == 0 else inner_ref[r, :] + t
            u = jnp.sum(grad * raw * r_ref[r, :], axis=0, keepdims=True)
            gain_sum = u if gain_sum is None else gain_sum + u
        gain_ref[:, c] = gain_sum


def unrotate(d, raw, rms, gain, cosine, sine, heads, transposed):
    n = len(raw)
    span = n * raw[0].shape[0]
    units = heads * HD
    return pl.pallas_call(
        functools.partial(unrotate_kernel, n, heads, transposed),
        in_specs=[vmem()] * (len(d) + n + 4),
        out_specs=[vmem()] * 3,
        out_shape=[
            jax.ShapeDtypeStruct((span, units), F32),
            jax.ShapeDtypeStruct((span, 1), F32),
            jax.ShapeDtypeStruct((1, units), F32),
        ],
    )(*d, *raw, rms, gain, cosine, sine)


def norm_back(raw, rms_inv, gain, grad_out):
    weighted = gain * grad_out
    inner = jnp.sum(weighted * raw, axis=1, keepdims=True)
    width = raw.shape[1]
    return (
        rms_inv[:, None] * weighted - raw * (rms_inv * rms_inv * rms_inv)[:, None] * inner / width
    )


def local(
    nc,
    nf,
    block_input,
    positions,
    query_weight,
    key_weight,
    value_weight,
    output_weight,
    query_gain,
    key_gain,
    attn_gain,
    mlp_gain,
    gate_weight,
    up_weight,
    down_weight,
    cotangent,
):
    rows, width = block_input.shape
    span = rows * nf
    units = query_weight.shape[1]
    heads = units // HD
    half = nf // 2
    me_c = lax.axis_index("ctx")
    me_f = lax.axis_index("fsdp")
    unit_start = me_f * units

    first_hop = shift(block_input, nf, 1)
    begin = gate(positions[:1], first_hop)
    begins = jnp.concatenate([begin] + [shift(begin, nf, t) for t in range(1, nf)])[None, :]
    b = 1
    while b < nc:
        begins = jnp.concatenate([begins, swap(begins, nc, b)])
        b *= 2
    x_slots = [block_input, first_hop]
    for s in range(2, nf):
        got = shift(x_slots[-1], nf, 1)
        x_slots.append(gate(got, begins) if s == nf - 1 else got)

    row_pos = (begins[0][:, None] + jnp.arange(rows)[None, :]).reshape(span)
    freqs = jnp.exp(-math.log(rope_base) * 2.0 * jnp.arange(HD // 2).astype(F32) / HD)
    angles = row_pos.astype(F32)[:, None] * freqs[None, :]
    cosine, sine = jnp.cos(angles), jnp.sin(angles)
    cosine = jnp.concatenate([cosine, cosine], axis=1)
    sine = jnp.concatenate([-sine, sine], axis=1)
    qpos = row_pos[None, :]

    q_raw = [mm(x, query_weight) for x in x_slots]
    k_raw = [mm(x, key_weight) for x in x_slots]
    v_raw = [mm(x, value_weight) for x in x_slots]
    squares = jnp.stack(
        [
            jnp.stack([jnp.sum(q * q, axis=1), jnp.sum(k * k, axis=1)])
            for q, k in zip(q_raw, k_raw)
        ]
    )
    squares = slot_sum(squares, nf)
    query_rms = lax.rsqrt(squares[:, 0].reshape(span, 1) / width + norm_eps)
    key_rms = lax.rsqrt(squares[:, 1].reshape(span, 1) / width + norm_eps)
    query_scale = lax.dynamic_slice_in_dim(query_gain, unit_start, units)[None, :]
    key_scale = lax.dynamic_slice_in_dim(key_gain, unit_start, units)[None, :]

    query_rot, kv_a, kv_b = pl.pallas_call(
        functools.partial(prep_kernel, nf, heads),
        in_specs=[vmem()] * (3 * nf + 6),
        out_specs=[vmem()] * 3,
        out_shape=[jax.ShapeDtypeStruct((span, units), BF)]
        + [jax.ShapeDtypeStruct((span // 2, 2 * units), BF)] * 2,
    )(*q_raw, *k_raw, *v_raw, query_rms, key_rms, query_scale, key_scale, cosine, sine)

    orders = bit_orders(nc)
    groups = group_order(nc)
    pieces = [{0: kv_a}, {0: kv_b}]

    def fetch(i, m, token):
        if m not in pieces[i]:
            src, bit = came_from(m, orders[i])
            have = fetch(i, src, token)
            if token is not None:
                have = gate(have, token)
            pieces[i][m] = swap(have, nc, bit)
        return pieces[i][m]

    def group_inputs(group):
        kv = [pieces[0][m] for m in group] + [pieces[1][m] for m in group]
        starts = jnp.concatenate(
            [begins[m, :half] for m in group] + [begins[m, half:] for m in group]
        )
        return starts, kv

    carry = None
    tokens = []
    for group in groups:
        for m in group:
            for i in range(2):
                far = distance(m)
                if far < 2:
                    fetch(i, m, None)
                else:
                    fetch(i, m, tokens[1] if m & 1 else tokens[0])
        starts, kv = group_inputs(group)
        carry = attend(
            starts, query_rot, qpos, kv, carry, heads, half, group is groups[-1]
        )
        tokens.append(carry[0])
    mixture, mixture_b, log_total = carry

    def rows_of(x, s):
        return x[s * rows : (s + 1) * rows]

    attn_out = ring_scatter(lambda s: mm(rows_of(mixture_b, s), output_weight), nf)
    attn_rms = lax.rsqrt(jnp.mean(attn_out * attn_out, axis=1) + norm_eps)
    hidden_state = block_input.astype(F32) + attn_out * attn_rms[:, None] * attn_gain[None, :]
    state_slots = ring_gather(hidden_state.astype(BF), nf)
    gate_pre = [mm(x, gate_weight) for x in state_slots]
    up_pre = [mm(x, up_weight) for x in state_slots]
    activated = [(jax.nn.silu(g) * u).astype(BF) for g, u in zip(gate_pre, up_pre)]
    mlp_out = ring_scatter(lambda s: mm(activated[s], down_weight), nf)
    mlp_rms = lax.rsqrt(jnp.mean(mlp_out * mlp_out, axis=1) + norm_eps)
    block_output = (hidden_state + mlp_out * mlp_rms[:, None] * mlp_gain[None, :]).astype(BF)
    upstream = cotangent.astype(F32)
    mlp_gain_part = jnp.sum(upstream * mlp_out * mlp_rms[:, None], axis=0)
    mlp_grad_b = norm_back(mlp_out, mlp_rms, mlp_gain[None, :], upstream).astype(BF)
    grad_slots = ring_gather(mlp_grad_b, nf)

    gate_grads, up_grads = [], []
    for s in range(nf):
        activ_grad = contract_cols(grad_slots[s], down_weight)
        sg = jax.nn.sigmoid(gate_pre[s])
        gate_grads.append(
            (activ_grad * up_pre[s] * sg * (1.0 + gate_pre[s] * (1.0 - sg))).astype(BF)
        )
        up_grads.append((activ_grad * gate_pre[s] * sg).astype(BF))
    def ctx_scatter(x):
        return lax.psum_scatter(x, "ctx", scatter_dimension=0, tiled=True)

    down_part = contract_rows(jnp.concatenate(grad_slots), jnp.concatenate(activated)).astype(BF)
    gate_up_part = contract_rows(
        jnp.concatenate(state_slots),
        jnp.concatenate([jnp.concatenate(gate_grads), jnp.concatenate(up_grads)], axis=1),
    ).astype(BF)
    state_grad = upstream + ring_scatter(
        lambda s: contract_cols(gate_grads[s], gate_weight)
        + contract_cols(up_grads[s], up_weight),
        nf,
        (down_part,),
    )
    down_sum = ctx_scatter(down_part)
    gate_up_sum = ctx_scatter(gate_up_part)

    attn_gain_part = jnp.sum(state_grad * attn_out * attn_rms[:, None], axis=0)
    attn_grad_b = norm_back(attn_out, attn_rms, attn_gain[None, :], state_grad).astype(BF)
    proj_slots = ring_gather(attn_grad_b, nf, {0: (gate_up_part,)})
    mixture_grad_b = jnp.concatenate(
        [contract_cols(x, output_weight).astype(BF) for x in proj_slots]
    )

    dq = None
    sums = [{}, {}]

    def send(i, m):
        into, bit = came_from(m, orders[i])
        got = swap(sums[i].pop(m), nc, bit)
        sums[i][into] = (sums[i][into].astype(F32) + got.astype(F32)).astype(BF)
        return got

    waits = []
    for gi, group in enumerate(groups[::-1]):
        starts, kv = group_inputs(group)
        if gi >= 2 and waits:
            dq = gate(dq, *waits[gi - 2])
        dq, *out = attend_back(
            starts, query_rot, mixture_grad_b, mixture, log_total, qpos, kv, dq, heads, half
        )
        for m, a, b in zip(group, out[: len(group)], out[len(group) :]):
            sums[0][m], sums[1][m] = a, b
        waits.append([send(i, m) for i in range(2) for m in group if m & 1])
    hops = []
    for far in range(max(distance(m) for m in range(nc)), 0, -1):
        for i in range(2):
            for m in [m for m in sums[i] if distance(m) == far]:
                got = send(i, m)
                if m == orders[i][-1]:
                    hops.append(got)
    dq = gate(dq, *hops)
    own_a, own_b = sums[0][0], sums[1][0]

    def unit_full(x):
        return lax.dynamic_update_slice_in_dim(jnp.zeros((width,), F32), x, unit_start, 0)

    def norm_grads(weighted, inner, raw, rms):
        cube = rms * rms * rms
        return [
            (
                rows_of(rms, s) * rows_of(weighted, s)
                - raw[s] * rows_of(cube, s) * inner[s][:, None] / width
            ).astype(BF)
            for s in range(nf)
        ]

    def spread(*vectors):
        return jnp.stack([v.reshape(nf, width // nf) for v in vectors], axis=1).reshape(nf, -1)

    def gathered(flat, count):
        return flat.reshape(nf, count, width // nf).transpose(1, 0, 2).reshape(count, width)

    query_weighted, query_inner, query_gain_part = unrotate(
        [dq], q_raw, query_rms, query_scale, cosine, sine, heads, True
    )
    query_inner, early_gains = slot_sum(
        query_inner.reshape(nf, rows),
        nf,
        spread(unit_full(query_gain_part[0]), attn_gain_part, mlp_gain_part),
    )
    query_grads = norm_grads(query_weighted, query_inner, q_raw, query_rms)

    x_rows = jnp.concatenate(x_slots)
    q_part = contract_rows(x_rows, jnp.concatenate(query_grads)).astype(BF)
    o_part = contract_rows(jnp.concatenate(proj_slots), mixture_b).astype(BF)
    q_part, o_part, own_a, own_b = lax.optimization_barrier((q_part, o_part, own_a, own_b))
    query_grad = halving(q_part, me_c, nc, orders[0])
    output_grad = halving(o_part, me_c, nc, orders[1]).T

    key_weighted, key_inner, key_gain_part = unrotate(
        [own_a, own_b], k_raw, key_rms, key_scale, cosine, sine, heads, False
    )
    key_inner, key_gain_sum = slot_sum(
        key_inner.reshape(nf, rows), nf, spread(unit_full(key_gain_part[0]))
    )
    key_grads = norm_grads(key_weighted, key_inner, k_raw, key_rms)
    own = jnp.concatenate([own_a[:, units:], own_b[:, units:]])
    value_grads = [rows_of(own, s) for s in range(nf)]

    started = []
    input_grad = state_grad + ring_scatter(
        lambda s: contract_cols(query_grads[s], query_weight)
        + contract_cols(key_grads[s], key_weight)
        + contract_cols(value_grads[s], value_weight),
        nf,
        started=started,
    )
    k_rows, v_rows, *_ = lax.optimization_barrier((jnp.concatenate(key_grads), own, *started))
    k_part = contract_rows(x_rows, k_rows).astype(BF)
    v_part = contract_rows(x_rows, v_rows).astype(BF)
    key_grad = halving(k_part, me_c, nc, orders[0], (down_sum,))
    value_grad = halving(v_part, me_c, nc, orders[1], (gate_up_sum,))
    gains = jnp.concatenate([gathered(early_gains, 3), gathered(key_gain_sum, 1)])
    gains_own = halving(gains.T, me_c, nc, orders[0]).T
    down_grad = down_sum.astype(F32).T
    ff = gate_weight.shape[1]
    gate_up = gate_up_sum.astype(F32)
    gate_grad, up_grad = gate_up[:, :ff], gate_up[:, ff:]
    return (
        block_output,
        input_grad,
        query_grad,
        key_grad,
        value_grad,
        output_grad,
        gains_own[0],
        gains_own[3],
        gains_own[1],
        gains_own[2],
        gate_grad,
        up_grad,
        down_grad,
    )


def solution(mesh):
    return jax.shard_map(
        functools.partial(local, mesh.shape["ctx"], mesh.shape["fsdp"]),
        mesh=mesh,
        in_specs=(
            P(("ctx", "fsdp"), None),
            P(("ctx", "fsdp")),
            P(None, "fsdp"),
            P(None, "fsdp"),
            P(None, "fsdp"),
            P("fsdp", None),
            P(),
            P(),
            P(),
            P(),
            P(None, "fsdp"),
            P(None, "fsdp"),
            P("fsdp", None),
            P(("ctx", "fsdp"), None),
        ),
        out_specs=(
            P(("ctx", "fsdp"), None),
            P(("ctx", "fsdp"), None),
            P("ctx", "fsdp"),
            P("ctx", "fsdp"),
            P("ctx", "fsdp"),
            P("fsdp", "ctx"),
            P("ctx"),
            P("ctx"),
            P("ctx"),
            P("ctx"),
            P("ctx", "fsdp"),
            P("ctx", "fsdp"),
            P("fsdp", "ctx"),
        ),
        check_vma=False,
    )
```

```python
import functools
import math

import jax
import jax.numpy as jnp
from jax import lax
from jax.experimental import pallas as pl
from jax.experimental.pallas import tpu as pltpu
from jax.sharding import PartitionSpec as P


HD = 128
norm_eps = 1e-06
rope_base = 500000.0
big_negative = -1e30
LOG2E = math.log2(math.e)
BF = jnp.bfloat16
F32 = jnp.float32


def mm(left, right):
    return jnp.dot(left, right, preferred_element_type=F32)


def contract_rows(left, right):
    return lax.dot_general(left, right, (((0,), (0,)), ((), ())), preferred_element_type=F32)


def contract_cols(left, right):
    return lax.dot_general(left, right, (((1,), (1,)), ((), ())), preferred_element_type=F32)


def gate(x, *tokens):
    return lax.optimization_barrier((x, *tokens))[0]


def shift(x, n, by):
    return lax.ppermute(x, "fsdp", [(i, (i + by) % n) for i in range(n)])


def ring_gather(x, n, around=None):
    slots = [x]
    for _ in range(n - 1):
        slots.append(shift(slots[-1], around or n, 1))
    return slots


def ring_scatter(part, n, under=(), started=None):
    if n == 1:
        return part(0)
    acc = part(1).astype(BF)
    if started is not None:
        started.append(acc)
    for s in range(2, n):
        acc = (shift(acc, n, 1).astype(F32) + part(s)).astype(BF)
    return gate(shift(acc, n, 1), *under).astype(F32) + part(0)


def slot_sum(x, n, flat=None):
    total, flat_total = x, flat
    cut = x.shape[-1]
    both = x if flat is None else jnp.concatenate([x, flat], axis=-1)
    for t in range(1, n):
        got = shift(both, n, t)
        total = total + jnp.roll(got[..., :cut], t, axis=0)
        if flat is not None:
            flat_total = flat_total + got[..., cut:]
    return total if flat is None else (total, flat_total)


def swap(x, n, bit):
    return lax.ppermute(x, "ctx", [(i, i ^ bit) for i in range(n)])


def bit_orders(n):
    bits = []
    b = 2
    while b < n:
        bits.append(b)
        b *= 2
    return bits, bits[::-1]


def halving(part, me, n, order, under=()):
    seq = ([1] if n > 1 else []) + list(order[::-1])
    block = part.shape[0] // n
    levels = len(seq)
    masks = [
        sum(seq[k] for k in range(levels) if t >> (levels - 1 - k) & 1) for t in range(n)
    ]

    def blocks(ms):
        return jnp.concatenate(
            [lax.dynamic_slice_in_dim(part, (me ^ m) * block, block) for m in ms]
        )

    keep, away = blocks(masks[: n // 2]), blocks(masks[n // 2 :])
    for k, bit in enumerate(seq):
        got = swap(away.astype(BF), n, bit)
        if k == 0 and under:
            got = gate(got, *under)
        total = keep.astype(F32) + got.astype(F32)
        rest = total.shape[0] // 2
        if k < levels - 1:
            total = total.astype(BF)
            keep, away = total[:rest], total[rest:]
    return total


def distance(m):
    return bin(m >> 1).count("1")


def group_order(n):
    pairs = [(m, m + 1) if n > 1 else (m,) for m in range(0, n, 2)]
    return sorted(pairs, key=lambda g: (distance(g[0]), g[0]))


def came_from(m, order):
    if m & 1:
        return m ^ 1, 1
    bit = [b for b in order if m & b][-1]
    return m ^ bit, bit


def vmem(*_):
    return pl.BlockSpec(memory_space=pltpu.VMEM)


def prep_kernel(n, heads, *refs):
    q_refs, k_refs, v_refs = refs[:n], refs[n : 2 * n], refs[2 * n : 3 * n]
    qr_ref, kr_ref, qg_ref, kg_ref, cos_ref, sin_ref = refs[3 * n : 3 * n + 6]
    qo_ref, kva_ref, kvb_ref = refs[3 * n + 6 :]
    rows = q_refs[0].shape[0]
    half = n // 2
    for s in range(n):
        r = slice(s * rows, (s + 1) * rows)
        cosine, sine = cos_ref[r, :], sin_ref[r, :]
        out = kva_ref if s < half else kvb_ref
        o = slice((s % half) * rows, (s % half + 1) * rows)
        for h in range(heads):
            c = slice(h * HD, (h + 1) * HD)
            x = q_refs[s][:, c] * qr_ref[r, :] * qg_ref[:, c]
            qo_ref[r, c] = (x * cosine + pltpu.roll(x, HD // 2, 1) * sine).astype(BF)
            y = k_refs[s][:, c] * kr_ref[r, :] * kg_ref[:, c]
            out[o, c] = (y * cosine + pltpu.roll(y, HD // 2, 1) * sine).astype(BF)
            out[o, heads * HD + h * HD : heads * HD + (h + 1) * HD] = v_refs[s][:, c].astype(BF)


def key_mask(starts_ref, piece, slots, rows, qpos):
    parts = []
    for j in range(slots):
        row = lax.broadcasted_iota(jnp.int32, (rows, 1), 0)
        parts.append(row + starts_ref[piece * slots + j])
    return jnp.concatenate(parts, axis=0) <= qpos


def fwd_kernel(npieces, slots, first, last, *refs):
    starts_ref, q_ref, qpos_ref = refs[:3]
    k_refs = refs[3 : 3 + npieces]
    v_refs = refs[3 + npieces : 3 + 2 * npieces]
    rest = refs[3 + 2 * npieces :]
    if not first:
        m_in, l_in, a_in = rest[:3]
        rest = rest[3:]
    rows = k_refs[0].shape[0] // slots
    c2 = LOG2E / math.sqrt(HD)
    q = q_ref[...]
    qpos = qpos_ref[...]
    scores = []
    top = None if first else m_in[0]
    for i in range(npieces):
        s = contract_cols(k_refs[i][...], q)
        s = jnp.where(key_mask(starts_ref, i, slots, rows, qpos), s, big_negative)
        scores.append(s)
        t = jnp.max(s, axis=0, keepdims=True)
        top = t if top is None else jnp.maximum(top, t)
    total = None
    acc = None
    for i in range(npieces):
        p = jnp.exp2((scores[i] - top) * c2)
        t = jnp.sum(p, axis=0, keepdims=True)
        a = contract_rows(v_refs[i][...], p.astype(BF))
        total = t if total is None else total + t
        acc = a if acc is None else acc + a
    if not first:
        alpha = jnp.exp2((m_in[0] - top) * c2)
        total = total + l_in[0] * alpha
        acc = acc + a_in[...] * alpha
    if last:
        mix_ref, mixb_ref, log_ref = rest
        mix = (acc / total).T
        mix_ref[...] = mix
        mixb_ref[...] = mix.astype(BF)
        log_ref[0] = top * c2 + jnp.log2(total)
    else:
        m_out, l_out, a_out = rest
        m_out[0] = top
        l_out[0] = total
        a_out[...] = acc


def attend(starts, q, qpos, kv, carry, heads, slots, last):
    span = q.shape[0]
    first = carry is None
    np_ = len(kv)
    pr = kv[0].shape[0]
    row = pl.BlockSpec((1, 1, span), lambda h: (h, 0, 0))
    accs = pl.BlockSpec((HD, span), lambda h: (h, 0))
    specs = [
        pl.BlockSpec(memory_space=pltpu.SMEM),
        pl.BlockSpec((span, HD), lambda h: (0, h)),
        pl.BlockSpec((1, span), lambda h: (0, 0)),
    ]
    specs += [pl.BlockSpec((pr, HD), lambda h: (0, h))] * np_
    specs += [pl.BlockSpec((pr, HD), lambda h: (0, heads + h))] * np_
    args = [starts, q, qpos, *kv, *kv]
    if not first:
        specs += [row, row, accs]
        args += list(carry)
    rshape = jax.ShapeDtypeStruct((heads, 1, span), F32)
    if last:
        mix = pl.BlockSpec((span, HD), lambda h: (0, h))
        outs = [mix, mix, row]
        shapes = [
            jax.ShapeDtypeStruct((span, heads * HD), F32),
            jax.ShapeDtypeStruct((span, heads * HD), BF),
            rshape,
        ]
    else:
        outs = [row, row, accs]
        shapes = [rshape, rshape, jax.ShapeDtypeStruct((heads * HD, span), F32)]
    keys = np_ * pr
    return pl.pallas_call(
        functools.partial(fwd_kernel, np_, slots, first, last),
        grid=(heads,),
        in_specs=specs,
        out_specs=outs,
        out_shape=shapes,
        cost_estimate=pl.CostEstimate(
            flops=8 * span * keys * HD * heads,
            bytes_accessed=4 * keys * heads * HD,
            transcendentals=span * keys * heads,
        ),
    )(*args)


def bwd_kernel(npieces, slots, heads, first, *refs):
    starts_ref, q_ref, do_ref, mix_ref, log_ref, qpos_ref = refs[:6]
    k_refs = refs[6 : 6 + npieces]
    v_refs = refs[6 + npieces : 6 + 2 * npieces]
    rest = refs[6 + 2 * npieces :]
    if not first:
        dq_in = rest[0]
        rest = rest[1:]
    dq_ref, out_refs = rest[0], rest[1:]
    h = pl.program_id(0)
    rows = k_refs[0].shape[0] // slots
    scale = 1.0 / math.sqrt(HD)
    c2 = LOG2E * scale
    q = q_ref[...]
    do = do_ref[...]
    delta = jnp.sum((do.astype(F32) * mix_ref[...]).T, axis=0, keepdims=True)
    log2 = log_ref[0]
    qpos = qpos_ref[...]
    dq = None
    for i in range(npieces):
        k = k_refs[i][...]
        s = contract_cols(k, q) * c2 - log2
        s = jnp.where(key_mask(starts_ref, i, slots, rows, qpos), s, big_negative)
        p = jnp.exp2(s)
        dp = contract_cols(v_refs[i][...], do)
        ds = (p * (dp - delta)).astype(BF)
        t = contract_rows(k, ds)
        dq = t if dq is None else dq + t
        kc = pl.ds(pl.multiple_of(h * HD, HD), HD)
        vc = pl.ds(pl.multiple_of((heads + h) * HD, HD), HD)
        out_refs[i][:, kc] = (mm(ds, q) * scale).astype(BF)
        out_refs[i][:, vc] = mm(p.astype(BF), do).astype(BF)
    dq = dq * scale
    dq_ref[...] = dq if first else dq + dq_in[...]


def attend_back(starts, q, do, mix, log, qpos, kv, dq, heads, slots):
    span = q.shape[0]
    first = dq is None
    np_ = len(kv)
    pr = kv[0].shape[0]
    head = pl.BlockSpec((span, HD), lambda h: (0, h))
    accs = pl.BlockSpec((HD, span), lambda h: (h, 0))
    specs = [
        pl.BlockSpec(memory_space=pltpu.SMEM),
        head,
        head,
        head,
        pl.BlockSpec((1, 1, span), lambda h: (h, 0, 0)),
        pl.BlockSpec((1, span), lambda h: (0, 0)),
    ]
    specs += [pl.BlockSpec((pr, HD), lambda h: (0, h))] * np_
    specs += [pl.BlockSpec((pr, HD), lambda h: (0, heads + h))] * np_
    args = [starts, q, do, mix, log, qpos, *kv, *kv]
    if not first:
        specs.append(accs)
        args.append(dq)
    keys = np_ * pr
    return pl.pallas_call(
        functools.partial(bwd_kernel, np_, slots, heads, first),
        grid=(heads,),
        in_specs=specs,
        out_specs=[accs] + [pl.BlockSpec((pr, 2 * heads * HD), lambda h: (0, 0))] * np_,
        out_shape=[jax.ShapeDtypeStruct((heads * HD, span), F32)]
        + [jax.ShapeDtypeStruct((pr, 2 * heads * HD), BF)] * np_,
        cost_estimate=pl.CostEstimate(
            flops=20 * span * keys * HD * heads,
            bytes_accessed=8 * keys * heads * HD,
            transcendentals=span * keys * heads,
        ),
    )(*args)


def turn_back(x, cosine, sine):
    return x * cosine - pltpu.roll(x, HD // 2, 1) * sine


def unrotate_kernel(n, heads, transposed, *refs):
    nd = 1 if transposed else 2
    d_refs = refs[:nd]
    raw_refs = refs[nd : nd + n]
    r_ref, g_ref, cos_ref, sin_ref, w_ref, inner_ref, gain_ref = refs[nd + n :]
    rows = raw_refs[0].shape[0]
    half = n // 2
    for h in range(heads):
        c = slice(h * HD, (h + 1) * HD)
        gain_sum = None
        whole = d_refs[0][c, :].T if transposed else None
        for s in range(n):
            r = slice(s * rows, (s + 1) * rows)
            if transposed:
                d = whole[r, :]
            else:
                o = slice((s % half) * rows, (s % half + 1) * rows)
                d = d_refs[0 if s < half else 1][o, c].astype(F32)
            grad = turn_back(d, cos_ref[r, :], sin_ref[r, :])
            raw = raw_refs[s][:, c]
            weighted = grad * g_ref[:, c]
            w_ref[r, c] = weighted
            t = jnp.sum(weighted * raw, axis=1, keepdims=True)
            inner_ref[r, :] = t if h == 0 else inner_ref[r, :] + t
            u = jnp.sum(grad * raw * r_ref[r, :], axis=0, keepdims=True)
            gain_sum = u if gain_sum is None else gain_sum + u
        gain_ref[:, c] = gain_sum


def unrotate(d, raw, rms, gain, cosine, sine, heads, transposed):
    n = len(raw)
    span = n * raw[0].shape[0]
    units = heads * HD
    return pl.pallas_call(
        functools.partial(unrotate_kernel, n, heads, transposed),
        in_specs=[vmem()] * (len(d) + n + 4),
        out_specs=[vmem()] * 3,
        out_shape=[
            jax.ShapeDtypeStruct((span, units), F32),
            jax.ShapeDtypeStruct((span, 1), F32),
            jax.ShapeDtypeStruct((1, units), F32),
        ],
    )(*d, *raw, rms, gain, cosine, sine)


def norm_back(raw, rms_inv, gain, grad_out):
    weighted = gain * grad_out
    inner = jnp.sum(weighted * raw, axis=1, keepdims=True)
    width = raw.shape[1]
    return (
        rms_inv[:, None] * weighted - raw * (rms_inv * rms_inv * rms_inv)[:, None] * inner / width
    )


def local(
    nc,
    nf,
    block_input,
    positions,
    query_weight,
    key_weight,
    value_weight,
    output_weight,
    query_gain,
    key_gain,
    attn_gain,
    mlp_gain,
    gate_weight,
    up_weight,
    down_weight,
    cotangent,
):
    rows, width = block_input.shape
    span = rows * nf
    units = query_weight.shape[1]
    heads = units // HD
    half = nf // 2
    me_c = lax.axis_index("ctx")
    me_f = lax.axis_index("fsdp")
    unit_start = me_f * units

    x_slots = [block_input]
    begin = positions[:1]
    begins = None
    for s in range(1, nf):
        got = shift(x_slots[-1], nf, 1)
        if s == min(2, nf - 1):
            begin, x_last = lax.optimization_barrier((begin, mm(x_slots[-1], query_weight)))
            begins = jnp.concatenate([begin] + [shift(begin, nf, t) for t in range(1, nf)])[None, :]
            b = 1
            while b < nc:
                begins = jnp.concatenate([begins, swap(begins, nc, b)])
                b *= 2
        if s == nf - 1:
            got, begins = lax.optimization_barrier((got, begins))
        x_slots.append(got)

    row_pos = (begins[0][:, None] + jnp.arange(rows)[None, :]).reshape(span)
    freqs = jnp.exp(-math.log(rope_base) * 2.0 * jnp.arange(HD // 2).astype(F32) / HD)
    angles = row_pos.astype(F32)[:, None] * freqs[None, :]
    cosine, sine = jnp.cos(angles), jnp.sin(angles)
    cosine = jnp.concatenate([cosine, cosine], axis=1)
    sine = jnp.concatenate([-sine, sine], axis=1)
    qpos = row_pos[None, :]

    q_raw = [mm(x, query_weight) for x in x_slots]
    q_raw[min(2, nf - 1) - 1] = x_last
    k_raw = [mm(x, key_weight) for x in x_slots]
    v_raw = [mm(x, value_weight) for x in x_slots]
    squares = jnp.stack(
        [
            jnp.stack([jnp.sum(q * q, axis=1), jnp.sum(k * k, axis=1)])
            for q, k in zip(q_raw, k_raw)
        ]
    )
    squares = slot_sum(squares, nf)
    query_rms = lax.rsqrt(squares[:, 0].reshape(span, 1) / width + norm_eps)
    key_rms = lax.rsqrt(squares[:, 1].reshape(span, 1) / width + norm_eps)
    query_scale = lax.dynamic_slice_in_dim(query_gain, unit_start, units)[None, :]
    key_scale = lax.dynamic_slice_in_dim(key_gain, unit_start, units)[None, :]

    query_rot, kv_a, kv_b = pl.pallas_call(
        functools.partial(prep_kernel, nf, heads),
        in_specs=[vmem()] * (3 * nf + 6),
        out_specs=[vmem()] * 3,
        out_shape=[jax.ShapeDtypeStruct((span, units), BF)]
        + [jax.ShapeDtypeStruct((span // 2, 2 * units), BF)] * 2,
    )(*q_raw, *k_raw, *v_raw, query_rms, key_rms, query_scale, key_scale, cosine, sine)

    orders = bit_orders(nc)
    groups = group_order(nc)
    pieces = [{0: kv_a}, {0: kv_b}]

    def fetch(i, m, token):
        if m not in pieces[i]:
            src, bit = came_from(m, orders[i])
            have = fetch(i, src, token)
            if token is not None:
                have = gate(have, token)
            pieces[i][m] = swap(have, nc, bit)
        return pieces[i][m]

    def group_inputs(group):
        kv = [pieces[0][m] for m in group] + [pieces[1][m] for m in group]
        starts = jnp.concatenate(
            [begins[m, :half] for m in group] + [begins[m, half:] for m in group]
        )
        return starts, kv

    carry = None
    tokens = []
    for group in groups:
        for m in group:
            for i in range(2):
                far = distance(m)
                if far < 2:
                    fetch(i, m, None)
                else:
                    fetch(i, m, tokens[1] if m & 1 else tokens[0])
        starts, kv = group_inputs(group)
        carry = attend(
            starts, query_rot, qpos, kv, carry, heads, half, group is groups[-1]
        )
        tokens.append(carry[0])
    mixture, mixture_b, log_total = carry

    def rows_of(x, s):
        return x[s * rows : (s + 1) * rows]

    attn_out = ring_scatter(lambda s: mm(rows_of(mixture_b, s), output_weight), nf)
    attn_rms = lax.rsqrt(jnp.mean(attn_out * attn_out, axis=1) + norm_eps)
    hidden_state = block_input.astype(F32) + attn_out * attn_rms[:, None] * attn_gain[None, :]
    state_slots = ring_gather(hidden_state.astype(BF), nf)
    gate_pre = [mm(x, gate_weight) for x in state_slots]
    up_pre = [mm(x, up_weight) for x in state_slots]
    activated = [(jax.nn.silu(g) * u).astype(BF) for g, u in zip(gate_pre, up_pre)]
    mlp_out = ring_scatter(lambda s: mm(activated[s], down_weight), nf)
    mlp_rms = lax.rsqrt(jnp.mean(mlp_out * mlp_out, axis=1) + norm_eps)
    block_output = (hidden_state + mlp_out * mlp_rms[:, None] * mlp_gain[None, :]).astype(BF)
    upstream = cotangent.astype(F32)
    mlp_gain_part = jnp.sum(upstream * mlp_out * mlp_rms[:, None], axis=0)
    mlp_grad_b = norm_back(mlp_out, mlp_rms, mlp_gain[None, :], upstream).astype(BF)

    def ctx_scatter(x):
        return lax.psum_scatter(x, "ctx", scatter_dimension=0, tiled=True)

    def slot_grads(s, rows_in):
        activ_grad = contract_cols(rows_in, down_weight)
        sg = jax.nn.sigmoid(gate_pre[s])
        g = (activ_grad * up_pre[s] * sg * (1.0 + gate_pre[s] * (1.0 - sg))).astype(BF)
        return g, (activ_grad * gate_pre[s] * sg).astype(BF)

    def state_part(g, u):
        return contract_cols(g, gate_weight) + contract_cols(u, up_weight)

    grad_slots, gate_grads, up_grads = [mlp_grad_b], [], []
    acc = None
    for s in range(nf):
        got = shift(grad_slots[-1], nf, 1) if s < nf - 1 else None
        g, u = slot_grads(s, grad_slots[s])
        if s == 1:
            acc = state_part(g, u).astype(BF)
        elif s > 1:
            acc = (shift(acc, nf, 1).astype(F32) + state_part(g, u)).astype(BF)
        if got is not None:
            got, g, u = lax.optimization_barrier((got, g, u))
            grad_slots.append(got)
        gate_grads.append(g)
        up_grads.append(u)
    down_part = contract_rows(jnp.concatenate(grad_slots), jnp.concatenate(activated)).astype(BF)
    state_grad = state_part(gate_grads[0], up_grads[0])
    if nf > 1:
        got = shift(acc, nf, 1)
        state_grad = got.astype(F32) + state_grad
    state_grad = upstream + state_grad
    down_sum = ctx_scatter(down_part)

    attn_gain_part = jnp.sum(state_grad * attn_out * attn_rms[:, None], axis=0)
    attn_grad_b = norm_back(attn_out, attn_rms, attn_gain[None, :], state_grad).astype(BF)
    gate_up_part = contract_rows(
        jnp.concatenate(state_slots),
        jnp.concatenate([jnp.concatenate(gate_grads), jnp.concatenate(up_grads)], axis=1),
    ).astype(BF)
    gate_up_sum = ctx_scatter(gate_up_part)
    first_hop = shift(attn_grad_b, nf, 1)
    proj_slots = [attn_grad_b] + ring_gather(first_hop, nf - 1, around=nf)
    mixture_grad_b = jnp.concatenate(
        [contract_cols(x, output_weight).astype(BF) for x in proj_slots]
    )

    dq = None
    sums = [{}, {}]

    def send(i, m):
        into, bit = came_from(m, orders[i])
        got = swap(sums[i].pop(m), nc, bit)
        sums[i][into] = (sums[i][into].astype(F32) + got.astype(F32)).astype(BF)
        return got

    waits = []
    for gi, group in enumerate(groups[::-1]):
        starts, kv = group_inputs(group)
        if gi:
            dq = gate(dq, *waits[gi - 1])
        dq, *out = attend_back(
            starts, query_rot, mixture_grad_b, mixture, log_total, qpos, kv, dq, heads, half
        )
        for m, a, b in zip(group, out[: len(group)], out[len(group) :]):
            sums[0][m], sums[1][m] = a, b
        waits.append([send(i, m) for i in range(2) for m in group if m & 1])
    hops = []
    for far in range(max(distance(m) for m in range(nc)), 0, -1):
        for i in range(2):
            for m in [m for m in sums[i] if distance(m) == far]:
                got = send(i, m)
                if m == orders[i][-1]:
                    hops.append(got)
    dq = gate(dq, *hops)
    own_a, own_b = sums[0][0], sums[1][0]

    def unit_full(x):
        return lax.dynamic_update_slice_in_dim(jnp.zeros((width,), F32), x, unit_start, 0)

    def norm_grads(weighted, inner, raw, rms):
        cube = rms * rms * rms
        return [
            (
                rows_of(rms, s) * rows_of(weighted, s)
                - raw[s] * rows_of(cube, s) * inner[s][:, None] / width
            ).astype(BF)
            for s in range(nf)
        ]

    def spread(*vectors):
        return jnp.stack([v.reshape(nf, width // nf) for v in vectors], axis=1).reshape(nf, -1)

    def gathered(flat, count):
        return flat.reshape(nf, count, width // nf).transpose(1, 0, 2).reshape(count, width)

    query_weighted, query_inner, query_gain_part = unrotate(
        [dq], q_raw, query_rms, query_scale, cosine, sine, heads, True
    )
    query_inner, early_gains = slot_sum(
        query_inner.reshape(nf, rows),
        nf,
        spread(unit_full(query_gain_part[0]), attn_gain_part, mlp_gain_part),
    )
    query_grads = norm_grads(query_weighted, query_inner, q_raw, query_rms)

    x_rows = jnp.concatenate(x_slots)
    q_part = contract_rows(x_rows, jnp.concatenate(query_grads)).astype(BF)
    o_part = contract_rows(jnp.concatenate(proj_slots), mixture_b).astype(BF)
    qo_part = jnp.concatenate([q_part, o_part], axis=1)
    qo_part, down_sum, own_a, own_b = lax.optimization_barrier((qo_part, down_sum, own_a, own_b))
    qo_grad = ctx_scatter(qo_part).astype(F32)
    query_grad, output_grad = qo_grad[:, :units], qo_grad[:, units:].T

    key_weighted, key_inner, key_gain_part = unrotate(
        [own_a, own_b], k_raw, key_rms, key_scale, cosine, sine, heads, False
    )
    key_inner, key_gain_sum = slot_sum(
        key_inner.reshape(nf, rows), nf, spread(unit_full(key_gain_part[0]))
    )
    key_grads = norm_grads(key_weighted, key_inner, k_raw, key_rms)
    own = jnp.concatenate([own_a[:, units:], own_b[:, units:]])
    value_grads = [rows_of(own, s) for s in range(nf)]

    started = []
    input_grad = state_grad + ring_scatter(
        lambda s: contract_cols(query_grads[s], query_weight)
        + contract_cols(key_grads[s], key_weight)
        + contract_cols(value_grads[s], value_weight),
        nf,
        started=started,
    )
    k_rows, v_rows, *_ = lax.optimization_barrier((jnp.concatenate(key_grads), own, *started))
    k_part = contract_rows(x_rows, k_rows).astype(BF)
    v_part = contract_rows(x_rows, v_rows).astype(BF)
    key_grad = halving(k_part, me_c, nc, orders[0])
    value_grad = halving(v_part, me_c, nc, orders[1], (gate_up_sum,))
    gains = jnp.concatenate([gathered(early_gains, 3), gathered(key_gain_sum, 1)])
    gains_own = halving(gains.T, me_c, nc, orders[0]).T
    down_grad = down_sum.astype(F32).T
    ff = gate_weight.shape[1]
    gate_up = gate_up_sum.astype(F32)
    gate_grad, up_grad = gate_up[:, :ff], gate_up[:, ff:]
    return (
        block_output,
        input_grad,
        query_grad,
        key_grad,
        value_grad,
        output_grad,
        gains_own[0],
        gains_own[3],
        gains_own[1],
        gains_own[2],
        gate_grad,
        up_grad,
        down_grad,
    )


def solution(mesh):
    def layer(*args):
        return local(mesh.shape["ctx"], mesh.shape["fsdp"], *args)

    return jax.shard_map(
        layer,
        mesh=mesh,
        in_specs=(
            P(("ctx", "fsdp"), None),
            P(("ctx", "fsdp")),
            P(None, "fsdp"),
            P(None, "fsdp"),
            P(None, "fsdp"),
            P("fsdp", None),
            P(),
            P(),
            P(),
            P(),
            P(None, "fsdp"),
            P(None, "fsdp"),
            P("fsdp", None),
            P(("ctx", "fsdp"), None),
        ),
        out_specs=(
            P(("ctx", "fsdp"), None),
            P(("ctx", "fsdp"), None),
            P("ctx", "fsdp"),
            P("ctx", "fsdp"),
            P("ctx", "fsdp"),
            P("fsdp", "ctx"),
            P("ctx"),
            P("ctx"),
            P("ctx"),
            P("ctx"),
            P("ctx", "fsdp"),
            P("ctx", "fsdp"),
            P("fsdp", "ctx"),
        ),
        check_vma=False,
    )
```

```python
import functools
import math

import jax
import jax.numpy as jnp
from jax import lax
from jax.experimental import pallas as pl
from jax.experimental.pallas import tpu as pltpu
from jax.sharding import PartitionSpec as P


HD = 128
norm_eps = 1e-06
rope_base = 500000.0
big_negative = -1e30
LOG2E = math.log2(math.e)
BF = jnp.bfloat16
F32 = jnp.float32


def mm(left, right):
    return jnp.dot(left, right, preferred_element_type=F32)


def contract_rows(left, right):
    return lax.dot_general(left, right, (((0,), (0,)), ((), ())), preferred_element_type=F32)


def contract_cols(left, right):
    return lax.dot_general(left, right, (((1,), (1,)), ((), ())), preferred_element_type=F32)


def gate(x, *tokens):
    return lax.optimization_barrier((x, *tokens))[0]


def shift(x, n, by):
    return lax.ppermute(x, "fsdp", [(i, (i + by) % n) for i in range(n)])


def ring_gather(x, n, around=None):
    slots = [x]
    for _ in range(n - 1):
        slots.append(shift(slots[-1], around or n, 1))
    return slots


def ring_scatter(part, n, under=(), started=None):
    if n == 1:
        return part(0)
    acc = part(1).astype(BF)
    if started is not None:
        started.append(acc)
    for s in range(2, n):
        acc = (shift(acc, n, 1).astype(F32) + part(s)).astype(BF)
    return gate(shift(acc, n, 1), *under).astype(F32) + part(0)


def slot_sum(x, n, flat=None):
    total, flat_total = x, flat
    cut = x.shape[-1]
    both = x if flat is None else jnp.concatenate([x, flat], axis=-1)
    for t in range(1, n):
        got = shift(both, n, t)
        total = total + jnp.roll(got[..., :cut], t, axis=0)
        if flat is not None:
            flat_total = flat_total + got[..., cut:]
    return total if flat is None else (total, flat_total)


def swap(x, n, bit):
    return lax.ppermute(x, "ctx", [(i, i ^ bit) for i in range(n)])


def bit_orders(n):
    bits = []
    b = 2
    while b < n:
        bits.append(b)
        b *= 2
    return bits, bits[::-1]


def halving(part, me, n, order, marks=None):
    seq = ([1] if n > 1 else []) + list(order[::-1])
    block = part.shape[0] // n
    levels = len(seq)
    masks = [
        sum(seq[k] for k in range(levels) if t >> (levels - 1 - k) & 1) for t in range(n)
    ]

    def blocks(ms):
        return jnp.concatenate(
            [lax.dynamic_slice_in_dim(part, (me ^ m) * block, block) for m in ms]
        )

    keep, away = blocks(masks[: n // 2]), blocks(masks[n // 2 :])
    for k, bit in enumerate(seq):
        got = swap(away.astype(BF), n, bit)
        total = keep.astype(F32) + got.astype(F32)
        rest = total.shape[0] // 2
        if k < levels - 1:
            total = total.astype(BF)
            if marks is not None:
                marks[k].append(total)
            keep, away = total[:rest], total[rest:]
    return total


def distance(m):
    return bin(m >> 1).count("1")


def group_order(n):
    pairs = [(m, m + 1) if n > 1 else (m,) for m in range(0, n, 2)]
    return sorted(pairs, key=lambda g: (distance(g[0]), g[0]))


def came_from(m, order):
    if m & 1:
        return m ^ 1, 1
    bit = [b for b in order if m & b][-1]
    return m ^ bit, bit


def vmem(*_):
    return pl.BlockSpec(memory_space=pltpu.VMEM)


def prep_kernel(n, heads, *refs):
    q_refs, k_refs, v_refs = refs[:n], refs[n : 2 * n], refs[2 * n : 3 * n]
    qr_ref, kr_ref, qg_ref, kg_ref, cos_ref, sin_ref = refs[3 * n : 3 * n + 6]
    qo_ref, kva_ref, kvb_ref = refs[3 * n + 6 :]
    rows = q_refs[0].shape[0]
    half = n // 2
    for s in range(n):
        r = slice(s * rows, (s + 1) * rows)
        cosine, sine = cos_ref[r, :], sin_ref[r, :]
        out = kva_ref if s < half else kvb_ref
        o = slice((s % half) * rows, (s % half + 1) * rows)
        for h in range(heads):
            c = slice(h * HD, (h + 1) * HD)
            x = q_refs[s][:, c] * qr_ref[r, :] * qg_ref[:, c]
            qo_ref[r, c] = (x * cosine + pltpu.roll(x, HD // 2, 1) * sine).astype(BF)
            y = k_refs[s][:, c] * kr_ref[r, :] * kg_ref[:, c]
            out[o, c] = (y * cosine + pltpu.roll(y, HD // 2, 1) * sine).astype(BF)
            out[o, heads * HD + h * HD : heads * HD + (h + 1) * HD] = v_refs[s][:, c].astype(BF)


def key_mask(starts_ref, piece, slots, rows, qpos):
    parts = []
    for j in range(slots):
        row = lax.broadcasted_iota(jnp.int32, (rows, 1), 0)
        parts.append(row + starts_ref[piece * slots + j])
    return jnp.concatenate(parts, axis=0) <= qpos


def fwd_kernel(npieces, slots, first, last, *refs):
    starts_ref, q_ref, qpos_ref = refs[:3]
    k_refs = refs[3 : 3 + npieces]
    v_refs = refs[3 + npieces : 3 + 2 * npieces]
    rest = refs[3 + 2 * npieces :]
    if not first:
        m_in, l_in, a_in = rest[:3]
        rest = rest[3:]
    rows = k_refs[0].shape[0] // slots
    c2 = LOG2E / math.sqrt(HD)
    q = q_ref[...]
    qpos = qpos_ref[...]
    scores = []
    top = None if first else m_in[0]
    for i in range(npieces):
        s = contract_cols(k_refs[i][...], q)
        s = jnp.where(key_mask(starts_ref, i, slots, rows, qpos), s, big_negative)
        scores.append(s)
        t = jnp.max(s, axis=0, keepdims=True)
        top = t if top is None else jnp.maximum(top, t)
    total = None
    acc = None
    for i in range(npieces):
        p = jnp.exp2((scores[i] - top) * c2)
        t = jnp.sum(p, axis=0, keepdims=True)
        a = contract_rows(v_refs[i][...], p.astype(BF))
        total = t if total is None else total + t
        acc = a if acc is None else acc + a
    if not first:
        alpha = jnp.exp2((m_in[0] - top) * c2)
        total = total + l_in[0] * alpha
        acc = acc + a_in[...] * alpha
    if last:
        mix_ref, mixb_ref, log_ref = rest
        mix = (acc / total).T
        mix_ref[...] = mix
        mixb_ref[...] = mix.astype(BF)
        log_ref[0] = top * c2 + jnp.log2(total)
    else:
        m_out, l_out, a_out = rest
        m_out[0] = top
        l_out[0] = total
        a_out[...] = acc


def attend(starts, q, qpos, kv, carry, heads, slots, last):
    span = q.shape[0]
    first = carry is None
    np_ = len(kv)
    pr = kv[0].shape[0]
    row = pl.BlockSpec((1, 1, span), lambda h: (h, 0, 0))
    accs = pl.BlockSpec((HD, span), lambda h: (h, 0))
    specs = [
        pl.BlockSpec(memory_space=pltpu.SMEM),
        pl.BlockSpec((span, HD), lambda h: (0, h)),
        pl.BlockSpec((1, span), lambda h: (0, 0)),
    ]
    specs += [pl.BlockSpec((pr, HD), lambda h: (0, h))] * np_
    specs += [pl.BlockSpec((pr, HD), lambda h: (0, heads + h))] * np_
    args = [starts, q, qpos, *kv, *kv]
    if not first:
        specs += [row, row, accs]
        args += list(carry)
    rshape = jax.ShapeDtypeStruct((heads, 1, span), F32)
    if last:
        mix = pl.BlockSpec((span, HD), lambda h: (0, h))
        outs = [mix, mix, row]
        shapes = [
            jax.ShapeDtypeStruct((span, heads * HD), F32),
            jax.ShapeDtypeStruct((span, heads * HD), BF),
            rshape,
        ]
    else:
        outs = [row, row, accs]
        shapes = [rshape, rshape, jax.ShapeDtypeStruct((heads * HD, span), F32)]
    keys = np_ * pr
    return pl.pallas_call(
        functools.partial(fwd_kernel, np_, slots, first, last),
        grid=(heads,),
        in_specs=specs,
        out_specs=outs,
        out_shape=shapes,
        cost_estimate=pl.CostEstimate(
            flops=8 * span * keys * HD * heads,
            bytes_accessed=4 * keys * heads * HD,
            transcendentals=span * keys * heads,
        ),
    )(*args)


def bwd_kernel(npieces, slots, heads, first, *refs):
    starts_ref, q_ref, do_ref, mix_ref, log_ref, qpos_ref = refs[:6]
    k_refs = refs[6 : 6 + npieces]
    v_refs = refs[6 + npieces : 6 + 2 * npieces]
    rest = refs[6 + 2 * npieces :]
    if not first:
        dq_in = rest[0]
        rest = rest[1:]
    dq_ref, out_refs = rest[0], rest[1:]
    h = pl.program_id(0)
    rows = k_refs[0].shape[0] // slots
    scale = 1.0 / math.sqrt(HD)
    c2 = LOG2E * scale
    q = q_ref[...]
    do = do_ref[...]
    delta = jnp.sum((do.astype(F32) * mix_ref[...]).T, axis=0, keepdims=True)
    log2 = log_ref[0]
    qpos = qpos_ref[...]
    dq = None
    for i in range(npieces):
        k = k_refs[i][...]
        s = contract_cols(k, q) * c2 - log2
        s = jnp.where(key_mask(starts_ref, i, slots, rows, qpos), s, big_negative)
        p = jnp.exp2(s)
        dp = contract_cols(v_refs[i][...], do)
        ds = (p * (dp - delta)).astype(BF)
        t = contract_rows(k, ds)
        dq = t if dq is None else dq + t
        kc = pl.ds(pl.multiple_of(h * HD, HD), HD)
        vc = pl.ds(pl.multiple_of((heads + h) * HD, HD), HD)
        out_refs[i][:, kc] = (mm(ds, q) * scale).astype(BF)
        out_refs[i][:, vc] = mm(p.astype(BF), do).astype(BF)
    dq = dq * scale
    dq_ref[...] = dq if first else dq + dq_in[...]


def attend_back(starts, q, do, mix, log, qpos, kv, dq, heads, slots):
    span = q.shape[0]
    first = dq is None
    np_ = len(kv)
    pr = kv[0].shape[0]
    head = pl.BlockSpec((span, HD), lambda h: (0, h))
    accs = pl.BlockSpec((HD, span), lambda h: (h, 0))
    specs = [
        pl.BlockSpec(memory_space=pltpu.SMEM),
        head,
        head,
        head,
        pl.BlockSpec((1, 1, span), lambda h: (h, 0, 0)),
        pl.BlockSpec((1, span), lambda h: (0, 0)),
    ]
    specs += [pl.BlockSpec((pr, HD), lambda h: (0, h))] * np_
    specs += [pl.BlockSpec((pr, HD), lambda h: (0, heads + h))] * np_
    args = [starts, q, do, mix, log, qpos, *kv, *kv]
    if not first:
        specs.append(accs)
        args.append(dq)
    keys = np_ * pr
    return pl.pallas_call(
        functools.partial(bwd_kernel, np_, slots, heads, first),
        grid=(heads,),
        in_specs=specs,
        out_specs=[accs] + [pl.BlockSpec((pr, 2 * heads * HD), lambda h: (0, 0))] * np_,
        out_shape=[jax.ShapeDtypeStruct((heads * HD, span), F32)]
        + [jax.ShapeDtypeStruct((pr, 2 * heads * HD), BF)] * np_,
        cost_estimate=pl.CostEstimate(
            flops=20 * span * keys * HD * heads,
            bytes_accessed=8 * keys * heads * HD,
            transcendentals=span * keys * heads,
        ),
    )(*args)


def turn_back(x, cosine, sine):
    return x * cosine - pltpu.roll(x, HD // 2, 1) * sine


def unrotate_kernel(n, heads, transposed, *refs):
    nd = 1 if transposed else 2
    d_refs = refs[:nd]
    raw_refs = refs[nd : nd + n]
    r_ref, g_ref, cos_ref, sin_ref, w_ref, inner_ref, gain_ref = refs[nd + n :]
    rows = raw_refs[0].shape[0]
    half = n // 2
    for h in range(heads):
        c = slice(h * HD, (h + 1) * HD)
        gain_sum = None
        whole = d_refs[0][c, :].T if transposed else None
        for s in range(n):
            r = slice(s * rows, (s + 1) * rows)
            if transposed:
                d = whole[r, :]
            else:
                o = slice((s % half) * rows, (s % half + 1) * rows)
                d = d_refs[0 if s < half else 1][o, c].astype(F32)
            grad = turn_back(d, cos_ref[r, :], sin_ref[r, :])
            raw = raw_refs[s][:, c]
            weighted = grad * g_ref[:, c]
            w_ref[r, c] = weighted
            t = jnp.sum(weighted * raw, axis=1, keepdims=True)
            inner_ref[r, :] = t if h == 0 else inner_ref[r, :] + t
            u = jnp.sum(grad * raw * r_ref[r, :], axis=0, keepdims=True)
            gain_sum = u if gain_sum is None else gain_sum + u
        gain_ref[:, c] = gain_sum


def unrotate(d, raw, rms, gain, cosine, sine, heads, transposed):
    n = len(raw)
    span = n * raw[0].shape[0]
    units = heads * HD
    return pl.pallas_call(
        functools.partial(unrotate_kernel, n, heads, transposed),
        in_specs=[vmem()] * (len(d) + n + 4),
        out_specs=[vmem()] * 3,
        out_shape=[
            jax.ShapeDtypeStruct((span, units), F32),
            jax.ShapeDtypeStruct((span, 1), F32),
            jax.ShapeDtypeStruct((1, units), F32),
        ],
    )(*d, *raw, rms, gain, cosine, sine)


def norm_back(raw, rms_inv, gain, grad_out):
    weighted = gain * grad_out
    inner = jnp.sum(weighted * raw, axis=1, keepdims=True)
    width = raw.shape[1]
    return (
        rms_inv[:, None] * weighted - raw * (rms_inv * rms_inv * rms_inv)[:, None] * inner / width
    )


def local(
    nc,
    nf,
    block_input,
    positions,
    query_weight,
    key_weight,
    value_weight,
    output_weight,
    query_gain,
    key_gain,
    attn_gain,
    mlp_gain,
    gate_weight,
    up_weight,
    down_weight,
    cotangent,
):
    rows, width = block_input.shape
    span = rows * nf
    units = query_weight.shape[1]
    heads = units // HD
    half = nf // 2
    me_c = lax.axis_index("ctx")
    me_f = lax.axis_index("fsdp")
    unit_start = me_f * units

    x_slots = [block_input]
    begin = positions[:1]
    begins = None
    for s in range(1, nf):
        got = shift(x_slots[-1], nf, 1)
        if s == min(2, nf - 1):
            begin, x_last = lax.optimization_barrier((begin, mm(x_slots[-1], query_weight)))
            begins = jnp.concatenate([begin] + [shift(begin, nf, t) for t in range(1, nf)])[None, :]
            b = 1
            while b < nc:
                begins = jnp.concatenate([begins, swap(begins, nc, b)])
                b *= 2
        if s == nf - 1:
            got, begins = lax.optimization_barrier((got, begins))
        x_slots.append(got)

    row_pos = (begins[0][:, None] + jnp.arange(rows)[None, :]).reshape(span)
    freqs = jnp.exp(-math.log(rope_base) * 2.0 * jnp.arange(HD // 2).astype(F32) / HD)
    angles = row_pos.astype(F32)[:, None] * freqs[None, :]
    cosine, sine = jnp.cos(angles), jnp.sin(angles)
    cosine = jnp.concatenate([cosine, cosine], axis=1)
    sine = jnp.concatenate([-sine, sine], axis=1)
    qpos = row_pos[None, :]

    q_raw = [mm(x, query_weight) for x in x_slots]
    q_raw[min(2, nf - 1) - 1] = x_last
    k_raw = [mm(x, key_weight) for x in x_slots]
    v_raw = [mm(x, value_weight) for x in x_slots]
    squares = jnp.stack(
        [
            jnp.stack([jnp.sum(q * q, axis=1), jnp.sum(k * k, axis=1)])
            for q, k in zip(q_raw, k_raw)
        ]
    )
    squares = slot_sum(squares, nf)
    query_rms = lax.rsqrt(squares[:, 0].reshape(span, 1) / width + norm_eps)
    key_rms = lax.rsqrt(squares[:, 1].reshape(span, 1) / width + norm_eps)
    query_scale = lax.dynamic_slice_in_dim(query_gain, unit_start, units)[None, :]
    key_scale = lax.dynamic_slice_in_dim(key_gain, unit_start, units)[None, :]

    query_rot, kv_a, kv_b = pl.pallas_call(
        functools.partial(prep_kernel, nf, heads),
        in_specs=[vmem()] * (3 * nf + 6),
        out_specs=[vmem()] * 3,
        out_shape=[jax.ShapeDtypeStruct((span, units), BF)]
        + [jax.ShapeDtypeStruct((span // 2, 2 * units), BF)] * 2,
    )(*q_raw, *k_raw, *v_raw, query_rms, key_rms, query_scale, key_scale, cosine, sine)

    orders = bit_orders(nc)
    groups = group_order(nc)
    pieces = [{0: kv_a}, {0: kv_b}]

    def fetch(i, m, token):
        if m not in pieces[i]:
            src, bit = came_from(m, orders[i])
            have = fetch(i, src, token)
            if token is not None:
                have = gate(have, token)
            pieces[i][m] = swap(have, nc, bit)
        return pieces[i][m]

    def group_inputs(group):
        kv = [pieces[0][m] for m in group] + [pieces[1][m] for m in group]
        starts = jnp.concatenate(
            [begins[m, :half] for m in group] + [begins[m, half:] for m in group]
        )
        return starts, kv

    carry = None
    tokens = []
    for group in groups:
        for m in group:
            for i in range(2):
                far = distance(m)
                if far < 2:
                    fetch(i, m, None)
                else:
                    fetch(i, m, tokens[1] if m & 1 else tokens[0])
        starts, kv = group_inputs(group)
        carry = attend(
            starts, query_rot, qpos, kv, carry, heads, half, group is groups[-1]
        )
        tokens.append(carry[0])
    mixture, mixture_b, log_total = carry

    def rows_of(x, s):
        return x[s * rows : (s + 1) * rows]

    attn_out = ring_scatter(lambda s: mm(rows_of(mixture_b, s), output_weight), nf)
    attn_rms = lax.rsqrt(jnp.mean(attn_out * attn_out, axis=1) + norm_eps)
    hidden_state = block_input.astype(F32) + attn_out * attn_rms[:, None] * attn_gain[None, :]
    state_slots = ring_gather(hidden_state.astype(BF), nf)
    gate_pre = [mm(x, gate_weight) for x in state_slots]
    up_pre = [mm(x, up_weight) for x in state_slots]
    activated = [(jax.nn.silu(g) * u).astype(BF) for g, u in zip(gate_pre, up_pre)]
    mlp_out = ring_scatter(lambda s: mm(activated[s], down_weight), nf)
    mlp_rms = lax.rsqrt(jnp.mean(mlp_out * mlp_out, axis=1) + norm_eps)
    block_output = (hidden_state + mlp_out * mlp_rms[:, None] * mlp_gain[None, :]).astype(BF)
    upstream = cotangent.astype(F32)
    mlp_gain_part = jnp.sum(upstream * mlp_out * mlp_rms[:, None], axis=0)
    mlp_grad_b = norm_back(mlp_out, mlp_rms, mlp_gain[None, :], upstream).astype(BF)

    def ctx_scatter(x):
        return lax.psum_scatter(x, "ctx", scatter_dimension=0, tiled=True)

    def slot_grads(s, rows_in):
        activ_grad = contract_cols(rows_in, down_weight)
        sg = jax.nn.sigmoid(gate_pre[s])
        g = (activ_grad * up_pre[s] * sg * (1.0 + gate_pre[s] * (1.0 - sg))).astype(BF)
        return g, (activ_grad * gate_pre[s] * sg).astype(BF)

    def state_part(g, u):
        return contract_cols(g, gate_weight) + contract_cols(u, up_weight)

    grad_slots, gate_grads, up_grads = [mlp_grad_b], [], []
    acc = None
    for s in range(nf):
        got = shift(grad_slots[-1], nf, 1) if s < nf - 1 else None
        g, u = slot_grads(s, grad_slots[s])
        if s == 1:
            acc = state_part(g, u).astype(BF)
        elif s > 1:
            acc = (shift(acc, nf, 1).astype(F32) + state_part(g, u)).astype(BF)
        if got is not None:
            got, g, u = lax.optimization_barrier((got, g, u))
            grad_slots.append(got)
        gate_grads.append(g)
        up_grads.append(u)
    grad_rows = jnp.concatenate(grad_slots)
    activ_rows = jnp.concatenate(activated)
    wide = activ_rows.shape[1] // 2
    down_parts = [
        contract_rows(grad_rows, activ_rows[:, i * wide : (i + 1) * wide]).astype(BF)
        for i in range(2)
    ]
    state_grad = state_part(gate_grads[0], up_grads[0])
    if nf > 1:
        got = shift(acc, nf, 1)
        state_grad = got.astype(F32) + state_grad
    state_grad = upstream + state_grad
    marks = [[] for _ in range(nc)]
    down_grad = jnp.concatenate(
        [
            halving(p, me_c, nc, order, marks)
            for p, order in zip(down_parts, bit_orders(nc))
        ],
        axis=1,
    ).T

    attn_gain_part = jnp.sum(state_grad * attn_out * attn_rms[:, None], axis=0)
    attn_grad_b = norm_back(attn_out, attn_rms, attn_gain[None, :], state_grad).astype(BF)
    gate_up_part = contract_rows(
        jnp.concatenate(state_slots[:-1] + [gate(state_slots[-1], *marks[0])]),
        jnp.concatenate([jnp.concatenate(gate_grads), jnp.concatenate(up_grads)], axis=1),
    ).astype(BF)
    gate_up_sum = ctx_scatter(gate_up_part)
    first_hop = shift(attn_grad_b, nf, 1)
    proj_slots = [attn_grad_b] + ring_gather(first_hop, nf - 1, around=nf)
    proj_slots[-1] = gate(proj_slots[-1], *marks[1])
    mixture_grad_b = jnp.concatenate(
        [contract_cols(x, output_weight).astype(BF) for x in proj_slots]
    )

    dq = None
    sums = [{}, {}]

    def send(i, m):
        into, bit = came_from(m, orders[i])
        got = swap(sums[i].pop(m), nc, bit)
        sums[i][into] = (sums[i][into].astype(F32) + got.astype(F32)).astype(BF)
        return got

    waits = []
    for gi, group in enumerate(groups[::-1]):
        starts, kv = group_inputs(group)
        if gi:
            dq = gate(dq, *waits[gi - 1])
        dq, *out = attend_back(
            starts, query_rot, mixture_grad_b, mixture, log_total, qpos, kv, dq, heads, half
        )
        for m, a, b in zip(group, out[: len(group)], out[len(group) :]):
            sums[0][m], sums[1][m] = a, b
        waits.append([send(i, m) for i in range(2) for m in group if m & 1])
    hops = []
    for far in range(max(distance(m) for m in range(nc)), 0, -1):
        for i in range(2):
            for m in [m for m in sums[i] if distance(m) == far]:
                got = send(i, m)
                if m == orders[i][-1]:
                    hops.append(got)
    dq = gate(dq, *hops)
    own_a, own_b = sums[0][0], sums[1][0]

    def unit_full(x):
        return lax.dynamic_update_slice_in_dim(jnp.zeros((width,), F32), x, unit_start, 0)

    def norm_grads(weighted, inner, raw, rms):
        cube = rms * rms * rms
        return [
            (
                rows_of(rms, s) * rows_of(weighted, s)
                - raw[s] * rows_of(cube, s) * inner[s][:, None] / width
            ).astype(BF)
            for s in range(nf)
        ]

    def spread(*vectors):
        return jnp.stack([v.reshape(nf, width // nf) for v in vectors], axis=1).reshape(nf, -1)

    def gathered(flat, count):
        return flat.reshape(nf, count, width // nf).transpose(1, 0, 2).reshape(count, width)

    query_weighted, query_inner, query_gain_part = unrotate(
        [dq], q_raw, query_rms, query_scale, cosine, sine, heads, True
    )
    query_inner, early_gains = slot_sum(
        query_inner.reshape(nf, rows),
        nf,
        spread(unit_full(query_gain_part[0]), attn_gain_part, mlp_gain_part),
    )
    query_grads = norm_grads(query_weighted, query_inner, q_raw, query_rms)

    x_rows = jnp.concatenate(x_slots)
    q_part = contract_rows(x_rows, jnp.concatenate(query_grads)).astype(BF)
    o_part = contract_rows(jnp.concatenate(proj_slots), mixture_b).astype(BF)
    qo_part = jnp.concatenate([q_part, o_part], axis=1)
    qo_part, gate_up_sum, own_a, own_b = lax.optimization_barrier(
        (qo_part, gate_up_sum, own_a, own_b)
    )
    qo_grad = ctx_scatter(qo_part).astype(F32)
    query_grad, output_grad = qo_grad[:, :units], qo_grad[:, units:].T

    key_weighted, key_inner, key_gain_part = unrotate(
        [own_a, own_b], k_raw, key_rms, key_scale, cosine, sine, heads, False
    )
    key_inner, key_gain_sum = slot_sum(
        key_inner.reshape(nf, rows), nf, spread(unit_full(key_gain_part[0]))
    )
    key_grads = norm_grads(key_weighted, key_inner, k_raw, key_rms)
    own = jnp.concatenate([own_a[:, units:], own_b[:, units:]])
    value_grads = [rows_of(own, s) for s in range(nf)]

    started = []
    input_grad = state_grad + ring_scatter(
        lambda s: contract_cols(query_grads[s], query_weight)
        + contract_cols(key_grads[s], key_weight)
        + contract_cols(value_grads[s], value_weight),
        nf,
        started=started,
    )
    k_rows, v_rows, *_ = lax.optimization_barrier((jnp.concatenate(key_grads), own, *started))
    k_part = contract_rows(x_rows, k_rows).astype(BF)
    v_part = contract_rows(x_rows, v_rows).astype(BF)
    key_grad = halving(k_part, me_c, nc, orders[0])
    value_grad = halving(v_part, me_c, nc, orders[1])
    gains = jnp.concatenate([gathered(early_gains, 3), gathered(key_gain_sum, 1)])
    gains_own = halving(gains.T, me_c, nc, orders[0]).T
    ff = gate_weight.shape[1]
    gate_up = gate_up_sum.astype(F32)
    gate_grad, up_grad = gate_up[:, :ff], gate_up[:, ff:]
    return (
        block_output,
        input_grad,
        query_grad,
        key_grad,
        value_grad,
        output_grad,
        gains_own[0],
        gains_own[3],
        gains_own[1],
        gains_own[2],
        gate_grad,
        up_grad,
        down_grad,
    )


def solution(mesh):
    def layer(*args):
        return local(mesh.shape["ctx"], mesh.shape["fsdp"], *args)

    return jax.shard_map(
        layer,
        mesh=mesh,
        in_specs=(
            P(("ctx", "fsdp"), None),
            P(("ctx", "fsdp")),
            P(None, "fsdp"),
            P(None, "fsdp"),
            P(None, "fsdp"),
            P("fsdp", None),
            P(),
            P(),
            P(),
            P(),
            P(None, "fsdp"),
            P(None, "fsdp"),
            P("fsdp", None),
            P(("ctx", "fsdp"), None),
        ),
        out_specs=(
            P(("ctx", "fsdp"), None),
            P(("ctx", "fsdp"), None),
            P("ctx", "fsdp"),
            P("ctx", "fsdp"),
            P("ctx", "fsdp"),
            P("fsdp", "ctx"),
            P("ctx"),
            P("ctx"),
            P("ctx"),
            P("ctx"),
            P("ctx", "fsdp"),
            P("ctx", "fsdp"),
            P("fsdp", "ctx"),
        ),
        check_vma=False,
    )
```

```python
import functools
import math

import jax
import jax.numpy as jnp
from jax import lax
from jax.experimental import pallas as pl
from jax.experimental.pallas import tpu as pltpu
from jax.sharding import PartitionSpec as P


HD = 128
norm_eps = 1e-06
rope_base = 500000.0
big_negative = -1e30
LOG2E = math.log2(math.e)
BF = jnp.bfloat16
F32 = jnp.float32


def mm(left, right):
    return jnp.dot(left, right, preferred_element_type=F32)


def contract_rows(left, right):
    return lax.dot_general(left, right, (((0,), (0,)), ((), ())), preferred_element_type=F32)


def contract_cols(left, right):
    return lax.dot_general(left, right, (((1,), (1,)), ((), ())), preferred_element_type=F32)


def gate(x, *tokens):
    return lax.optimization_barrier((x, *tokens))[0]


def shift(x, n, by):
    return lax.ppermute(x, "fsdp", [(i, (i + by) % n) for i in range(n)])


def ring_gather(x, n):
    slots = [x]
    for _ in range(n - 1):
        slots.append(shift(slots[-1], n, 1))
    return slots


def ring_scatter(part, n, under=(), started=None):
    if n == 1:
        return part(0)
    acc = part(1).astype(BF)
    if started is not None:
        started.append(acc)
    for s in range(2, n):
        acc = (shift(acc, n, 1).astype(F32) + part(s)).astype(BF)
    return gate(shift(acc, n, 1), *under).astype(F32) + part(0)


def slot_sum(x, n, flat=None):
    total, flat_total = x, flat
    cut = x.shape[-1]
    both = x if flat is None else jnp.concatenate([x, flat], axis=-1)
    for t in range(1, n):
        got = shift(both, n, t)
        total = total + jnp.roll(got[..., :cut], t, axis=0)
        if flat is not None:
            flat_total = flat_total + got[..., cut:]
    return total if flat is None else (total, flat_total)


def swap(x, n, bit):
    return lax.ppermute(x, "ctx", [(i, i ^ bit) for i in range(n)])


def bit_orders(n):
    bits = []
    b = 2
    while b < n:
        bits.append(b)
        b *= 2
    return bits, bits[::-1]


def halving(part, me, n, order, marks=None):
    seq = ([1] if n > 1 else []) + list(order[::-1])
    block = part.shape[0] // n
    levels = len(seq)
    masks = [
        sum(seq[k] for k in range(levels) if t >> (levels - 1 - k) & 1) for t in range(n)
    ]

    def blocks(ms):
        return jnp.concatenate(
            [lax.dynamic_slice_in_dim(part, (me ^ m) * block, block) for m in ms]
        )

    keep, away = blocks(masks[: n // 2]), blocks(masks[n // 2 :])
    for k, bit in enumerate(seq):
        got = swap(away.astype(BF), n, bit)
        total = keep.astype(F32) + got.astype(F32)
        rest = total.shape[0] // 2
        if k < levels - 1:
            total = total.astype(BF)
            if marks is not None:
                marks[k].append(total)
            keep, away = total[:rest], total[rest:]
    return total


def distance(m):
    return bin(m >> 1).count("1")


def group_order(n):
    pairs = [(m, m + 1) if n > 1 else (m,) for m in range(0, n, 2)]
    return sorted(pairs, key=lambda g: (distance(g[0]), g[0]))


def came_from(m, order):
    if m & 1:
        return m ^ 1, 1
    bit = [b for b in order if m & b][-1]
    return m ^ bit, bit


def vmem(*_):
    return pl.BlockSpec(memory_space=pltpu.VMEM)


def prep_kernel(n, heads, *refs):
    q_refs, k_refs, v_refs = refs[:n], refs[n : 2 * n], refs[2 * n : 3 * n]
    qr_ref, kr_ref, qg_ref, kg_ref, cos_ref, sin_ref = refs[3 * n : 3 * n + 6]
    qo_ref, kva_ref, kvb_ref = refs[3 * n + 6 :]
    rows = q_refs[0].shape[0]
    half = n // 2
    for s in range(n):
        r = slice(s * rows, (s + 1) * rows)
        cosine, sine = cos_ref[r, :], sin_ref[r, :]
        out = kva_ref if s < half else kvb_ref
        o = slice((s % half) * rows, (s % half + 1) * rows)
        for h in range(heads):
            c = slice(h * HD, (h + 1) * HD)
            x = q_refs[s][:, c] * qr_ref[r, :] * qg_ref[:, c]
            qo_ref[r, c] = (x * cosine + pltpu.roll(x, HD // 2, 1) * sine).astype(BF)
            y = k_refs[s][:, c] * kr_ref[r, :] * kg_ref[:, c]
            out[o, c] = (y * cosine + pltpu.roll(y, HD // 2, 1) * sine).astype(BF)
            out[o, heads * HD + h * HD : heads * HD + (h + 1) * HD] = v_refs[s][:, c].astype(BF)


def key_mask(starts_ref, piece, slots, rows, qpos):
    parts = []
    for j in range(slots):
        row = lax.broadcasted_iota(jnp.int32, (rows, 1), 0)
        parts.append(row + starts_ref[piece * slots + j])
    return jnp.concatenate(parts, axis=0) <= qpos


def fwd_kernel(npieces, slots, first, last, *refs):
    starts_ref, q_ref, qpos_ref = refs[:3]
    k_refs = refs[3 : 3 + npieces]
    v_refs = refs[3 + npieces : 3 + 2 * npieces]
    rest = refs[3 + 2 * npieces :]
    if not first:
        m_in, l_in, a_in = rest[:3]
        rest = rest[3:]
    rows = k_refs[0].shape[0] // slots
    c2 = LOG2E / math.sqrt(HD)
    q = q_ref[...]
    qpos = qpos_ref[...]
    scores = []
    top = None if first else m_in[0]
    for i in range(npieces):
        s = contract_cols(k_refs[i][...], q)
        s = jnp.where(key_mask(starts_ref, i, slots, rows, qpos), s, big_negative)
        scores.append(s)
        t = jnp.max(s, axis=0, keepdims=True)
        top = t if top is None else jnp.maximum(top, t)
    total = None
    acc = None
    for i in range(npieces):
        p = jnp.exp2((scores[i] - top) * c2)
        t = jnp.sum(p, axis=0, keepdims=True)
        a = contract_rows(v_refs[i][...], p.astype(BF))
        total = t if total is None else total + t
        acc = a if acc is None else acc + a
    if not first:
        alpha = jnp.exp2((m_in[0] - top) * c2)
        total = total + l_in[0] * alpha
        acc = acc + a_in[...] * alpha
    if last:
        mix_ref, mixb_ref, log_ref = rest
        mix = (acc / total).T
        mix_ref[...] = mix
        mixb_ref[...] = mix.astype(BF)
        log_ref[0] = top * c2 + jnp.log2(total)
    else:
        m_out, l_out, a_out = rest
        m_out[0] = top
        l_out[0] = total
        a_out[...] = acc


def attend(starts, q, qpos, kv, carry, heads, slots, last):
    span = q.shape[0]
    first = carry is None
    np_ = len(kv)
    pr = kv[0].shape[0]
    row = pl.BlockSpec((1, 1, span), lambda h: (h, 0, 0))
    accs = pl.BlockSpec((HD, span), lambda h: (h, 0))
    specs = [
        pl.BlockSpec(memory_space=pltpu.SMEM),
        pl.BlockSpec((span, HD), lambda h: (0, h)),
        pl.BlockSpec((1, span), lambda h: (0, 0)),
    ]
    specs += [pl.BlockSpec((pr, HD), lambda h: (0, h))] * np_
    specs += [pl.BlockSpec((pr, HD), lambda h: (0, heads + h))] * np_
    args = [starts, q, qpos, *kv, *kv]
    if not first:
        specs += [row, row, accs]
        args += list(carry)
    rshape = jax.ShapeDtypeStruct((heads, 1, span), F32)
    if last:
        mix = pl.BlockSpec((span, HD), lambda h: (0, h))
        outs = [mix, mix, row]
        shapes = [
            jax.ShapeDtypeStruct((span, heads * HD), F32),
            jax.ShapeDtypeStruct((span, heads * HD), BF),
            rshape,
        ]
    else:
        outs = [row, row, accs]
        shapes = [rshape, rshape, jax.ShapeDtypeStruct((heads * HD, span), F32)]
    keys = np_ * pr
    return pl.pallas_call(
        functools.partial(fwd_kernel, np_, slots, first, last),
        grid=(heads,),
        in_specs=specs,
        out_specs=outs,
        out_shape=shapes,
        cost_estimate=pl.CostEstimate(
            flops=8 * span * keys * HD * heads,
            bytes_accessed=4 * keys * heads * HD,
            transcendentals=span * keys * heads,
        ),
    )(*args)


def bwd_kernel(npieces, slots, heads, first, *refs):
    starts_ref, q_ref, do_ref, mix_ref, log_ref, qpos_ref = refs[:6]
    k_refs = refs[6 : 6 + npieces]
    v_refs = refs[6 + npieces : 6 + 2 * npieces]
    rest = refs[6 + 2 * npieces :]
    if not first:
        dq_in = rest[0]
        rest = rest[1:]
    dq_ref, out_refs = rest[0], rest[1:]
    h = pl.program_id(0)
    rows = k_refs[0].shape[0] // slots
    scale = 1.0 / math.sqrt(HD)
    c2 = LOG2E * scale
    q = q_ref[...]
    do = do_ref[...]
    delta = jnp.sum((do.astype(F32) * mix_ref[...]).T, axis=0, keepdims=True)
    log2 = log_ref[0]
    qpos = qpos_ref[...]
    dq = None
    for i in range(npieces):
        k = k_refs[i][...]
        s = contract_cols(k, q) * c2 - log2
        s = jnp.where(key_mask(starts_ref, i, slots, rows, qpos), s, big_negative)
        p = jnp.exp2(s)
        dp = contract_cols(v_refs[i][...], do)
        ds = (p * (dp - delta)).astype(BF)
        t = contract_rows(k, ds)
        dq = t if dq is None else dq + t
        kc = pl.ds(pl.multiple_of(h * HD, HD), HD)
        vc = pl.ds(pl.multiple_of((heads + h) * HD, HD), HD)
        out_refs[i][:, kc] = (mm(ds, q) * scale).astype(BF)
        out_refs[i][:, vc] = mm(p.astype(BF), do).astype(BF)
    dq = dq * scale
    dq_ref[...] = dq if first else dq + dq_in[...]


def attend_back(starts, q, do, mix, log, qpos, kv, dq, heads, slots):
    span = q.shape[0]
    first = dq is None
    np_ = len(kv)
    pr = kv[0].shape[0]
    head = pl.BlockSpec((span, HD), lambda h: (0, h))
    accs = pl.BlockSpec((HD, span), lambda h: (h, 0))
    specs = [
        pl.BlockSpec(memory_space=pltpu.SMEM),
        head,
        head,
        head,
        pl.BlockSpec((1, 1, span), lambda h: (h, 0, 0)),
        pl.BlockSpec((1, span), lambda h: (0, 0)),
    ]
    specs += [pl.BlockSpec((pr, HD), lambda h: (0, h))] * np_
    specs += [pl.BlockSpec((pr, HD), lambda h: (0, heads + h))] * np_
    args = [starts, q, do, mix, log, qpos, *kv, *kv]
    if not first:
        specs.append(accs)
        args.append(dq)
    keys = np_ * pr
    return pl.pallas_call(
        functools.partial(bwd_kernel, np_, slots, heads, first),
        grid=(heads,),
        in_specs=specs,
        out_specs=[accs] + [pl.BlockSpec((pr, 2 * heads * HD), lambda h: (0, 0))] * np_,
        out_shape=[jax.ShapeDtypeStruct((heads * HD, span), F32)]
        + [jax.ShapeDtypeStruct((pr, 2 * heads * HD), BF)] * np_,
        cost_estimate=pl.CostEstimate(
            flops=20 * span * keys * HD * heads,
            bytes_accessed=8 * keys * heads * HD,
            transcendentals=span * keys * heads,
        ),
    )(*args)


def turn_back(x, cosine, sine):
    return x * cosine - pltpu.roll(x, HD // 2, 1) * sine


def unrotate_kernel(n, heads, transposed, *refs):
    nd = 1 if transposed else 2
    d_refs = refs[:nd]
    raw_refs = refs[nd : nd + n]
    r_ref, g_ref, cos_ref, sin_ref, w_ref, inner_ref, gain_ref = refs[nd + n :]
    rows = raw_refs[0].shape[0]
    half = n // 2
    for h in range(heads):
        c = slice(h * HD, (h + 1) * HD)
        gain_sum = None
        whole = d_refs[0][c, :].T if transposed else None
        for s in range(n):
            r = slice(s * rows, (s + 1) * rows)
            if transposed:
                d = whole[r, :]
            else:
                o = slice((s % half) * rows, (s % half + 1) * rows)
                d = d_refs[0 if s < half else 1][o, c].astype(F32)
            grad = turn_back(d, cos_ref[r, :], sin_ref[r, :])
            raw = raw_refs[s][:, c]
            weighted = grad * g_ref[:, c]
            w_ref[r, c] = weighted
            t = jnp.sum(weighted * raw, axis=1, keepdims=True)
            inner_ref[r, :] = t if h == 0 else inner_ref[r, :] + t
            u = jnp.sum(grad * raw * r_ref[r, :], axis=0, keepdims=True)
            gain_sum = u if gain_sum is None else gain_sum + u
        gain_ref[:, c] = gain_sum


def unrotate(d, raw, rms, gain, cosine, sine, heads, transposed):
    n = len(raw)
    span = n * raw[0].shape[0]
    units = heads * HD
    return pl.pallas_call(
        functools.partial(unrotate_kernel, n, heads, transposed),
        in_specs=[vmem()] * (len(d) + n + 4),
        out_specs=[vmem()] * 3,
        out_shape=[
            jax.ShapeDtypeStruct((span, units), F32),
            jax.ShapeDtypeStruct((span, 1), F32),
            jax.ShapeDtypeStruct((1, units), F32),
        ],
    )(*d, *raw, rms, gain, cosine, sine)


def norm_back(raw, rms_inv, gain, grad_out):
    weighted = gain * grad_out
    inner = jnp.sum(weighted * raw, axis=1, keepdims=True)
    width = raw.shape[1]
    return (
        rms_inv[:, None] * weighted - raw * (rms_inv * rms_inv * rms_inv)[:, None] * inner / width
    )


def local(
    nc,
    nf,
    block_input,
    positions,
    query_weight,
    key_weight,
    value_weight,
    output_weight,
    query_gain,
    key_gain,
    attn_gain,
    mlp_gain,
    gate_weight,
    up_weight,
    down_weight,
    cotangent,
):
    rows, width = block_input.shape
    span = rows * nf
    units = query_weight.shape[1]
    heads = units // HD
    half = nf // 2
    me_c = lax.axis_index("ctx")
    me_f = lax.axis_index("fsdp")
    unit_start = me_f * units

    x_slots = [block_input]
    begin = positions[:1]
    begins = None
    for s in range(1, nf):
        got = shift(x_slots[-1], nf, 1)
        if s == min(2, nf - 1):
            begin, x_last = lax.optimization_barrier((begin, mm(x_slots[-1], query_weight)))
            begins = jnp.concatenate([begin] + [shift(begin, nf, t) for t in range(1, nf)])[None, :]
            b = 1
            while b < nc:
                begins = jnp.concatenate([begins, swap(begins, nc, b)])
                b *= 2
        if s == nf - 1:
            got, begins = lax.optimization_barrier((got, begins))
        x_slots.append(got)

    row_pos = (begins[0][:, None] + jnp.arange(rows)[None, :]).reshape(span)
    freqs = jnp.exp(-math.log(rope_base) * 2.0 * jnp.arange(HD // 2).astype(F32) / HD)
    angles = row_pos.astype(F32)[:, None] * freqs[None, :]
    cosine, sine = jnp.cos(angles), jnp.sin(angles)
    cosine = jnp.concatenate([cosine, cosine], axis=1)
    sine = jnp.concatenate([-sine, sine], axis=1)
    qpos = row_pos[None, :]

    q_raw = [mm(x, query_weight) for x in x_slots]
    q_raw[min(2, nf - 1) - 1] = x_last
    k_raw = [mm(x, key_weight) for x in x_slots]
    v_raw = [mm(x, value_weight) for x in x_slots]
    squares = jnp.stack(
        [
            jnp.stack([jnp.sum(q * q, axis=1), jnp.sum(k * k, axis=1)])
            for q, k in zip(q_raw, k_raw)
        ]
    )
    squares = slot_sum(squares, nf)
    query_rms = lax.rsqrt(squares[:, 0].reshape(span, 1) / width + norm_eps)
    key_rms = lax.rsqrt(squares[:, 1].reshape(span, 1) / width + norm_eps)
    query_scale = lax.dynamic_slice_in_dim(query_gain, unit_start, units)[None, :]
    key_scale = lax.dynamic_slice_in_dim(key_gain, unit_start, units)[None, :]

    query_rot, kv_a, kv_b = pl.pallas_call(
        functools.partial(prep_kernel, nf, heads),
        in_specs=[vmem()] * (3 * nf + 6),
        out_specs=[vmem()] * 3,
        out_shape=[jax.ShapeDtypeStruct((span, units), BF)]
        + [jax.ShapeDtypeStruct((span // 2, 2 * units), BF)] * 2,
    )(*q_raw, *k_raw, *v_raw, query_rms, key_rms, query_scale, key_scale, cosine, sine)

    orders = bit_orders(nc)
    groups = group_order(nc)
    pieces = [{0: kv_a}, {0: kv_b}]

    def fetch(i, m, token):
        if m not in pieces[i]:
            src, bit = came_from(m, orders[i])
            have = fetch(i, src, token)
            if token is not None:
                have = gate(have, token)
            pieces[i][m] = swap(have, nc, bit)
        return pieces[i][m]

    def group_inputs(group):
        kv = [pieces[0][m] for m in group] + [pieces[1][m] for m in group]
        starts = jnp.concatenate(
            [begins[m, :half] for m in group] + [begins[m, half:] for m in group]
        )
        return starts, kv

    carry = None
    tokens = []
    for group in groups:
        for m in group:
            for i in range(2):
                far = distance(m)
                if far < 2:
                    fetch(i, m, None)
                else:
                    fetch(i, m, tokens[1] if m & 1 else tokens[0])
        starts, kv = group_inputs(group)
        carry = attend(
            starts, query_rot, qpos, kv, carry, heads, half, group is groups[-1]
        )
        tokens.append(carry[0])
    mixture, mixture_b, log_total = carry

    def rows_of(x, s):
        return x[s * rows : (s + 1) * rows]

    attn_out = ring_scatter(lambda s: mm(rows_of(mixture_b, s), output_weight), nf)
    attn_rms = lax.rsqrt(jnp.mean(attn_out * attn_out, axis=1) + norm_eps)
    hidden_state = block_input.astype(F32) + attn_out * attn_rms[:, None] * attn_gain[None, :]
    state_slots = ring_gather(hidden_state.astype(BF), nf)
    gate_pre = [mm(x, gate_weight) for x in state_slots]
    up_pre = [mm(x, up_weight) for x in state_slots]
    activated = [(jax.nn.silu(g) * u).astype(BF) for g, u in zip(gate_pre, up_pre)]
    mlp_out = ring_scatter(lambda s: mm(activated[s], down_weight), nf)
    mlp_rms = lax.rsqrt(jnp.mean(mlp_out * mlp_out, axis=1) + norm_eps)
    block_output = (hidden_state + mlp_out * mlp_rms[:, None] * mlp_gain[None, :]).astype(BF)
    upstream = cotangent.astype(F32)
    mlp_gain_part = jnp.sum(upstream * mlp_out * mlp_rms[:, None], axis=0)
    mlp_grad_b = norm_back(mlp_out, mlp_rms, mlp_gain[None, :], upstream).astype(BF)

    def ctx_scatter(x):
        return lax.psum_scatter(x, "ctx", scatter_dimension=0, tiled=True)

    def slot_grads(s, rows_in):
        activ_grad = contract_cols(rows_in, down_weight)
        sg = jax.nn.sigmoid(gate_pre[s])
        g = (activ_grad * up_pre[s] * sg * (1.0 + gate_pre[s] * (1.0 - sg))).astype(BF)
        return g, (activ_grad * gate_pre[s] * sg).astype(BF)

    def state_part(g, u):
        return contract_cols(g, gate_weight) + contract_cols(u, up_weight)

    grad_slots, gate_grads, up_grads = [mlp_grad_b], [], []
    acc = None
    for s in range(nf):
        got = shift(grad_slots[-1], nf, 1) if s < nf - 1 else None
        g, u = slot_grads(s, grad_slots[s])
        if s == 1:
            acc = state_part(g, u).astype(BF)
        elif s > 1:
            acc = (shift(acc, nf, 1).astype(F32) + state_part(g, u)).astype(BF)
        if got is not None:
            got, g, u = lax.optimization_barrier((got, g, u))
            grad_slots.append(got)
        gate_grads.append(g)
        up_grads.append(u)
    grad_rows = jnp.concatenate(grad_slots)
    activ_rows = jnp.concatenate(activated)
    wide = activ_rows.shape[1] // 2
    down_parts = [
        contract_rows(grad_rows, activ_rows[:, i * wide : (i + 1) * wide]).astype(BF)
        for i in range(2)
    ]
    state_grad = state_part(gate_grads[0], up_grads[0])
    if nf > 1:
        got = shift(acc, nf, 1)
        state_grad = got.astype(F32) + state_grad
    state_grad = upstream + state_grad
    marks = [[] for _ in range(nc)]
    down_grad = jnp.concatenate(
        [
            halving(p, me_c, nc, order, marks)
            for p, order in zip(down_parts, bit_orders(nc))
        ],
        axis=1,
    ).T

    attn_gain_part = jnp.sum(state_grad * attn_out * attn_rms[:, None], axis=0)
    attn_grad_b = norm_back(attn_out, attn_rms, attn_gain[None, :], state_grad).astype(BF)
    gate_up_part = contract_rows(
        jnp.concatenate(state_slots),
        jnp.concatenate([jnp.concatenate(gate_grads), jnp.concatenate(up_grads)], axis=1),
    ).astype(BF)
    gate_up_sum = ctx_scatter(gate_up_part)
    first_hop = shift(attn_grad_b, nf, 1)
    proj_slots = [attn_grad_b, first_hop]
    for s in range(2, nf):
        got = shift(proj_slots[-1], nf, 1)
        proj_slots.append(gate(got, *marks[0]) if s == 2 else got)
    mixture_grad_b = jnp.concatenate(
        [contract_cols(x, output_weight).astype(BF) for x in proj_slots]
    )

    dq = None
    sums = [{}, {}]

    def send(i, m):
        into, bit = came_from(m, orders[i])
        got = swap(sums[i].pop(m), nc, bit)
        sums[i][into] = (sums[i][into].astype(F32) + got.astype(F32)).astype(BF)
        return got

    waits = []
    for gi, group in enumerate(groups[::-1]):
        starts, kv = group_inputs(group)
        if gi:
            dq = gate(dq, *waits[gi - 1], *(marks[1] if gi == 1 else []))
        dq, *out = attend_back(
            starts, query_rot, mixture_grad_b, mixture, log_total, qpos, kv, dq, heads, half
        )
        for m, a, b in zip(group, out[: len(group)], out[len(group) :]):
            sums[0][m], sums[1][m] = a, b
        waits.append([send(i, m) for i in range(2) for m in group if m & 1])
    for far in range(max(distance(m) for m in range(nc)), 0, -1):
        for i in range(2):
            for m in [m for m in sums[i] if distance(m) == far]:
                send(i, m)
    own_a, own_b = sums[0][0], sums[1][0]

    def unit_full(x):
        return lax.dynamic_update_slice_in_dim(jnp.zeros((width,), F32), x, unit_start, 0)

    def norm_grads(weighted, inner, raw, rms):
        cube = rms * rms * rms
        return [
            (
                rows_of(rms, s) * rows_of(weighted, s)
                - raw[s] * rows_of(cube, s) * inner[s][:, None] / width
            ).astype(BF)
            for s in range(nf)
        ]

    def spread(*vectors):
        return jnp.stack([v.reshape(nf, width // nf) for v in vectors], axis=1).reshape(nf, -1)

    def gathered(flat, count):
        return flat.reshape(nf, count, width // nf).transpose(1, 0, 2).reshape(count, width)

    query_weighted, query_inner, query_gain_part = unrotate(
        [dq], q_raw, query_rms, query_scale, cosine, sine, heads, True
    )
    query_inner, early_gains = slot_sum(
        query_inner.reshape(nf, rows),
        nf,
        spread(unit_full(query_gain_part[0]), attn_gain_part, mlp_gain_part),
    )
    query_grads = norm_grads(query_weighted, query_inner, q_raw, query_rms)

    x_rows = jnp.concatenate(x_slots)
    q_part = contract_rows(x_rows, jnp.concatenate(query_grads)).astype(BF)
    o_part = contract_rows(jnp.concatenate(proj_slots), mixture_b).astype(BF)
    qo_part = jnp.concatenate([q_part, o_part], axis=1)
    gate_up_sum, own_a, own_b = lax.optimization_barrier((gate_up_sum, own_a, own_b))
    qo_part, gate_up_sum = lax.optimization_barrier((qo_part, gate_up_sum))
    qo_grad = ctx_scatter(qo_part).astype(F32)
    query_grad, output_grad = qo_grad[:, :units], qo_grad[:, units:].T

    key_weighted, key_inner, key_gain_part = unrotate(
        [own_a, own_b], k_raw, key_rms, key_scale, cosine, sine, heads, False
    )
    key_inner, key_gain_sum = slot_sum(
        key_inner.reshape(nf, rows), nf, spread(unit_full(key_gain_part[0]))
    )
    key_grads = norm_grads(key_weighted, key_inner, k_raw, key_rms)
    own = jnp.concatenate([own_a[:, units:], own_b[:, units:]])
    value_grads = [rows_of(own, s) for s in range(nf)]

    started = []
    input_grad = state_grad + ring_scatter(
        lambda s: contract_cols(query_grads[s], query_weight)
        + contract_cols(key_grads[s], key_weight)
        + contract_cols(value_grads[s], value_weight),
        nf,
        started=started,
    )
    k_rows, v_rows, *_ = lax.optimization_barrier((jnp.concatenate(key_grads), own, *started))
    k_part = contract_rows(x_rows, k_rows).astype(BF)
    v_part = contract_rows(x_rows, v_rows).astype(BF)
    key_grad = halving(k_part, me_c, nc, orders[0])
    value_grad = halving(v_part, me_c, nc, orders[1])
    gains = jnp.concatenate([gathered(early_gains, 3), gathered(key_gain_sum, 1)])
    gains_own = halving(gains.T, me_c, nc, orders[0]).T
    ff = gate_weight.shape[1]
    gate_up = gate_up_sum.astype(F32)
    gate_grad, up_grad = gate_up[:, :ff], gate_up[:, ff:]
    return (
        block_output,
        input_grad,
        query_grad,
        key_grad,
        value_grad,
        output_grad,
        gains_own[0],
        gains_own[3],
        gains_own[1],
        gains_own[2],
        gate_grad,
        up_grad,
        down_grad,
    )


def solution(mesh):
    def layer(*args):
        return local(mesh.shape["ctx"], mesh.shape["fsdp"], *args)

    return jax.shard_map(
        layer,
        mesh=mesh,
        in_specs=(
            P(("ctx", "fsdp"), None),
            P(("ctx", "fsdp")),
            P(None, "fsdp"),
            P(None, "fsdp"),
            P(None, "fsdp"),
            P("fsdp", None),
            P(),
            P(),
            P(),
            P(),
            P(None, "fsdp"),
            P(None, "fsdp"),
            P("fsdp", None),
            P(("ctx", "fsdp"), None),
        ),
        out_specs=(
            P(("ctx", "fsdp"), None),
            P(("ctx", "fsdp"), None),
            P("ctx", "fsdp"),
            P("ctx", "fsdp"),
            P("ctx", "fsdp"),
            P("fsdp", "ctx"),
            P("ctx"),
            P("ctx"),
            P("ctx"),
            P("ctx"),
            P("ctx", "fsdp"),
            P("ctx", "fsdp"),
            P("fsdp", "ctx"),
        ),
        check_vma=False,
    )
```

```python
import functools
import math

import jax
import jax.numpy as jnp
from jax import lax
from jax.experimental import pallas as pl
from jax.experimental.pallas import tpu as pltpu
from jax.sharding import PartitionSpec as P


HD = 128
norm_eps = 1e-06
rope_base = 500000.0
big_negative = -1e30
LOG2E = math.log2(math.e)
BF = jnp.bfloat16
F32 = jnp.float32


def mm(left, right):
    return jnp.dot(left, right, preferred_element_type=F32)


def contract_rows(left, right):
    return lax.dot_general(left, right, (((0,), (0,)), ((), ())), preferred_element_type=F32)


def contract_cols(left, right):
    return lax.dot_general(left, right, (((1,), (1,)), ((), ())), preferred_element_type=F32)


def gate(x, *tokens):
    return lax.optimization_barrier((x, *tokens))[0]


def shift(x, n, by):
    return lax.ppermute(x, "fsdp", [(i, (i + by) % n) for i in range(n)])


def ring_gather(x, n):
    slots = [x]
    for _ in range(n - 1):
        slots.append(shift(slots[-1], n, 1))
    return slots


def ring_scatter(part, n, under=(), started=None):
    if n == 1:
        return part(0)
    acc = part(1).astype(BF)
    if started is not None:
        started.append(acc)
    for s in range(2, n):
        acc = (shift(acc, n, 1).astype(F32) + part(s)).astype(BF)
    return gate(shift(acc, n, 1), *under).astype(F32) + part(0)


def slot_sum(x, n, flat=None):
    total, flat_total = x, flat
    cut = x.shape[-1]
    both = x if flat is None else jnp.concatenate([x, flat], axis=-1)
    for t in range(1, n):
        got = shift(both, n, t)
        total = total + jnp.roll(got[..., :cut], t, axis=0)
        if flat is not None:
            flat_total = flat_total + got[..., cut:]
    return total if flat is None else (total, flat_total)


def swap(x, n, bit):
    return lax.ppermute(x, "ctx", [(i, i ^ bit) for i in range(n)])


def bit_orders(n):
    bits = []
    b = 2
    while b < n:
        bits.append(b)
        b *= 2
    return bits, bits[::-1]


def halving(part, me, n, order, marks=None):
    seq = ([1] if n > 1 else []) + list(order[::-1])
    block = part.shape[0] // n
    levels = len(seq)
    masks = [
        sum(seq[k] for k in range(levels) if t >> (levels - 1 - k) & 1) for t in range(n)
    ]

    def blocks(ms):
        return jnp.concatenate(
            [lax.dynamic_slice_in_dim(part, (me ^ m) * block, block) for m in ms]
        )

    keep, away = blocks(masks[: n // 2]), blocks(masks[n // 2 :])
    for k, bit in enumerate(seq):
        got = swap(away.astype(BF), n, bit)
        total = keep.astype(F32) + got.astype(F32)
        rest = total.shape[0] // 2
        if k < levels - 1:
            total = total.astype(BF)
            if marks is not None:
                marks[k].append(total)
            keep, away = total[:rest], total[rest:]
    return total


def distance(m):
    return bin(m >> 1).count("1")


def group_order(n):
    pairs = [(m, m + 1) if n > 1 else (m,) for m in range(0, n, 2)]
    return sorted(pairs, key=lambda g: (distance(g[0]), g[0]))


def came_from(m, order):
    if m & 1:
        return m ^ 1, 1
    bit = [b for b in order if m & b][-1]
    return m ^ bit, bit


def vmem(*_):
    return pl.BlockSpec(memory_space=pltpu.VMEM)


def prep_kernel(n, heads, *refs):
    q_refs, k_refs, v_refs = refs[:n], refs[n : 2 * n], refs[2 * n : 3 * n]
    qr_ref, kr_ref, qg_ref, kg_ref, cos_ref, sin_ref = refs[3 * n : 3 * n + 6]
    qo_ref, kva_ref, kvb_ref = refs[3 * n + 6 :]
    rows = q_refs[0].shape[0]
    half = n // 2
    for s in range(n):
        r = slice(s * rows, (s + 1) * rows)
        cosine, sine = cos_ref[r, :], sin_ref[r, :]
        out = kva_ref if s < half else kvb_ref
        o = slice((s % half) * rows, (s % half + 1) * rows)
        for h in range(heads):
            c = slice(h * HD, (h + 1) * HD)
            x = q_refs[s][:, c] * qr_ref[r, :] * qg_ref[:, c]
            qo_ref[r, c] = (x * cosine + pltpu.roll(x, HD // 2, 1) * sine).astype(BF)
            y = k_refs[s][:, c] * kr_ref[r, :] * kg_ref[:, c]
            out[o, c] = (y * cosine + pltpu.roll(y, HD // 2, 1) * sine).astype(BF)
            out[o, heads * HD + h * HD : heads * HD + (h + 1) * HD] = v_refs[s][:, c].astype(BF)


def key_mask(starts_ref, piece, slots, rows, qpos):
    parts = []
    for j in range(slots):
        row = lax.broadcasted_iota(jnp.int32, (rows, 1), 0)
        parts.append(row + starts_ref[piece * slots + j])
    return jnp.concatenate(parts, axis=0) <= qpos


def fwd_kernel(npieces, slots, first, last, *refs):
    starts_ref, q_ref, qpos_ref = refs[:3]
    k_refs = refs[3 : 3 + npieces]
    v_refs = refs[3 + npieces : 3 + 2 * npieces]
    rest = refs[3 + 2 * npieces :]
    if not first:
        m_in, l_in, a_in = rest[:3]
        rest = rest[3:]
    rows = k_refs[0].shape[0] // slots
    c2 = LOG2E / math.sqrt(HD)
    q = q_ref[...]
    qpos = qpos_ref[...]
    scores = []
    top = None if first else m_in[0]
    for i in range(npieces):
        s = contract_cols(k_refs[i][...], q)
        s = jnp.where(key_mask(starts_ref, i, slots, rows, qpos), s, big_negative)
        scores.append(s)
        t = jnp.max(s, axis=0, keepdims=True)
        top = t if top is None else jnp.maximum(top, t)
    total = None
    acc = None
    for i in range(npieces):
        p = jnp.exp2((scores[i] - top) * c2)
        t = jnp.sum(p, axis=0, keepdims=True)
        a = contract_rows(v_refs[i][...], p.astype(BF))
        total = t if total is None else total + t
        acc = a if acc is None else acc + a
    if not first:
        alpha = jnp.exp2((m_in[0] - top) * c2)
        total = total + l_in[0] * alpha
        acc = acc + a_in[...] * alpha
    if last:
        mix_ref, mixb_ref, log_ref = rest
        mix = (acc / total).T
        mix_ref[...] = mix
        mixb_ref[...] = mix.astype(BF)
        log_ref[0] = top * c2 + jnp.log2(total)
    else:
        m_out, l_out, a_out = rest
        m_out[0] = top
        l_out[0] = total
        a_out[...] = acc


def attend(starts, q, qpos, kv, carry, heads, slots, last):
    span = q.shape[0]
    first = carry is None
    np_ = len(kv)
    pr = kv[0].shape[0]
    row = pl.BlockSpec((1, 1, span), lambda h: (h, 0, 0))
    accs = pl.BlockSpec((HD, span), lambda h: (h, 0))
    specs = [
        pl.BlockSpec(memory_space=pltpu.SMEM),
        pl.BlockSpec((span, HD), lambda h: (0, h)),
        pl.BlockSpec((1, span), lambda h: (0, 0)),
    ]
    specs += [pl.BlockSpec((pr, HD), lambda h: (0, h))] * np_
    specs += [pl.BlockSpec((pr, HD), lambda h: (0, heads + h))] * np_
    args = [starts, q, qpos, *kv, *kv]
    if not first:
        specs += [row, row, accs]
        args += list(carry)
    rshape = jax.ShapeDtypeStruct((heads, 1, span), F32)
    if last:
        mix = pl.BlockSpec((span, HD), lambda h: (0, h))
        outs = [mix, mix, row]
        shapes = [
            jax.ShapeDtypeStruct((span, heads * HD), F32),
            jax.ShapeDtypeStruct((span, heads * HD), BF),
            rshape,
        ]
    else:
        outs = [row, row, accs]
        shapes = [rshape, rshape, jax.ShapeDtypeStruct((heads * HD, span), F32)]
    keys = np_ * pr
    return pl.pallas_call(
        functools.partial(fwd_kernel, np_, slots, first, last),
        grid=(heads,),
        in_specs=specs,
        out_specs=outs,
        out_shape=shapes,
        cost_estimate=pl.CostEstimate(
            flops=8 * span * keys * HD * heads,
            bytes_accessed=4 * keys * heads * HD,
            transcendentals=span * keys * heads,
        ),
    )(*args)


def bwd_kernel(npieces, slots, heads, first, *refs):
    starts_ref, q_ref, do_ref, mix_ref, log_ref, qpos_ref = refs[:6]
    k_refs = refs[6 : 6 + npieces]
    v_refs = refs[6 + npieces : 6 + 2 * npieces]
    rest = refs[6 + 2 * npieces :]
    if not first:
        dq_in = rest[0]
        rest = rest[1:]
    dq_ref, out_refs = rest[0], rest[1:]
    h = pl.program_id(0)
    rows = k_refs[0].shape[0] // slots
    scale = 1.0 / math.sqrt(HD)
    c2 = LOG2E * scale
    q = q_ref[...]
    do = do_ref[...]
    delta = jnp.sum((do.astype(F32) * mix_ref[...]).T, axis=0, keepdims=True)
    log2 = log_ref[0]
    qpos = qpos_ref[...]
    dq = None
    for i in range(npieces):
        k = k_refs[i][...]
        s = contract_cols(k, q) * c2 - log2
        s = jnp.where(key_mask(starts_ref, i, slots, rows, qpos), s, big_negative)
        p = jnp.exp2(s)
        dp = contract_cols(v_refs[i][...], do)
        ds = (p * (dp - delta)).astype(BF)
        t = contract_rows(k, ds)
        dq = t if dq is None else dq + t
        kc = pl.ds(pl.multiple_of(h * HD, HD), HD)
        vc = pl.ds(pl.multiple_of((heads + h) * HD, HD), HD)
        out_refs[i][:, kc] = (mm(ds, q) * scale).astype(BF)
        out_refs[i][:, vc] = mm(p.astype(BF), do).astype(BF)
    dq = dq * scale
    dq_ref[...] = dq if first else dq + dq_in[...]


def attend_back(starts, q, do, mix, log, qpos, kv, dq, heads, slots):
    span = q.shape[0]
    first = dq is None
    np_ = len(kv)
    pr = kv[0].shape[0]
    head = pl.BlockSpec((span, HD), lambda h: (0, h))
    accs = pl.BlockSpec((HD, span), lambda h: (h, 0))
    specs = [
        pl.BlockSpec(memory_space=pltpu.SMEM),
        head,
        head,
        head,
        pl.BlockSpec((1, 1, span), lambda h: (h, 0, 0)),
        pl.BlockSpec((1, span), lambda h: (0, 0)),
    ]
    specs += [pl.BlockSpec((pr, HD), lambda h: (0, h))] * np_
    specs += [pl.BlockSpec((pr, HD), lambda h: (0, heads + h))] * np_
    args = [starts, q, do, mix, log, qpos, *kv, *kv]
    if not first:
        specs.append(accs)
        args.append(dq)
    keys = np_ * pr
    return pl.pallas_call(
        functools.partial(bwd_kernel, np_, slots, heads, first),
        grid=(heads,),
        in_specs=specs,
        out_specs=[accs] + [pl.BlockSpec((pr, 2 * heads * HD), lambda h: (0, 0))] * np_,
        out_shape=[jax.ShapeDtypeStruct((heads * HD, span), F32)]
        + [jax.ShapeDtypeStruct((pr, 2 * heads * HD), BF)] * np_,
        cost_estimate=pl.CostEstimate(
            flops=20 * span * keys * HD * heads,
            bytes_accessed=8 * keys * heads * HD,
            transcendentals=span * keys * heads,
        ),
    )(*args)


def turn_back(x, cosine, sine):
    return x * cosine - pltpu.roll(x, HD // 2, 1) * sine


def unrotate_kernel(n, heads, transposed, *refs):
    nd = 1 if transposed else 2
    d_refs = refs[:nd]
    raw_refs = refs[nd : nd + n]
    r_ref, g_ref, cos_ref, sin_ref, w_ref, inner_ref, gain_ref = refs[nd + n :]
    rows = raw_refs[0].shape[0]
    half = n // 2
    for h in range(heads):
        c = slice(h * HD, (h + 1) * HD)
        gain_sum = None
        whole = d_refs[0][c, :].T if transposed else None
        for s in range(n):
            r = slice(s * rows, (s + 1) * rows)
            if transposed:
                d = whole[r, :]
            else:
                o = slice((s % half) * rows, (s % half + 1) * rows)
                d = d_refs[0 if s < half else 1][o, c].astype(F32)
            grad = turn_back(d, cos_ref[r, :], sin_ref[r, :])
            raw = raw_refs[s][:, c]
            weighted = grad * g_ref[:, c]
            w_ref[r, c] = weighted
            t = jnp.sum(weighted * raw, axis=1, keepdims=True)
            inner_ref[r, :] = t if h == 0 else inner_ref[r, :] + t
            u = jnp.sum(grad * raw * r_ref[r, :], axis=0, keepdims=True)
            gain_sum = u if gain_sum is None else gain_sum + u
        gain_ref[:, c] = gain_sum


def unrotate(d, raw, rms, gain, cosine, sine, heads, transposed):
    n = len(raw)
    span = n * raw[0].shape[0]
    units = heads * HD
    return pl.pallas_call(
        functools.partial(unrotate_kernel, n, heads, transposed),
        in_specs=[vmem()] * (len(d) + n + 4),
        out_specs=[vmem()] * 3,
        out_shape=[
            jax.ShapeDtypeStruct((span, units), F32),
            jax.ShapeDtypeStruct((span, 1), F32),
            jax.ShapeDtypeStruct((1, units), F32),
        ],
    )(*d, *raw, rms, gain, cosine, sine)


def norm_back(raw, rms_inv, gain, grad_out):
    weighted = gain * grad_out
    inner = jnp.sum(weighted * raw, axis=1, keepdims=True)
    width = raw.shape[1]
    return (
        rms_inv[:, None] * weighted - raw * (rms_inv * rms_inv * rms_inv)[:, None] * inner / width
    )


def local(
    nc,
    nf,
    block_input,
    positions,
    query_weight,
    key_weight,
    value_weight,
    output_weight,
    query_gain,
    key_gain,
    attn_gain,
    mlp_gain,
    gate_weight,
    up_weight,
    down_weight,
    cotangent,
):
    rows, width = block_input.shape
    span = rows * nf
    units = query_weight.shape[1]
    heads = units // HD
    half = nf // 2
    me_c = lax.axis_index("ctx")
    me_f = lax.axis_index("fsdp")
    unit_start = me_f * units

    x_slots = [block_input]
    begin = positions[:1]
    begins = None
    for s in range(1, nf):
        got = shift(x_slots[-1], nf, 1)
        if s == min(2, nf - 1):
            begin, x_last = lax.optimization_barrier((begin, mm(x_slots[-1], query_weight)))
            begins = jnp.concatenate([begin] + [shift(begin, nf, t) for t in range(1, nf)])[None, :]
            b = 1
            while b < nc:
                begins = jnp.concatenate([begins, swap(begins, nc, b)])
                b *= 2
        if s == nf - 1:
            got, begins = lax.optimization_barrier((got, begins))
        x_slots.append(got)

    row_pos = (begins[0][:, None] + jnp.arange(rows)[None, :]).reshape(span)
    freqs = jnp.exp(-math.log(rope_base) * 2.0 * jnp.arange(HD // 2).astype(F32) / HD)
    angles = row_pos.astype(F32)[:, None] * freqs[None, :]
    cosine, sine = jnp.cos(angles), jnp.sin(angles)
    cosine = jnp.concatenate([cosine, cosine], axis=1)
    sine = jnp.concatenate([-sine, sine], axis=1)
    qpos = row_pos[None, :]

    q_raw = [mm(x, query_weight) for x in x_slots]
    q_raw[min(2, nf - 1) - 1] = x_last
    k_raw = [mm(x, key_weight) for x in x_slots]
    v_raw = [mm(x, value_weight) for x in x_slots]
    squares = jnp.stack(
        [
            jnp.stack([jnp.sum(q * q, axis=1), jnp.sum(k * k, axis=1)])
            for q, k in zip(q_raw, k_raw)
        ]
    )
    squares = slot_sum(squares, nf)
    query_rms = lax.rsqrt(squares[:, 0].reshape(span, 1) / width + norm_eps)
    key_rms = lax.rsqrt(squares[:, 1].reshape(span, 1) / width + norm_eps)
    query_scale = lax.dynamic_slice_in_dim(query_gain, unit_start, units)[None, :]
    key_scale = lax.dynamic_slice_in_dim(key_gain, unit_start, units)[None, :]

    query_rot, kv_a, kv_b = pl.pallas_call(
        functools.partial(prep_kernel, nf, heads),
        in_specs=[vmem()] * (3 * nf + 6),
        out_specs=[vmem()] * 3,
        out_shape=[jax.ShapeDtypeStruct((span, units), BF)]
        + [jax.ShapeDtypeStruct((span // 2, 2 * units), BF)] * 2,
    )(*q_raw, *k_raw, *v_raw, query_rms, key_rms, query_scale, key_scale, cosine, sine)

    orders = bit_orders(nc)
    groups = group_order(nc)
    pieces = [{0: kv_a}, {0: kv_b}]

    def fetch(i, m, token):
        if m not in pieces[i]:
            src, bit = came_from(m, orders[i])
            have = fetch(i, src, token)
            if token is not None:
                have = gate(have, token)
            pieces[i][m] = swap(have, nc, bit)
        return pieces[i][m]

    def group_inputs(group):
        kv = [pieces[0][m] for m in group] + [pieces[1][m] for m in group]
        starts = jnp.concatenate(
            [begins[m, :half] for m in group] + [begins[m, half:] for m in group]
        )
        return starts, kv

    carry = None
    tokens = []
    for group in groups:
        for m in group:
            for i in range(2):
                far = distance(m)
                if far < 2:
                    fetch(i, m, None)
                else:
                    fetch(i, m, tokens[1] if m & 1 else tokens[0])
        starts, kv = group_inputs(group)
        carry = attend(
            starts, query_rot, qpos, kv, carry, heads, half, group is groups[-1]
        )
        tokens.append(carry[0])
    mixture, mixture_b, log_total = carry

    def rows_of(x, s):
        return x[s * rows : (s + 1) * rows]

    attn_out = ring_scatter(lambda s: mm(rows_of(mixture_b, s), output_weight), nf)
    attn_rms = lax.rsqrt(jnp.mean(attn_out * attn_out, axis=1) + norm_eps)
    hidden_state = block_input.astype(F32) + attn_out * attn_rms[:, None] * attn_gain[None, :]
    state_slots = ring_gather(hidden_state.astype(BF), nf)
    gate_pre = [mm(x, gate_weight) for x in state_slots]
    up_pre = [mm(x, up_weight) for x in state_slots]
    activated = [(jax.nn.silu(g) * u).astype(BF) for g, u in zip(gate_pre, up_pre)]
    mlp_out = ring_scatter(lambda s: mm(activated[s], down_weight), nf)

    activ = [{0: jnp.concatenate(activated[:half])}, {0: jnp.concatenate(activated[half:])}]

    def fetch_activ(i, m):
        if m not in activ[i]:
            src, bit = came_from(m, orders[i])
            have = fetch_activ(i, src)
            activ[i][m] = swap(have, nc, bit)
        return activ[i][m]

    for i in range(2):
        for m in range(nc):
            fetch_activ(i, m)

    mlp_rms = lax.rsqrt(jnp.mean(mlp_out * mlp_out, axis=1) + norm_eps)
    block_output = (hidden_state + mlp_out * mlp_rms[:, None] * mlp_gain[None, :]).astype(BF)
    upstream = cotangent.astype(F32)
    mlp_gain_part = jnp.sum(upstream * mlp_out * mlp_rms[:, None], axis=0)
    mlp_grad_b = norm_back(mlp_out, mlp_rms, mlp_gain[None, :], upstream).astype(BF)

    def ctx_scatter(x):
        return lax.psum_scatter(x, "ctx", scatter_dimension=0, tiled=True)

    def slot_grads(s, rows_in):
        activ_grad = contract_cols(rows_in, down_weight)
        sg = jax.nn.sigmoid(gate_pre[s])
        g = (activ_grad * up_pre[s] * sg * (1.0 + gate_pre[s] * (1.0 - sg))).astype(BF)
        return g, (activ_grad * gate_pre[s] * sg).astype(BF)

    def state_part(g, u):
        return contract_cols(g, gate_weight) + contract_cols(u, up_weight)

    grad_slots, gate_grads, up_grads = [mlp_grad_b], [], []
    acc = None
    for s in range(nf):
        got = shift(grad_slots[-1], nf, 1) if s < nf - 1 else None
        g, u = slot_grads(s, grad_slots[s])
        if s == 1:
            acc = state_part(g, u).astype(BF)
        elif s > 1:
            acc = (shift(acc, nf, 1).astype(F32) + state_part(g, u)).astype(BF)
        if got is not None:
            got, g, u = lax.optimization_barrier((got, g, u))
            grad_slots.append(got)
        gate_grads.append(g)
        up_grads.append(u)
    gate_up_part = contract_rows(
        jnp.concatenate(state_slots),
        jnp.concatenate([jnp.concatenate(gate_grads), jnp.concatenate(up_grads)], axis=1),
    ).astype(BF)
    gate_up_sum = ctx_scatter(gate_up_part)
    state_grad = state_part(gate_grads[0], up_grads[0])
    if nf > 1:
        got = shift(acc, nf, 1)
        state_grad = got.astype(F32) + state_grad
    state_grad = upstream + state_grad
    grad_rows = jnp.concatenate(grad_slots)
    block = width // nc

    def columns(m):
        cut = lax.dynamic_slice_in_dim(grad_rows, (me_c ^ m) * block, block, axis=1)
        if m == 0:
            return cut
        return swap(cut, nc, m)

    down_grad = None
    for masks in (range(nc // 2), range(nc // 2, nc)):
        part = contract_rows(
            jnp.concatenate([activ[i][m] for m in masks for i in range(2)]),
            jnp.concatenate([columns(m) for m in masks]),
        )
        down_grad = part if down_grad is None else down_grad + part

    attn_gain_part = jnp.sum(state_grad * attn_out * attn_rms[:, None], axis=0)
    attn_grad_b = norm_back(attn_out, attn_rms, attn_gain[None, :], state_grad).astype(BF)
    first_hop = shift(attn_grad_b, nf, 1)
    proj_slots = [attn_grad_b, first_hop]
    for _ in range(2, nf):
        got = shift(proj_slots[-1], nf, 1)
        proj_slots.append(got)
    mixture_grads = []
    for s in range(nf):
        mixture_grads.append(contract_cols(proj_slots[s], output_weight).astype(BF))
    mixture_grad_b = jnp.concatenate(mixture_grads)

    dq = None
    sums = [{}, {}]

    def send(i, m):
        into, bit = came_from(m, orders[i])
        got = swap(sums[i].pop(m), nc, bit)
        sums[i][into] = (sums[i][into].astype(F32) + got.astype(F32)).astype(BF)
        return got

    waits = []
    for gi, group in enumerate(groups[::-1]):
        starts, kv = group_inputs(group)
        if gi:
            dq = gate(dq, *waits[gi - 1])
        dq, *out = attend_back(
            starts, query_rot, mixture_grad_b, mixture, log_total, qpos, kv, dq, heads, half
        )
        for m, a, b in zip(group, out[: len(group)], out[len(group) :]):
            sums[0][m], sums[1][m] = a, b
        waits.append([send(i, m) for i in range(2) for m in group if m & 1])
    for far in range(max(distance(m) for m in range(nc)), 0, -1):
        for i in range(2):
            for m in [m for m in sums[i] if distance(m) == far]:
                send(i, m)
    own_a, own_b = sums[0][0], sums[1][0]

    def unit_full(x):
        return lax.dynamic_update_slice_in_dim(jnp.zeros((width,), F32), x, unit_start, 0)

    def norm_grads(weighted, inner, raw, rms):
        cube = rms * rms * rms
        return [
            (
                rows_of(rms, s) * rows_of(weighted, s)
                - raw[s] * rows_of(cube, s) * inner[s][:, None] / width
            ).astype(BF)
            for s in range(nf)
        ]

    def spread(*vectors):
        return jnp.stack([v.reshape(nf, width // nf) for v in vectors], axis=1).reshape(nf, -1)

    def gathered(flat, count):
        return flat.reshape(nf, count, width // nf).transpose(1, 0, 2).reshape(count, width)

    query_weighted, query_inner, query_gain_part = unrotate(
        [dq], q_raw, query_rms, query_scale, cosine, sine, heads, True
    )
    query_inner, early_gains = slot_sum(
        query_inner.reshape(nf, rows),
        nf,
        spread(unit_full(query_gain_part[0]), attn_gain_part, mlp_gain_part),
    )
    query_grads = norm_grads(query_weighted, query_inner, q_raw, query_rms)

    x_rows = jnp.concatenate(x_slots)
    q_part = contract_rows(x_rows, jnp.concatenate(query_grads)).astype(BF)
    o_part = contract_rows(jnp.concatenate(proj_slots), mixture_b).astype(BF)
    qo_part = jnp.concatenate([q_part, o_part], axis=1)
    gate_up_sum, own_a, own_b = lax.optimization_barrier((gate_up_sum, own_a, own_b))
    qo_part, gate_up_sum = lax.optimization_barrier((qo_part, gate_up_sum))
    qo_grad = ctx_scatter(qo_part).astype(F32)
    query_grad, output_grad = qo_grad[:, :units], qo_grad[:, units:].T

    key_weighted, key_inner, key_gain_part = unrotate(
        [own_a, own_b], k_raw, key_rms, key_scale, cosine, sine, heads, False
    )
    key_inner, key_gain_sum = slot_sum(
        key_inner.reshape(nf, rows), nf, spread(unit_full(key_gain_part[0]))
    )
    key_grads = norm_grads(key_weighted, key_inner, k_raw, key_rms)
    own = jnp.concatenate([own_a[:, units:], own_b[:, units:]])
    value_grads = [rows_of(own, s) for s in range(nf)]

    started = []
    input_grad = state_grad + ring_scatter(
        lambda s: contract_cols(query_grads[s], query_weight)
        + contract_cols(key_grads[s], key_weight)
        + contract_cols(value_grads[s], value_weight),
        nf,
        started=started,
    )
    k_rows, v_rows, *_ = lax.optimization_barrier((jnp.concatenate(key_grads), own, *started))
    k_part = contract_rows(x_rows, k_rows).astype(BF)
    v_part = contract_rows(x_rows, v_rows).astype(BF)
    key_grad = halving(k_part, me_c, nc, orders[0])
    value_grad = halving(v_part, me_c, nc, orders[1])
    gains = jnp.concatenate([gathered(early_gains, 3), gathered(key_gain_sum, 1)])
    gains_own = halving(gains.T, me_c, nc, orders[0]).T
    ff = gate_weight.shape[1]
    gate_up = gate_up_sum.astype(F32)
    gate_grad, up_grad = gate_up[:, :ff], gate_up[:, ff:]
    return (
        block_output,
        input_grad,
        query_grad,
        key_grad,
        value_grad,
        output_grad,
        gains_own[0],
        gains_own[3],
        gains_own[1],
        gains_own[2],
        gate_grad,
        up_grad,
        down_grad,
    )


def solution(mesh):
    def layer(*args):
        return local(mesh.shape["ctx"], mesh.shape["fsdp"], *args)

    return jax.shard_map(
        layer,
        mesh=mesh,
        in_specs=(
            P(("ctx", "fsdp"), None),
            P(("ctx", "fsdp")),
            P(None, "fsdp"),
            P(None, "fsdp"),
            P(None, "fsdp"),
            P("fsdp", None),
            P(),
            P(),
            P(),
            P(),
            P(None, "fsdp"),
            P(None, "fsdp"),
            P("fsdp", None),
            P(("ctx", "fsdp"), None),
        ),
        out_specs=(
            P(("ctx", "fsdp"), None),
            P(("ctx", "fsdp"), None),
            P("ctx", "fsdp"),
            P("ctx", "fsdp"),
            P("ctx", "fsdp"),
            P("fsdp", "ctx"),
            P("ctx"),
            P("ctx"),
            P("ctx"),
            P("ctx"),
            P("ctx", "fsdp"),
            P("ctx", "fsdp"),
            P("fsdp", "ctx"),
        ),
        check_vma=False,
    )
```

```python
import functools
import math

import jax
import jax.numpy as jnp
from jax import lax
from jax.experimental import pallas as pl
from jax.experimental.pallas import tpu as pltpu
from jax.sharding import PartitionSpec as P


HD = 128
norm_eps = 1e-06
rope_base = 500000.0
big_negative = -1e30
LOG2E = math.log2(math.e)
BF = jnp.bfloat16
F32 = jnp.float32


def mm(left, right):
    return jnp.dot(left, right, preferred_element_type=F32)


def contract_rows(left, right):
    return lax.dot_general(left, right, (((0,), (0,)), ((), ())), preferred_element_type=F32)


def contract_cols(left, right):
    return lax.dot_general(left, right, (((1,), (1,)), ((), ())), preferred_element_type=F32)


def gate(x, *tokens):
    return lax.optimization_barrier((x, *tokens))[0]


def shift(x, n, by):
    return lax.ppermute(x, "fsdp", [(i, (i + by) % n) for i in range(n)])


def ring_gather(x, n):
    slots = [x]
    for _ in range(n - 1):
        slots.append(shift(slots[-1], n, 1))
    return slots


def ring_scatter(part, n, under=(), started=None):
    if n == 1:
        return part(0)
    acc = part(1).astype(BF)
    if started is not None:
        started.append(acc)
    for s in range(2, n):
        acc = (shift(acc, n, 1).astype(F32) + part(s)).astype(BF)
    return gate(shift(acc, n, 1), *under).astype(F32) + part(0)


def slot_sum(x, n, flat=None):
    total, flat_total = x, flat
    cut = x.shape[-1]
    both = x if flat is None else jnp.concatenate([x, flat], axis=-1)
    for t in range(1, n):
        got = shift(both, n, t)
        total = total + jnp.roll(got[..., :cut], t, axis=0)
        if flat is not None:
            flat_total = flat_total + got[..., cut:]
    return total if flat is None else (total, flat_total)


def swap(x, n, bit):
    return lax.ppermute(x, "ctx", [(i, i ^ bit) for i in range(n)])


def bit_orders(n):
    bits = []
    b = 2
    while b < n:
        bits.append(b)
        b *= 2
    return bits, bits[::-1]


def halving(part, me, n, order, marks=None):
    seq = ([1] if n > 1 else []) + list(order[::-1])
    block = part.shape[0] // n
    levels = len(seq)
    masks = [
        sum(seq[k] for k in range(levels) if t >> (levels - 1 - k) & 1) for t in range(n)
    ]

    def blocks(ms):
        return jnp.concatenate(
            [lax.dynamic_slice_in_dim(part, (me ^ m) * block, block) for m in ms]
        )

    keep, away = blocks(masks[: n // 2]), blocks(masks[n // 2 :])
    for k, bit in enumerate(seq):
        got = swap(away.astype(BF), n, bit)
        total = keep.astype(F32) + got.astype(F32)
        rest = total.shape[0] // 2
        if k < levels - 1:
            total = total.astype(BF)
            if marks is not None:
                marks[k].append(total)
            keep, away = total[:rest], total[rest:]
    return total


def distance(m):
    return bin(m >> 1).count("1")


def group_order(n):
    pairs = [(m, m + 1) if n > 1 else (m,) for m in range(0, n, 2)]
    return sorted(pairs, key=lambda g: (distance(g[0]), g[0]))


def came_from(m, order):
    if m & 1:
        return m ^ 1, 1
    bit = [b for b in order if m & b][-1]
    return m ^ bit, bit


def vmem(*_):
    return pl.BlockSpec(memory_space=pltpu.VMEM)


def prep_kernel(n, heads, *refs):
    q_refs, k_refs, v_refs = refs[:n], refs[n : 2 * n], refs[2 * n : 3 * n]
    qr_ref, kr_ref, qg_ref, kg_ref, cos_ref, sin_ref = refs[3 * n : 3 * n + 6]
    qo_ref, kva_ref, kvb_ref = refs[3 * n + 6 :]
    rows = q_refs[0].shape[0]
    half = n // 2
    for s in range(n):
        r = slice(s * rows, (s + 1) * rows)
        cosine, sine = cos_ref[r, :], sin_ref[r, :]
        out = kva_ref if s < half else kvb_ref
        o = slice((s % half) * rows, (s % half + 1) * rows)
        for h in range(heads):
            c = slice(h * HD, (h + 1) * HD)
            x = q_refs[s][:, c] * qr_ref[r, :] * qg_ref[:, c]
            qo_ref[r, c] = (x * cosine + pltpu.roll(x, HD // 2, 1) * sine).astype(BF)
            y = k_refs[s][:, c] * kr_ref[r, :] * kg_ref[:, c]
            out[o, c] = (y * cosine + pltpu.roll(y, HD // 2, 1) * sine).astype(BF)
            out[o, heads * HD + h * HD : heads * HD + (h + 1) * HD] = v_refs[s][:, c].astype(BF)


def key_mask(starts_ref, piece, slots, rows, qpos):
    parts = []
    for j in range(slots):
        row = lax.broadcasted_iota(jnp.int32, (rows, 1), 0)
        parts.append(row + starts_ref[piece * slots + j])
    return jnp.concatenate(parts, axis=0) <= qpos


def fwd_kernel(npieces, slots, first, last, *refs):
    starts_ref, q_ref, qpos_ref = refs[:3]
    k_refs = refs[3 : 3 + npieces]
    v_refs = refs[3 + npieces : 3 + 2 * npieces]
    rest = refs[3 + 2 * npieces :]
    if not first:
        m_in, l_in, a_in = rest[:3]
        rest = rest[3:]
    rows = k_refs[0].shape[0] // slots
    c2 = LOG2E / math.sqrt(HD)
    q = q_ref[...]
    qpos = qpos_ref[...]
    scores = []
    top = None if first else m_in[0]
    for i in range(npieces):
        s = contract_cols(k_refs[i][...], q)
        s = jnp.where(key_mask(starts_ref, i, slots, rows, qpos), s, big_negative)
        scores.append(s)
        t = jnp.max(s, axis=0, keepdims=True)
        top = t if top is None else jnp.maximum(top, t)
    total = None
    acc = None
    for i in range(npieces):
        p = jnp.exp2((scores[i] - top) * c2)
        t = jnp.sum(p, axis=0, keepdims=True)
        a = contract_rows(v_refs[i][...], p.astype(BF))
        total = t if total is None else total + t
        acc = a if acc is None else acc + a
    if not first:
        alpha = jnp.exp2((m_in[0] - top) * c2)
        total = total + l_in[0] * alpha
        acc = acc + a_in[...] * alpha
    if last:
        mix_ref, mixb_ref, log_ref = rest
        mix = (acc / total).T
        mix_ref[...] = mix
        mixb_ref[...] = mix.astype(BF)
        log_ref[0] = top * c2 + jnp.log2(total)
    else:
        m_out, l_out, a_out = rest
        m_out[0] = top
        l_out[0] = total
        a_out[...] = acc


def attend(starts, q, qpos, kv, carry, heads, slots, last):
    span = q.shape[0]
    first = carry is None
    np_ = len(kv)
    pr = kv[0].shape[0]
    row = pl.BlockSpec((1, 1, span), lambda h: (h, 0, 0))
    accs = pl.BlockSpec((HD, span), lambda h: (h, 0))
    specs = [
        pl.BlockSpec(memory_space=pltpu.SMEM),
        pl.BlockSpec((span, HD), lambda h: (0, h)),
        pl.BlockSpec((1, span), lambda h: (0, 0)),
    ]
    specs += [pl.BlockSpec((pr, HD), lambda h: (0, h))] * np_
    specs += [pl.BlockSpec((pr, HD), lambda h: (0, heads + h))] * np_
    args = [starts, q, qpos, *kv, *kv]
    if not first:
        specs += [row, row, accs]
        args += list(carry)
    rshape = jax.ShapeDtypeStruct((heads, 1, span), F32)
    if last:
        mix = pl.BlockSpec((span, HD), lambda h: (0, h))
        outs = [mix, mix, row]
        shapes = [
            jax.ShapeDtypeStruct((span, heads * HD), F32),
            jax.ShapeDtypeStruct((span, heads * HD), BF),
            rshape,
        ]
    else:
        outs = [row, row, accs]
        shapes = [rshape, rshape, jax.ShapeDtypeStruct((heads * HD, span), F32)]
    keys = np_ * pr
    return pl.pallas_call(
        functools.partial(fwd_kernel, np_, slots, first, last),
        grid=(heads,),
        in_specs=specs,
        out_specs=outs,
        out_shape=shapes,
        cost_estimate=pl.CostEstimate(
            flops=8 * span * keys * HD * heads,
            bytes_accessed=4 * keys * heads * HD,
            transcendentals=span * keys * heads,
        ),
    )(*args)


def bwd_kernel(npieces, slots, heads, first, *refs):
    starts_ref, q_ref, do_ref, mix_ref, log_ref, qpos_ref = refs[:6]
    k_refs = refs[6 : 6 + npieces]
    v_refs = refs[6 + npieces : 6 + 2 * npieces]
    rest = refs[6 + 2 * npieces :]
    if not first:
        dq_in = rest[0]
        rest = rest[1:]
    dq_ref, out_refs = rest[0], rest[1:]
    h = pl.program_id(0)
    rows = k_refs[0].shape[0] // slots
    scale = 1.0 / math.sqrt(HD)
    c2 = LOG2E * scale
    q = q_ref[...]
    do = do_ref[...]
    delta = jnp.sum((do.astype(F32) * mix_ref[...]).T, axis=0, keepdims=True)
    log2 = log_ref[0]
    qpos = qpos_ref[...]
    dq = None
    for i in range(npieces):
        k = k_refs[i][...]
        s = contract_cols(k, q) * c2 - log2
        s = jnp.where(key_mask(starts_ref, i, slots, rows, qpos), s, big_negative)
        p = jnp.exp2(s)
        dp = contract_cols(v_refs[i][...], do)
        ds = (p * (dp - delta)).astype(BF)
        t = contract_rows(k, ds)
        dq = t if dq is None else dq + t
        kc = pl.ds(pl.multiple_of(h * HD, HD), HD)
        vc = pl.ds(pl.multiple_of((heads + h) * HD, HD), HD)
        out_refs[i][:, kc] = (mm(ds, q) * scale).astype(BF)
        out_refs[i][:, vc] = mm(p.astype(BF), do).astype(BF)
    dq = dq * scale
    dq_ref[...] = dq if first else dq + dq_in[...]


def attend_back(starts, q, do, mix, log, qpos, kv, dq, heads, slots):
    span = q.shape[0]
    first = dq is None
    np_ = len(kv)
    pr = kv[0].shape[0]
    head = pl.BlockSpec((span, HD), lambda h: (0, h))
    accs = pl.BlockSpec((HD, span), lambda h: (h, 0))
    specs = [
        pl.BlockSpec(memory_space=pltpu.SMEM),
        head,
        head,
        head,
        pl.BlockSpec((1, 1, span), lambda h: (h, 0, 0)),
        pl.BlockSpec((1, span), lambda h: (0, 0)),
    ]
    specs += [pl.BlockSpec((pr, HD), lambda h: (0, h))] * np_
    specs += [pl.BlockSpec((pr, HD), lambda h: (0, heads + h))] * np_
    args = [starts, q, do, mix, log, qpos, *kv, *kv]
    if not first:
        specs.append(accs)
        args.append(dq)
    keys = np_ * pr
    return pl.pallas_call(
        functools.partial(bwd_kernel, np_, slots, heads, first),
        grid=(heads,),
        in_specs=specs,
        out_specs=[accs] + [pl.BlockSpec((pr, 2 * heads * HD), lambda h: (0, 0))] * np_,
        out_shape=[jax.ShapeDtypeStruct((heads * HD, span), F32)]
        + [jax.ShapeDtypeStruct((pr, 2 * heads * HD), BF)] * np_,
        cost_estimate=pl.CostEstimate(
            flops=20 * span * keys * HD * heads,
            bytes_accessed=8 * keys * heads * HD,
            transcendentals=span * keys * heads,
        ),
    )(*args)


def turn_back(x, cosine, sine):
    return x * cosine - pltpu.roll(x, HD // 2, 1) * sine


def unrotate_kernel(n, heads, transposed, *refs):
    nd = 1 if transposed else 2
    d_refs = refs[:nd]
    raw_refs = refs[nd : nd + n]
    r_ref, g_ref, cos_ref, sin_ref, w_ref, inner_ref, gain_ref = refs[nd + n :]
    rows = raw_refs[0].shape[0]
    half = n // 2
    for h in range(heads):
        c = slice(h * HD, (h + 1) * HD)
        gain_sum = None
        whole = d_refs[0][c, :].T if transposed else None
        for s in range(n):
            r = slice(s * rows, (s + 1) * rows)
            if transposed:
                d = whole[r, :]
            else:
                o = slice((s % half) * rows, (s % half + 1) * rows)
                d = d_refs[0 if s < half else 1][o, c].astype(F32)
            grad = turn_back(d, cos_ref[r, :], sin_ref[r, :])
            raw = raw_refs[s][:, c]
            weighted = grad * g_ref[:, c]
            w_ref[r, c] = weighted
            t = jnp.sum(weighted * raw, axis=1, keepdims=True)
            inner_ref[r, :] = t if h == 0 else inner_ref[r, :] + t
            u = jnp.sum(grad * raw * r_ref[r, :], axis=0, keepdims=True)
            gain_sum = u if gain_sum is None else gain_sum + u
        gain_ref[:, c] = gain_sum


def unrotate(d, raw, rms, gain, cosine, sine, heads, transposed):
    n = len(raw)
    span = n * raw[0].shape[0]
    units = heads * HD
    return pl.pallas_call(
        functools.partial(unrotate_kernel, n, heads, transposed),
        in_specs=[vmem()] * (len(d) + n + 4),
        out_specs=[vmem()] * 3,
        out_shape=[
            jax.ShapeDtypeStruct((span, units), F32),
            jax.ShapeDtypeStruct((span, 1), F32),
            jax.ShapeDtypeStruct((1, units), F32),
        ],
    )(*d, *raw, rms, gain, cosine, sine)


def norm_back(raw, rms_inv, gain, grad_out):
    weighted = gain * grad_out
    inner = jnp.sum(weighted * raw, axis=1, keepdims=True)
    width = raw.shape[1]
    return (
        rms_inv[:, None] * weighted - raw * (rms_inv * rms_inv * rms_inv)[:, None] * inner / width
    )


def local(
    nc,
    nf,
    block_input,
    positions,
    query_weight,
    key_weight,
    value_weight,
    output_weight,
    query_gain,
    key_gain,
    attn_gain,
    mlp_gain,
    gate_weight,
    up_weight,
    down_weight,
    cotangent,
):
    rows, width = block_input.shape
    span = rows * nf
    units = query_weight.shape[1]
    heads = units // HD
    half = nf // 2
    me_c = lax.axis_index("ctx")
    me_f = lax.axis_index("fsdp")
    unit_start = me_f * units

    x_slots = [block_input]
    begin = positions[:1]
    begins = None
    for s in range(1, nf):
        got = shift(x_slots[-1], nf, 1)
        if s == min(2, nf - 1):
            begin, x_last = lax.optimization_barrier((begin, mm(x_slots[-1], query_weight)))
            begins = jnp.concatenate([begin] + [shift(begin, nf, t) for t in range(1, nf)])[None, :]
            b = 1
            while b < nc:
                begins = jnp.concatenate([begins, swap(begins, nc, b)])
                b *= 2
        if s == nf - 1:
            got, begins = lax.optimization_barrier((got, begins))
        x_slots.append(got)

    row_pos = (begins[0][:, None] + jnp.arange(rows)[None, :]).reshape(span)
    freqs = jnp.exp(-math.log(rope_base) * 2.0 * jnp.arange(HD // 2).astype(F32) / HD)
    angles = row_pos.astype(F32)[:, None] * freqs[None, :]
    cosine, sine = jnp.cos(angles), jnp.sin(angles)
    cosine = jnp.concatenate([cosine, cosine], axis=1)
    sine = jnp.concatenate([-sine, sine], axis=1)
    qpos = row_pos[None, :]

    q_raw = [mm(x, query_weight) for x in x_slots]
    q_raw[min(2, nf - 1) - 1] = x_last
    k_raw = [mm(x, key_weight) for x in x_slots]
    v_raw = [mm(x, value_weight) for x in x_slots]
    squares = jnp.stack(
        [
            jnp.stack([jnp.sum(q * q, axis=1), jnp.sum(k * k, axis=1)])
            for q, k in zip(q_raw, k_raw)
        ]
    )
    squares = slot_sum(squares, nf)
    query_rms = lax.rsqrt(squares[:, 0].reshape(span, 1) / width + norm_eps)
    key_rms = lax.rsqrt(squares[:, 1].reshape(span, 1) / width + norm_eps)
    query_scale = lax.dynamic_slice_in_dim(query_gain, unit_start, units)[None, :]
    key_scale = lax.dynamic_slice_in_dim(key_gain, unit_start, units)[None, :]

    query_rot, kv_a, kv_b = pl.pallas_call(
        functools.partial(prep_kernel, nf, heads),
        in_specs=[vmem()] * (3 * nf + 6),
        out_specs=[vmem()] * 3,
        out_shape=[jax.ShapeDtypeStruct((span, units), BF)]
        + [jax.ShapeDtypeStruct((span // 2, 2 * units), BF)] * 2,
    )(*q_raw, *k_raw, *v_raw, query_rms, key_rms, query_scale, key_scale, cosine, sine)

    orders = bit_orders(nc)
    groups = group_order(nc)
    pieces = [{0: kv_a}, {0: kv_b}]

    def fetch(i, m, token):
        if m not in pieces[i]:
            src, bit = came_from(m, orders[i])
            have = fetch(i, src, token)
            if token is not None:
                have = gate(have, token)
            pieces[i][m] = swap(have, nc, bit)
        return pieces[i][m]

    def group_inputs(group):
        kv = [pieces[0][m] for m in group] + [pieces[1][m] for m in group]
        starts = jnp.concatenate(
            [begins[m, :half] for m in group] + [begins[m, half:] for m in group]
        )
        return starts, kv

    carry = None
    tokens = []
    for group in groups:
        for m in group:
            for i in range(2):
                far = distance(m)
                if far < 2:
                    fetch(i, m, None)
                else:
                    fetch(i, m, tokens[1] if m & 1 else tokens[0])
        starts, kv = group_inputs(group)
        carry = attend(
            starts, query_rot, qpos, kv, carry, heads, half, group is groups[-1]
        )
        tokens.append(carry[0])
    mixture, mixture_b, log_total = carry

    def rows_of(x, s):
        return x[s * rows : (s + 1) * rows]

    attn_out = ring_scatter(lambda s: mm(rows_of(mixture_b, s), output_weight), nf)
    attn_rms = lax.rsqrt(jnp.mean(attn_out * attn_out, axis=1) + norm_eps)
    hidden_state = block_input.astype(F32) + attn_out * attn_rms[:, None] * attn_gain[None, :]
    state_slots = ring_gather(hidden_state.astype(BF), nf)
    gate_pre = [mm(x, gate_weight) for x in state_slots]
    up_pre = [mm(x, up_weight) for x in state_slots]
    activated = [(jax.nn.silu(g) * u).astype(BF) for g, u in zip(gate_pre, up_pre)]
    mlp_out = ring_scatter(lambda s: mm(activated[s], down_weight), nf)

    activ = [{0: jnp.concatenate(activated[:half])}, {0: jnp.concatenate(activated[half:])}]

    def fetch_activ(i, m):
        if m not in activ[i]:
            src, bit = came_from(m, orders[i])
            have = fetch_activ(i, src)
            activ[i][m] = swap(have, nc, bit)
        return activ[i][m]

    for i in range(2):
        for m in range(nc):
            fetch_activ(i, m)

    mlp_rms = lax.rsqrt(jnp.mean(mlp_out * mlp_out, axis=1) + norm_eps)
    block_output = (hidden_state + mlp_out * mlp_rms[:, None] * mlp_gain[None, :]).astype(BF)
    upstream = cotangent.astype(F32)
    mlp_gain_part = jnp.sum(upstream * mlp_out * mlp_rms[:, None], axis=0)
    mlp_grad_b = norm_back(mlp_out, mlp_rms, mlp_gain[None, :], upstream).astype(BF)

    def ctx_scatter(x):
        return lax.psum_scatter(x, "ctx", scatter_dimension=0, tiled=True)

    def slot_grads(s, rows_in):
        activ_grad = contract_cols(rows_in, down_weight)
        sg = jax.nn.sigmoid(gate_pre[s])
        g = (activ_grad * up_pre[s] * sg * (1.0 + gate_pre[s] * (1.0 - sg))).astype(BF)
        return g, (activ_grad * gate_pre[s] * sg).astype(BF)

    def state_part(g, u):
        return contract_cols(g, gate_weight) + contract_cols(u, up_weight)

    grad_slots, gate_grads, up_grads = [mlp_grad_b], [], []
    acc = None
    for s in range(nf):
        got = shift(grad_slots[-1], nf, 1) if s < nf - 1 else None
        g, u = slot_grads(s, grad_slots[s])
        if s == 1:
            acc = state_part(g, u).astype(BF)
        elif s > 1:
            acc = (shift(acc, nf, 1).astype(F32) + state_part(g, u)).astype(BF)
        if got is not None:
            got, g, u = lax.optimization_barrier((got, g, u))
            grad_slots.append(got)
        gate_grads.append(g)
        up_grads.append(u)
    gate_up_part = contract_rows(
        jnp.concatenate(state_slots),
        jnp.concatenate([jnp.concatenate(gate_grads), jnp.concatenate(up_grads)], axis=1),
    ).astype(BF)
    gate_up_sum = ctx_scatter(gate_up_part)
    state_grad = state_part(gate_grads[0], up_grads[0])
    if nf > 1:
        got = shift(acc, nf, 1)
        state_grad = got.astype(F32) + state_grad
    state_grad = upstream + state_grad
    grad_rows = jnp.concatenate(grad_slots)
    block = width // nc

    def columns(m):
        cut = lax.dynamic_slice_in_dim(grad_rows, (me_c ^ m) * block, block, axis=1)
        if m == 0:
            return cut
        return swap(cut, nc, m)

    cuts = [columns(m) for m in range(nc)]

    attn_gain_part = jnp.sum(state_grad * attn_out * attn_rms[:, None], axis=0)
    attn_grad_b = norm_back(attn_out, attn_rms, attn_gain[None, :], state_grad).astype(BF)
    first_hop = shift(attn_grad_b, nf, 1)
    proj_slots = [attn_grad_b, first_hop]
    for _ in range(2, nf):
        got = shift(proj_slots[-1], nf, 1)
        proj_slots.append(got)
    mixture_grads = []
    for s in range(nf):
        mixture_grads.append(contract_cols(proj_slots[s], output_weight).astype(BF))
    mixture_grad_b = jnp.concatenate(mixture_grads)

    dq = None
    sums = [{}, {}]

    def send(i, m):
        into, bit = came_from(m, orders[i])
        got = swap(sums[i].pop(m), nc, bit)
        sums[i][into] = (sums[i][into].astype(F32) + got.astype(F32)).astype(BF)
        return got

    waits = []
    for gi, group in enumerate(groups[::-1]):
        starts, kv = group_inputs(group)
        if gi:
            dq = gate(dq, *waits[gi - 1])
        dq, *out = attend_back(
            starts, query_rot, mixture_grad_b, mixture, log_total, qpos, kv, dq, heads, half
        )
        for m, a, b in zip(group, out[: len(group)], out[len(group) :]):
            sums[0][m], sums[1][m] = a, b
        waits.append([send(i, m) for i in range(2) for m in group if m & 1])
    for far in range(max(distance(m) for m in range(nc)), 0, -1):
        for i in range(2):
            for m in [m for m in sums[i] if distance(m) == far]:
                send(i, m)
    own_a, own_b = sums[0][0], sums[1][0]

    def unit_full(x):
        return lax.dynamic_update_slice_in_dim(jnp.zeros((width,), F32), x, unit_start, 0)

    def norm_grads(weighted, inner, raw, rms):
        cube = rms * rms * rms
        return [
            (
                rows_of(rms, s) * rows_of(weighted, s)
                - raw[s] * rows_of(cube, s) * inner[s][:, None] / width
            ).astype(BF)
            for s in range(nf)
        ]

    def spread(*vectors):
        return jnp.stack([v.reshape(nf, width // nf) for v in vectors], axis=1).reshape(nf, -1)

    def gathered(flat, count):
        return flat.reshape(nf, count, width // nf).transpose(1, 0, 2).reshape(count, width)

    query_weighted, query_inner, query_gain_part = unrotate(
        [dq], q_raw, query_rms, query_scale, cosine, sine, heads, True
    )
    query_inner, early_gains = slot_sum(
        query_inner.reshape(nf, rows),
        nf,
        spread(unit_full(query_gain_part[0]), attn_gain_part, mlp_gain_part),
    )
    query_grads = norm_grads(query_weighted, query_inner, q_raw, query_rms)

    x_rows = jnp.concatenate(x_slots)
    q_part = contract_rows(x_rows, jnp.concatenate(query_grads)).astype(BF)
    o_part = contract_rows(jnp.concatenate(proj_slots), mixture_b).astype(BF)
    qo_part = jnp.concatenate([q_part, o_part], axis=1)
    gate_up_sum, own_a, own_b = lax.optimization_barrier((gate_up_sum, own_a, own_b))
    qo_part, gate_up_sum = lax.optimization_barrier((qo_part, gate_up_sum))
    qo_grad = ctx_scatter(qo_part).astype(F32)
    query_grad, output_grad = qo_grad[:, :units], qo_grad[:, units:].T

    key_weighted, key_inner, key_gain_part = unrotate(
        [own_a, own_b], k_raw, key_rms, key_scale, cosine, sine, heads, False
    )
    key_inner, key_gain_sum = slot_sum(
        key_inner.reshape(nf, rows), nf, spread(unit_full(key_gain_part[0]))
    )
    key_grads = norm_grads(key_weighted, key_inner, k_raw, key_rms)
    own = jnp.concatenate([own_a[:, units:], own_b[:, units:]])
    value_grads = [rows_of(own, s) for s in range(nf)]

    started = []
    input_grad = state_grad + ring_scatter(
        lambda s: contract_cols(query_grads[s], query_weight)
        + contract_cols(key_grads[s], key_weight)
        + contract_cols(value_grads[s], value_weight),
        nf,
        started=started,
    )
    down_grad = None
    for m in range(nc):
        cut = cuts[m] if m < nc // 2 else gate(cuts[m], *started)
        for i in range(2):
            tall = activ[i][m].shape[0]
            part = contract_rows(activ[i][m], cut[i * tall : (i + 1) * tall])
            down_grad = part if down_grad is None else down_grad + part

    k_rows, v_rows, *_ = lax.optimization_barrier((jnp.concatenate(key_grads), own, *started))
    k_part = contract_rows(x_rows, k_rows).astype(BF)
    v_part = contract_rows(x_rows, v_rows).astype(BF)
    key_grad = halving(k_part, me_c, nc, orders[0])
    value_grad = halving(v_part, me_c, nc, orders[1])
    gains = jnp.concatenate([gathered(early_gains, 3), gathered(key_gain_sum, 1)])
    gains_own = halving(gains.T, me_c, nc, orders[0]).T
    ff = gate_weight.shape[1]
    gate_up = gate_up_sum.astype(F32)
    gate_grad, up_grad = gate_up[:, :ff], gate_up[:, ff:]
    return (
        block_output,
        input_grad,
        query_grad,
        key_grad,
        value_grad,
        output_grad,
        gains_own[0],
        gains_own[3],
        gains_own[1],
        gains_own[2],
        gate_grad,
        up_grad,
        down_grad,
    )


def solution(mesh):
    def layer(*args):
        return local(mesh.shape["ctx"], mesh.shape["fsdp"], *args)

    return jax.shard_map(
        layer,
        mesh=mesh,
        in_specs=(
            P(("ctx", "fsdp"), None),
            P(("ctx", "fsdp")),
            P(None, "fsdp"),
            P(None, "fsdp"),
            P(None, "fsdp"),
            P("fsdp", None),
            P(),
            P(),
            P(),
            P(),
            P(None, "fsdp"),
            P(None, "fsdp"),
            P("fsdp", None),
            P(("ctx", "fsdp"), None),
        ),
        out_specs=(
            P(("ctx", "fsdp"), None),
            P(("ctx", "fsdp"), None),
            P("ctx", "fsdp"),
            P("ctx", "fsdp"),
            P("ctx", "fsdp"),
            P("fsdp", "ctx"),
            P("ctx"),
            P("ctx"),
            P("ctx"),
            P("ctx"),
            P("ctx", "fsdp"),
            P("ctx", "fsdp"),
            P("fsdp", "ctx"),
        ),
        check_vma=False,
    )
```
